64 devices in a mesh: dp: 4 (over x, y), tp: 16 (over z, core).
Axes of the slice: x: 2, y: 2, z: 8, core: 2. Of those that a mesh axis runs over, the one named last changes fastest.
The devices are a block of a 4x4x8 slice.
Arguments:
- hidden: bfloat16 [1024, 8192], P('dp'), parts along dimension 0
- w_query: bfloat16 [8192, 8192], P(None, 'tp')
- w_key: bfloat16 [8192, 256], replicated
- w_value: bfloat16 [8192, 256], replicated
- w_out: bfloat16 [8192, 8192], P('tp')
- k_cache: bfloat16 [1024, 512, 256], P(('dp', 'tp')), parts along dimension 0
- v_cache: bfloat16 [1024, 512, 256], P(('dp', 'tp')), parts along dimension 0
- lengths: int32 [1024], P('dp'), parts along dimension 0
Outputs:
- output 1: bfloat16 [1024, 8192], P('dp', 'tp'), parts along dimension 0
- output 2: bfloat16 [1024, 512, 256], P(('dp', 'tp')), parts along dimension 0
- output 3: bfloat16 [1024, 512, 256], P(('dp', 'tp')), parts along dimension 0
There are 4 independent parts. The reference program is written for one: setup_inputs(seed, part) draws one part's arguments, and reference() takes and returns one part's arrays. A program takes and returns all parts, laid end to end along the dimension named above; an argument that names none is the same for every part.
All inputs are finite; a program needn't handle non-finite values.
Results may differ from the reference program's by a relative error of at most 0.0199816.
Values are sent between devices in bfloat16 or wider.
A program may use at most 768 MiB of HBM per device.

```python
import jax
import jax.numpy as jnp
from jax import lax

BATCH_ROWS = 256
EMBED_DIM = 8192
Q_HEADS = 32
HEAD_DIM = 256
SEQ_LEN = 512


def setup_inputs(seed: int = 0, part: int = 0) -> dict:
    part_key = jax.random.fold_in(jax.random.key(seed), part)
    key_hid, key_kc, key_vc, key_mean, key_len, key_top = jax.random.split(part_key, 6)
    weight_keys = jax.random.split(jax.random.key(seed + 1), 4)
    total_cols = Q_HEADS * HEAD_DIM
    hidden = jax.random.normal(key_hid, (BATCH_ROWS, EMBED_DIM), jnp.float32)
    w_query = jax.random.normal(weight_keys[0], (EMBED_DIM, total_cols), jnp.float32) * EMBED_DIM ** -0.5
    w_key = jax.random.normal(weight_keys[1], (EMBED_DIM, HEAD_DIM), jnp.float32) * (2.5 * EMBED_DIM ** -0.5)
    w_value = jax.random.normal(weight_keys[2], (EMBED_DIM, HEAD_DIM), jnp.float32) * EMBED_DIM ** -0.5
    w_out = jax.random.normal(weight_keys[3], (total_cols, EMBED_DIM), jnp.float32) * total_cols ** -0.5
    k_cache = 2.5 * jax.random.normal(key_kc, (BATCH_ROWS, SEQ_LEN, HEAD_DIM), jnp.float32)
    v_mean = 0.5 * jax.random.normal(key_mean, (BATCH_ROWS, 1, HEAD_DIM), jnp.float32)
    v_cache = v_mean + jax.random.normal(key_vc, (BATCH_ROWS, SEQ_LEN, HEAD_DIM), jnp.float32)
    drawn_len = jax.random.randint(key_len, (BATCH_ROWS,), 0, SEQ_LEN)
    top_row = jax.random.randint(key_top, (), 0, BATCH_ROWS)
    lengths = jnp.where(jnp.arange(BATCH_ROWS) == top_row, SEQ_LEN - 1, drawn_len).astype(jnp.int32)
    return {
        'hidden': hidden.astype(jnp.bfloat16),
        'w_query': w_query.astype(jnp.bfloat16),
        'w_key': w_key.astype(jnp.bfloat16),
        'w_value': w_value.astype(jnp.bfloat16),
        'w_out': w_out.astype(jnp.bfloat16),
        'k_cache': k_cache.astype(jnp.bfloat16),
        'v_cache': v_cache.astype(jnp.bfloat16),
        'lengths': lengths,
    }


def rope_angles(positions):
    half_dim = HEAD_DIM // 2
    inv_freq = 10000.0 ** (-(jnp.arange(half_dim, dtype=jnp.float32) * 2.0) / HEAD_DIM)
    return positions.astype(jnp.float32)[:, None] * inv_freq[None, :]


def apply_rope(values_in, angles):
    half_dim = values_in.shape[-1] // 2
    first_half = values_in[..., :half_dim]
    second_half = values_in[..., half_dim:]
    cosines = jnp.cos(angles)
    sines = jnp.sin(angles)
    return jnp.concatenate([first_half * cosines - second_half * sines, second_half * cosines + first_half * sines], axis=-1)


def attend_row(row_args):
    q_row, k_row, v_row, length = row_args
    scores = jnp.dot(q_row, k_row.T, preferred_element_type=jnp.float32) * (HEAD_DIM ** -0.5)
    valid_mask = jnp.arange(SEQ_LEN)[None, :] <= length
    scores = jnp.where(valid_mask, scores, -1e30)
    row_max = jnp.max(scores, axis=-1, keepdims=True)
    weights = jnp.exp(scores - row_max)
    denominator = jnp.sum(weights, axis=-1, keepdims=True)
    summed = jnp.dot(weights.astype(jnp.bfloat16), v_row, preferred_element_type=jnp.float32)
    return (summed / denominator).astype(jnp.bfloat16)


def reference(hidden, w_query, w_key, w_value, w_out, k_cache, v_cache, lengths):
    q_flat = jnp.dot(hidden, w_query, preferred_element_type=jnp.float32).astype(jnp.bfloat16)
    k_new = jnp.dot(hidden, w_key, preferred_element_type=jnp.float32).astype(jnp.bfloat16)
    v_new = jnp.dot(hidden, w_value, preferred_element_type=jnp.float32).astype(jnp.bfloat16)
    angles = rope_angles(lengths)
    q_heads = q_flat.reshape(BATCH_ROWS, Q_HEADS, HEAD_DIM).astype(jnp.float32)
    q_rot = apply_rope(q_heads, angles[:, None, :]).astype(jnp.bfloat16)
    k_rot = apply_rope(k_new.astype(jnp.float32), angles).astype(jnp.bfloat16)
    new_slot = (jnp.arange(SEQ_LEN)[None, :] == lengths[:, None])[:, :, None]
    k_cache_out = jnp.where(new_slot, k_rot[:, None, :], k_cache)
    v_cache_out = jnp.where(new_slot, v_new[:, None, :], v_cache)
    attn_out = lax.map(attend_row, (q_rot, k_cache_out, v_cache_out, lengths))
    y_out = jnp.dot(attn_out.reshape(BATCH_ROWS, Q_HEADS * HEAD_DIM), w_out, preferred_element_type=jnp.float32).astype(jnp.bfloat16)
    return (y_out, k_cache_out, v_cache_out)
```

```python
import functools

import jax
import jax.numpy as jnp
from jax import lax
from jax.experimental import pallas as pl
from jax.experimental.pallas import tpu as pltpu
from jax.sharding import PartitionSpec as P

MESH = pl.DeviceIdType.MESH
HALVES = 2
K_CHUNKS = 8
F32 = jnp.float32
BF16 = jnp.bfloat16


def rope_angles(positions, head_dim):
    half_dim = head_dim // 2
    inv_freq = 10000.0 ** (-(jnp.arange(half_dim, dtype=jnp.float32) * 2.0) / head_dim)
    return positions.astype(jnp.float32)[:, None] * inv_freq[None, :]


def decode_kernel(
    n, hid_hbm, wq_hbm, wk_hbm, wv_hbm, wo_hbm, kc_hbm, vc_hbm, cos_ref, sin_ref, len_ref,
    y_ref, knew_ref, vnew_ref,
    hid, wq, wk, wv, wo, kc, vc, acc, qs, qr, q_lo, q_hi, o_lo, o_hi, osend, orecv, kf, vf,
    pm, ps, pr, rs, rr,
    sem_h, sem_w, sem_kv, sem_kc, sem_vc, sem_wo, q_ssem, q_rsem, o_ssem, o_rsem, p_ssem, p_rsem, r_ssem, r_rsem,
):
    me = lax.axis_index("tp")
    chips = n // 2
    core = lax.rem(me, 2)
    chip = me // 2
    partner = me + 1 - 2 * core
    right = lax.rem(me + 2, n)
    left = lax.rem(me + n - 2, n)
    neighbours = (right, left)

    batch, depth = hid.shape
    cols = wq.shape[1]
    rows = batch // n
    half_rows = rows // HALVES
    seq_len, head_dim = kc.shape[1:]
    half_dim = head_dim // 2
    dev_heads = cols // head_dim
    heads = dev_heads * n
    block = depth // K_CHUNKS
    part = cols // 2
    scale = head_dim ** -0.5

    barrier = pltpu.get_barrier_semaphore()

    def greet(i, carry):
        pl.semaphore_signal(barrier, inc=1, device_id={"tp": lax.rem(me + i, n)}, device_id_type=MESH)
        return carry

    lax.fori_loop(1, n, greet, 0)

    def load_h(i):
        return pltpu.make_async_copy(hid_hbm.at[:, pl.ds(i * block, block)], hid.at[:, pl.ds(i * block, block)], sem_h.at[i])

    def load_w(i):
        return pltpu.make_async_copy(wq_hbm.at[pl.ds(i * block, block)], wq.at[pl.ds(i * block, block)], sem_w.at[i])

    def load_cache(hbm, vmem, sem, h):
        return pltpu.make_async_copy(hbm.at[pl.ds(h * half_rows, half_rows)], vmem.at[pl.ds(h * half_rows, half_rows)], sem.at[h])

    wk_copy = pltpu.make_async_copy(wk_hbm, wk, sem_kv.at[0])
    wv_copy = pltpu.make_async_copy(wv_hbm, wv, sem_kv.at[1])
    wo_copy = pltpu.make_async_copy(wo_hbm, wo, sem_wo.at[0])

    for i in range(K_CHUNKS):
        load_h(i).start()
        load_w(i).start()
    acc[...] = jnp.zeros_like(acc)

    def q_step(i):
        span = pl.ds(pl.multiple_of(i * block, block), block)
        acc[...] += jnp.dot(hid[:, span], wq[span, :], preferred_element_type=F32)

    for i in range(K_CHUNKS):
        load_h(i).wait()
        load_w(i).wait()
        if i == K_CHUNKS - 2:
            wk_copy.start()
            wv_copy.start()
            for h in range(HALVES):
                load_cache(kc_hbm, kc, sem_kc, h).start()
                load_cache(vc_hbm, vc, sem_vc, h).start()
            wo_copy.start()
        q_step(i)

    q_all = acc[...].reshape(n, HALVES, half_rows, cols)
    for h in range(HALVES):
        qs[h] = q_all[:, h].astype(BF16)

    pl.semaphore_wait(barrier, n - 1)

    def exchange(src, dst, send_sem, recv_sem, h):
        def send(i, carry):
            peer = lax.rem(me + i, n)
            pltpu.make_async_remote_copy(
                src_ref=src.at[h, peer],
                dst_ref=dst.at[h, me],
                send_sem=send_sem.at[h],
                recv_sem=recv_sem.at[h],
                device_id={"tp": peer},
                device_id_type=MESH,
            ).start()
            return carry

        lax.fori_loop(1, n, send, 0)
        dst[h, me] = src[h, me]

    def exchange_wait(buf, sem, h):
        others = buf.at[h, pl.ds(0, n - 1)]
        pltpu.make_async_copy(others, others, sem.at[h]).wait()

    for h in range(HALVES):
        exchange(qs, qr, q_ssem, q_rsem, h)

    wk_copy.wait()
    wv_copy.wait()
    own = pl.ds(pl.multiple_of(me * rows, rows), rows)

    def kv_step(i, carry):
        k_sum, v_sum = carry
        span = pl.ds(pl.multiple_of(i * block, block), block)
        h_own = hid[own, span]
        return (
            k_sum + jnp.dot(h_own, wk[span, :], preferred_element_type=F32),
            v_sum + jnp.dot(h_own, wv[span, :], preferred_element_type=F32),
        )

    zero = jnp.zeros((rows, head_dim), F32)
    k_sum, v_sum = lax.fori_loop(0, K_CHUNKS, kv_step, (zero, zero))
    k_full = k_sum.astype(BF16).astype(F32)
    cosines, sines = cos_ref[...], sin_ref[...]
    k_lo, k_hi = k_full[:, :half_dim], k_full[:, half_dim:]
    k_rot = jnp.concatenate([k_lo * cosines - k_hi * sines, k_hi * cosines + k_lo * sines], axis=-1).astype(BF16)
    knew_ref[...] = k_rot
    vnew_ref[...] = v_sum.astype(BF16)
    kf[...] = k_rot.astype(F32)
    vf[...] = v_sum.astype(BF16).astype(F32)

    slots = lax.broadcasted_iota(jnp.int32, (heads, seq_len), 1)

    def attend(h):
        exchange_wait(qr, q_rsem, h)
        span = pl.ds(h * half_rows, half_rows)
        cosines, sines = cos_ref[span, :], sin_ref[span, :]
        for src in range(n):
            for j in range(dev_heads):
                x = qr[h, src, :, pl.ds(j * head_dim, head_dim)].astype(F32)
                lo, hi = x[:, :half_dim], x[:, half_dim:]
                place = pl.ds(src * dev_heads + j, half_rows, stride=heads)
                q_lo[place, :] = lo * cosines - hi * sines
                q_hi[place, :] = hi * cosines + lo * sines
        load_cache(kc_hbm, kc, sem_kc, h).wait()
        load_cache(vc_hbm, vc, sem_vc, h).wait()
        for r in range(half_rows):
            b = h * half_rows + r
            at = pl.ds(r * heads, heads)
            q = jnp.concatenate([q_lo[at, :], q_hi[at, :]], axis=-1).astype(BF16)
            length = len_ref[me * rows + b]
            k_row, v_row = kf[pl.ds(b, 1), :], vf[pl.ds(b, 1), :]
            s = lax.dot_general(q, kc[b], (((1,), (1,)), ((), ())), preferred_element_type=F32) * scale
            s_new = jnp.sum(q.astype(F32) * k_row, axis=-1, keepdims=True) * scale
            s = jnp.where(slots < length, s, -1e30)
            top = jnp.maximum(jnp.max(s, axis=-1, keepdims=True), s_new)
            e = jnp.where(slots < length, jnp.exp(s - top), 0.0)
            e_new = jnp.exp(s_new - top)
            total = jnp.sum(e, axis=-1, keepdims=True) + e_new
            o = jnp.dot(e.astype(BF16), vc[b], preferred_element_type=F32)
            o = (o + e_new.astype(BF16).astype(F32) * v_row) / total
            o_lo[at, :] = o[:, :half_dim]
            o_hi[at, :] = o[:, half_dim:]
        for dst in range(n):
            for j in range(dev_heads):
                place = pl.ds(dst * dev_heads + j, half_rows, stride=heads)
                osend[h, dst, :, pl.ds(j * head_dim, half_dim)] = o_lo[place, :].astype(BF16)
                osend[h, dst, :, pl.ds(j * head_dim + half_dim, half_dim)] = o_hi[place, :].astype(BF16)
        exchange(osend, orecv, o_ssem, o_rsem, h)

    for h in range(HALVES):
        attend(h)

    wo_copy.wait()

    def owner(k, way):
        return lax.rem(chip + chips - 1 - k, chips) if way == 0 else lax.rem(chip + 1 + k, chips)

    def partner_copy(h, k):
        return pltpu.make_async_remote_copy(
            src_ref=ps.at[h, k], dst_ref=pr.at[h, k], send_sem=p_ssem.at[h], recv_sem=p_rsem.at[h, k],
            device_id={"tp": partner}, device_id_type=MESH,
        )

    def multiply(h, k):
        o_cols = orecv[h].reshape(n * half_rows, cols)
        for way in range(2):
            base = owner(k, way) * 2
            other = pl.ds(pl.multiple_of((base + 1 - core) * cols + way * part, part), part)
            mine = pl.ds(pl.multiple_of((base + core) * cols + way * part, part), part)
            ps[h, k, way] = jnp.dot(o_cols, wo[:, other], preferred_element_type=F32).astype(BF16)
            pm[h, k, way] = jnp.dot(o_cols, wo[:, mine], preferred_element_type=F32)
        partner_copy(h, k).start()

    def ring_copy(h, k, way):
        return pltpu.make_async_remote_copy(
            src_ref=rs.at[h, k, way], dst_ref=rr.at[h, k, way], send_sem=r_ssem.at[h], recv_sem=r_rsem.at[h, k, way],
            device_id={"tp": neighbours[way]}, device_id_type=MESH,
        )

    def reduce_step(h, k):
        partner_copy(h, k).wait_recv()
        for way in range(2):
            value = pm[h, k, way] + pr[h, k, way].astype(F32)
            if k > 0:
                ring_copy(h, k - 1, way).wait_recv()
                value = value + rr[h, k - 1, way].astype(F32)
            if k < chips - 1:
                rs[h, k, way] = value.astype(BF16)
                ring_copy(h, k, way).start()
            else:
                out = value.astype(BF16) if HALVES == 1 else value
                y_ref[:, h, :, pl.ds(way * part, part)] = out.reshape(n, half_rows, part).astype(BF16)

    def multiplies(h, lo, hi):
        def body(k, carry):
            multiply(h, k)
            return carry

        lax.fori_loop(lo, hi, body, 0)

    for h in range(HALVES):
        exchange_wait(orecv, o_rsem, h)
        multiplies(h, 0, 2)
        reduce_step(h, 0)
        if h == 0:
            multiplies(h, 2, chips)
    reduce_step(0, 1)
    for h in range(1, HALVES):
        multiplies(h, 2, chips)
    for k in range(1, chips):
        for h in range(HALVES):
            if (h, k) != (0, 1):
                reduce_step(h, k)

    for h in range(HALVES):
        exchange_wait(qs, q_ssem, h)
        exchange_wait(osend, o_ssem, h)
        pltpu.make_async_copy(ps.at[h], ps.at[h], p_ssem.at[h]).wait()
        pltpu.make_async_copy(rs.at[h], rs.at[h], r_ssem.at[h]).wait()


def solution(mesh):
    n = mesh.shape["tp"]
    cache_spec = P(("dp", "tp"), None, None)

    def local_step(hidden, w_query, w_key, w_value, w_out, k_cache, v_cache, lengths):
        rows, seq_len, head_dim = k_cache.shape
        batch, depth = hidden.shape
        cols = w_query.shape[1]
        half_rows = rows // HALVES
        chips = n // 2
        part = cols // 2
        heads = cols * n // head_dim
        half_dim = head_dim // 2
        own_lengths = lax.dynamic_slice_in_dim(lengths, lax.axis_index("tp") * rows, rows, axis=0)
        angles = rope_angles(own_lengths, head_dim)
        any_spec = pl.BlockSpec(memory_space=pl.ANY)
        vmem_spec = pl.BlockSpec(memory_space=pltpu.VMEM)
        smem_spec = pl.BlockSpec(memory_space=pltpu.SMEM)
        dma = pltpu.SemaphoreType.DMA
        piece = (n * half_rows, part)
        y, k_new, v_new = pl.pallas_call(
            functools.partial(decode_kernel, n),
            out_shape=(
                jax.ShapeDtypeStruct((n, HALVES, half_rows, cols), BF16),
                jax.ShapeDtypeStruct((rows, head_dim), BF16),
                jax.ShapeDtypeStruct((rows, head_dim), BF16),
            ),
            in_specs=[any_spec] * 7 + [vmem_spec, vmem_spec, smem_spec],
            out_specs=(vmem_spec, vmem_spec, vmem_spec),
            scratch_shapes=[
                pltpu.VMEM((batch, depth), BF16),
                pltpu.VMEM((depth, cols), BF16),
                pltpu.VMEM((depth, head_dim), BF16),
                pltpu.VMEM((depth, head_dim), BF16),
                pltpu.VMEM(w_out.shape, BF16),
                pltpu.VMEM(k_cache.shape, BF16),
                pltpu.VMEM(v_cache.shape, BF16),
                pltpu.VMEM((batch, cols), F32),
                pltpu.VMEM((HALVES, n, half_rows, cols), BF16),
                pltpu.VMEM((HALVES, n, half_rows, cols), BF16),
                pltpu.VMEM((half_rows * heads, half_dim), F32),
                pltpu.VMEM((half_rows * heads, half_dim), F32),
                pltpu.VMEM((half_rows * heads, half_dim), F32),
                pltpu.VMEM((half_rows * heads, half_dim), F32),
                pltpu.VMEM((HALVES, n, half_rows, cols), BF16),
                pltpu.VMEM((HALVES, n, half_rows, cols), BF16),
                pltpu.VMEM((rows, head_dim), F32),
                pltpu.VMEM((rows, head_dim), F32),
                pltpu.VMEM((HALVES, chips, 2) + piece, F32),
                pltpu.VMEM((HALVES, chips, 2) + piece, BF16),
                pltpu.VMEM((HALVES, chips, 2) + piece, BF16),
                pltpu.VMEM((HALVES, chips - 1, 2) + piece, BF16),
                pltpu.VMEM((HALVES, chips - 1, 2) + piece, BF16),
                dma((K_CHUNKS,)),
                dma((K_CHUNKS,)),
                dma((2,)),
                dma((HALVES,)),
                dma((HALVES,)),
                dma((1,)),
                dma((HALVES,)),
                dma((HALVES,)),
                dma((HALVES,)),
                dma((HALVES,)),
                dma((HALVES,)),
                dma((HALVES, chips)),
                dma((HALVES,)),
                dma((HALVES, chips - 1, 2)),
            ],
            compiler_params=pltpu.CompilerParams(
                collective_id=0, has_side_effects=True, vmem_limit_bytes=52 * 1024 * 1024
            ),
        )(hidden, w_query, w_key, w_value, w_out, k_cache, v_cache, jnp.cos(angles), jnp.sin(angles), lengths)
        new_slot = (lax.broadcasted_iota(jnp.int32, (1, seq_len), 1) == own_lengths[:, None])[:, :, None]
        k_out = jnp.where(new_slot, k_new[:, None, :], k_cache)
        v_out = jnp.where(new_slot, v_new[:, None, :], v_cache)
        return y.reshape(batch, cols), k_out, v_out

    return jax.shard_map(
        local_step,
        mesh=mesh,
        in_specs=(P("dp", None), P(None, "tp"), P(), P(), P("tp", None), cache_spec, cache_spec, P("dp")),
        out_specs=(P("dp", "tp"), cache_spec, cache_spec),
        check_vma=False,
    )
```

```python
import functools

import jax
import jax.numpy as jnp
from jax import lax
from jax.experimental import pallas as pl
from jax.experimental.pallas import tpu as pltpu
from jax.sharding import PartitionSpec as P

MESH = pl.DeviceIdType.MESH
HALVES = 2
SUBS = 2
K_CHUNKS = 8
AHEAD = 6
WRITES = 4
F32 = jnp.float32
BF16 = jnp.bfloat16


def decode_kernel(
    n, hid_hbm, wq_hbm, wk_hbm, wv_hbm, wo_hbm, kc_hbm, vc_hbm, len_hbm, freq_ref,
    y_ref, kc, vc,
    hid, wq, wk, wv, wo, lens, acc, qs, qr, q_lo, q_hi, o_lo, o_hi, s_buf, e_buf, osend, orecv, cos_ref, sin_ref, kf, vf,
    pm, ps, pr, rs, rr,
    sem_len, sem_h, sem_w, sem_k, sem_v, sem_kc, sem_vc, sem_wo,
    q_ssem, q_rsem, o_ssem, o_rsem, p_ssem, p_rsem, r_ssem, r_rsem,
):
    me = lax.axis_index("tp")
    chips = n // 2
    core = lax.rem(me, 2)
    chip = me // 2
    partner = me + 1 - 2 * core
    neighbours = (lax.rem(me + 2, n), lax.rem(me + n - 2, n))

    batch, depth = hid.shape
    cols = wq.shape[1]
    rows = batch // n
    half_rows = rows // HALVES
    seq_len, head_dim = kc.shape[1:]
    half_dim = head_dim // 2
    dev_heads = cols // head_dim
    heads = dev_heads * n
    block = depth // K_CHUNKS
    part = cols // (2 * SUBS)
    out_block = wo.shape[1] // 4
    scale = head_dim ** -0.5

    def load_h(i):
        return pltpu.make_async_copy(hid_hbm.at[:, pl.ds(i * block, block)], hid.at[:, pl.ds(i * block, block)], sem_h.at[i])

    def load_rows(hbm, vmem, sem, size, i):
        return pltpu.make_async_copy(hbm.at[pl.ds(i * size, size)], vmem.at[pl.ds(i * size, size)], sem.at[i])

    def load_w(i):
        return load_rows(wq_hbm, wq, sem_w, block, i)

    def load_k(i):
        return load_rows(wk_hbm, wk, sem_k, 2 * block, i)

    def load_v(i):
        return load_rows(wv_hbm, wv, sem_v, 2 * block, i)

    def load_kc(h):
        return load_rows(kc_hbm, kc, sem_kc, half_rows, h)

    def load_vc(h):
        return load_rows(vc_hbm, vc, sem_vc, half_rows, h)

    def load_o(i):
        span = pl.ds(i * out_block, out_block)
        return pltpu.make_async_copy(wo_hbm.at[:, span], wo.at[:, span], sem_wo.at[i])

    len_copy = pltpu.make_async_copy(len_hbm, lens, sem_len.at[0])
    queue = [(load_h(i), load_w(i)) for i in range(K_CHUNKS)]
    queue += [(load_k(i), load_v(i)) for i in range(K_CHUNKS // 2)]
    queue += [(load_kc(h), load_vc(h)) for h in range(HALVES)]
    queue += [(load_o(i),) for i in range(4)]

    def issue(count):
        for _ in range(count):
            if queue:
                for copy in queue.pop(0):
                    copy.start()

    len_copy.start()
    issue(AHEAD)

    barrier = pltpu.get_barrier_semaphore()
    order = sorted(range(1, n), key=lambda i: (min(i, n - i), i), reverse=True)
    for i in order:
        pl.semaphore_signal(barrier, inc=1, device_id={"tp": lax.rem(me + i, n)}, device_id_type=MESH)

    with jax.named_scope("angles"):
        len_copy.wait()
        for r in range(rows):
            cos_ref[pl.ds(r, 1), :] = lens[me * rows + r].astype(F32) * freq_ref[...]
        angles = cos_ref[...]
        sin_ref[...] = jnp.sin(angles)
        cos_ref[...] = jnp.cos(angles)

    with jax.named_scope("q_mm"):
        for i in range(K_CHUNKS):
            load_h(i).wait()
            load_w(i).wait()
            issue(1)
            span = pl.ds(i * block, block)
            term = jnp.dot(hid[:, span], wq[span, :], preferred_element_type=F32)
            if i == 0:
                acc[...] = term
            elif i < K_CHUNKS - 1:
                acc[...] += term
            else:
                q_all = (acc[...] + term).reshape(n, HALVES, half_rows, cols)
                for h in range(HALVES):
                    qs[h] = q_all[:, h].astype(BF16)

    with jax.named_scope("barrier"):
        pl.semaphore_wait(barrier, n - 1)

    def exchange(src, dst, send_sem, recv_sem, h):
        for i in order:
            peer = lax.rem(me + i, n)
            pltpu.make_async_remote_copy(
                src_ref=src.at[h, peer],
                dst_ref=dst.at[h, me],
                send_sem=send_sem.at[h],
                recv_sem=recv_sem.at[h],
                device_id={"tp": peer},
                device_id_type=MESH,
            ).start()
        dst[h, me] = src[h, me]

    def exchange_wait(buf, sem, h):
        others = buf.at[h, pl.ds(0, n - 1)]
        pltpu.make_async_copy(others, others, sem.at[h]).wait()

    with jax.named_scope("q_send"):
        for h in range(HALVES):
            exchange(qs, qr, q_ssem, q_rsem, h)

    own = pl.ds(pl.multiple_of(me * rows, rows), rows)
    k_sum = jnp.zeros((rows, head_dim), F32)
    v_sum = jnp.zeros((rows, head_dim), F32)
    for i in range(K_CHUNKS // 2):
        with jax.named_scope(f"kv_wait{i}"):
            load_k(i).wait()
            load_v(i).wait()
        issue(1)
        span = pl.ds(i * 2 * block, 2 * block)
        h_own = hid[own, span]
        k_sum += jnp.dot(h_own, wk[span, :], preferred_element_type=F32)
        v_sum += jnp.dot(h_own, wv[span, :], preferred_element_type=F32)
    k_full = k_sum.astype(BF16).astype(F32)
    cosines, sines = cos_ref[...], sin_ref[...]
    k_lo, k_hi = k_full[:, :half_dim], k_full[:, half_dim:]
    k_rot = jnp.concatenate([k_lo * cosines - k_hi * sines, k_hi * cosines + k_lo * sines], axis=-1)
    kf[...] = k_rot.astype(BF16).astype(F32)
    vf[...] = v_sum.astype(BF16).astype(F32)
    issue(len(queue))

    slots = lax.broadcasted_iota(jnp.int32, (heads, seq_len), 1)

    def attend(h):
        with jax.named_scope(f"q_wait{h}"):
            exchange_wait(qr, q_rsem, h)
        with jax.named_scope(f"rope{h}"):
            span = pl.ds(h * half_rows, half_rows)
            cosines, sines = cos_ref[span, :], sin_ref[span, :]
            for src in range(n):
                for j in range(dev_heads):
                    x = qr[h, src, :, pl.ds(j * head_dim, head_dim)].astype(F32)
                    lo, hi = x[:, :half_dim], x[:, half_dim:]
                    place = pl.ds(src * dev_heads + j, half_rows, stride=heads)
                    q_lo[place, :] = lo * cosines - hi * sines
                    q_hi[place, :] = hi * cosines + lo * sines
        with jax.named_scope(f"cache_wait{h}"):
            load_kc(h).wait()
            load_vc(h).wait()
        with jax.named_scope(f"rows{h}"):
            ats = [pl.ds(r * heads, heads) for r in range(half_rows)]
            news = []
            for r, at in enumerate(ats):
                b = h * half_rows + r
                q = jnp.concatenate([q_lo[at, :], q_hi[at, :]], axis=-1).astype(BF16)
                s_buf[at, :] = lax.dot_general(q, kc[b], (((1,), (1,)), ((), ())), preferred_element_type=F32)
                news.append(jnp.sum(q.astype(F32) * kf[pl.ds(b, 1), :], axis=-1, keepdims=True) * scale)
            sums = []
            for r, at in enumerate(ats):
                length = lens[me * rows + h * half_rows + r]
                s = jnp.where(slots < length, s_buf[at, :] * scale, -1e30)
                top = jnp.maximum(jnp.max(s, axis=-1, keepdims=True), news[r])
                e = jnp.where(slots < length, jnp.exp(s - top), 0.0)
                e_new = jnp.exp(news[r] - top)
                e_buf[at, :] = e.astype(BF16)
                sums.append((e_new, jnp.sum(e, axis=-1, keepdims=True) + e_new))
            for r, at in enumerate(ats):
                b = h * half_rows + r
                e_new, total = sums[r]
                o = jnp.dot(e_buf[at, :], vc[b], preferred_element_type=F32)
                o = (o + e_new.astype(BF16).astype(F32) * vf[pl.ds(b, 1), :]) / total
                o_lo[at, :] = o[:, :half_dim]
                o_hi[at, :] = o[:, half_dim:]
        with jax.named_scope(f"opack{h}"):
            for dst in range(n):
                for j in range(dev_heads):
                    place = pl.ds(dst * dev_heads + j, half_rows, stride=heads)
                    osend[h, dst, :, pl.ds(j * head_dim, half_dim)] = o_lo[place, :].astype(BF16)
                    osend[h, dst, :, pl.ds(j * head_dim + half_dim, half_dim)] = o_hi[place, :].astype(BF16)
        with jax.named_scope(f"o_send{h}"):
            exchange(osend, orecv, o_ssem, o_rsem, h)

    for h in range(HALVES):
        attend(h)

    def owner(k, way):
        return lax.rem(chip + chips - 1 - k, chips) if way == 0 else lax.rem(chip + 1 + k, chips)

    def partner_copy(h, k):
        return pltpu.make_async_remote_copy(
            src_ref=ps.at[h, k], dst_ref=pr.at[h, k], send_sem=p_ssem.at[h], recv_sem=p_rsem.at[h, k],
            device_id={"tp": partner}, device_id_type=MESH,
        )

    def multiply(h, k):
        o_cols = orecv[h].reshape(n * half_rows, cols)

        def product(way, side):
            first = pl.multiple_of((owner(k, way) * 2 + side) * cols + way * (cols // 2), cols // 2)
            return jnp.dot(o_cols, wo[:, pl.ds(first, cols // 2)], preferred_element_type=F32)

        for way in range(2):
            ahead = product(way, 1 - core).astype(BF16)
            for sub in range(SUBS):
                ps[h, k, way, sub] = ahead[:, sub * part : (sub + 1) * part]
        partner_copy(h, k).start()
        for way in range(2):
            kept = product(way, core)
            for sub in range(SUBS):
                pm[h, k, way, sub] = kept[:, sub * part : (sub + 1) * part]

    def ring_copy(h, k, way, sub):
        return pltpu.make_async_remote_copy(
            src_ref=rs.at[h, k, way, sub], dst_ref=rr.at[h, k, way, sub],
            send_sem=r_ssem.at[h], recv_sem=r_rsem.at[h, k, way, sub],
            device_id={"tp": neighbours[way]}, device_id_type=MESH,
        )

    def reduce_step(h, k):
        with jax.named_scope(f"pw{h}_{k}"):
            partner_copy(h, k).wait_recv()
        for sub in range(SUBS):
            for way in range(2):
                value = pm[h, k, way, sub] + pr[h, k, way, sub].astype(F32)
                if k > 0:
                    with jax.named_scope(f"rw{h}_{k}_{way}_{sub}"):
                        ring_copy(h, k - 1, way, sub).wait_recv()
                    value = value + rr[h, k - 1, way, sub].astype(F32)
                if k < chips - 1:
                    rs[h, k, way, sub] = value.astype(BF16)
                    ring_copy(h, k, way, sub).start()
                else:
                    out = value.reshape(n, half_rows, part).astype(BF16)
                    y_ref[:, h, :, pl.ds((way * SUBS + sub) * part, part)] = out

    def multiplies(h, lo, hi):
        def body(k, carry):
            multiply(h, k)
            return carry

        with jax.named_scope(f"mult{h}_{lo}"):
            lax.fori_loop(lo, hi, body, 0)

    row_slots = lax.broadcasted_iota(jnp.int32, (seq_len, head_dim), 0)

    def update(b):
        with jax.named_scope(f"update{b}"):
            length = lens[me * rows + b]
            for cache, new in ((kc, kf), (vc, vf)):
                row = jnp.broadcast_to(new[pl.ds(b, 1), :].astype(BF16), (seq_len, head_dim))
                cache[b] = jnp.where(row_slots == length, row, cache[b])

    with jax.named_scope("wo_wait"):
        for i in range(4):
            load_o(i).wait()
    for h in range(HALVES):
        with jax.named_scope(f"o_wait{h}"):
            exchange_wait(orecv, o_rsem, h)
        multiplies(h, 0, 1)
        multiplies(h, 1, 3)
        reduce_step(h, 0)
        if h == 0:
            multiplies(h, 3, chips)
    reduce_step(0, 1)
    for h in range(1, HALVES):
        multiplies(h, 3, chips)
    pending = list(range(rows))
    for k in range(1, chips):
        for h in range(HALVES):
            if (h, k) != (0, 1):
                reduce_step(h, k)
                for _ in range(2):
                    if pending and k > 1:
                        update(pending.pop(0))
    for b in pending:
        update(b)

    with jax.named_scope("tail"):
        for h in range(HALVES):
            exchange_wait(qs, q_ssem, h)
            exchange_wait(osend, o_ssem, h)
            pltpu.make_async_copy(ps.at[h], ps.at[h], p_ssem.at[h]).wait()
            pltpu.make_async_copy(rs.at[h], rs.at[h], r_ssem.at[h]).wait()


def write_kernel(y, kc, vc, y_out, k_out, v_out, sem):
    rows = kc.shape[0] // WRITES
    copies = [pltpu.make_async_copy(y, y_out, sem.at[0])]
    for i in range(WRITES):
        span = pl.ds(i * rows, rows)
        copies.append(pltpu.make_async_copy(kc.at[span], k_out.at[span], sem.at[1 + 2 * i]))
        copies.append(pltpu.make_async_copy(vc.at[span], v_out.at[span], sem.at[2 + 2 * i]))
    for copy in copies:
        copy.start()
    for copy in copies:
        copy.wait()


def solution(mesh):
    n = mesh.shape["tp"]
    cache_spec = P(("dp", "tp"), None, None)

    def local_step(hidden, w_query, w_key, w_value, w_out, k_cache, v_cache, lengths):
        rows, seq_len, head_dim = k_cache.shape
        batch, depth = hidden.shape
        cols = w_query.shape[1]
        half_rows = rows // HALVES
        chips = n // 2
        heads = cols * n // head_dim
        half_dim = head_dim // 2
        inv_freq = 10000.0 ** (-(jnp.arange(half_dim, dtype=F32) * 2.0) / head_dim)
        hbm_spec = pl.BlockSpec(memory_space=pltpu.HBM)
        vmem_spec = pl.BlockSpec(memory_space=pltpu.VMEM)
        dma = pltpu.SemaphoreType.DMA
        piece = (2, SUBS, n * half_rows, cols // (2 * SUBS))
        y, k_vmem, v_vmem = pl.pallas_call(
            functools.partial(decode_kernel, n),
            out_shape=(
                jax.ShapeDtypeStruct((n, HALVES, half_rows, cols), BF16),
                jax.ShapeDtypeStruct(k_cache.shape, BF16),
                jax.ShapeDtypeStruct(v_cache.shape, BF16),
            ),
            in_specs=[hbm_spec] * 8 + [vmem_spec],
            out_specs=(vmem_spec, vmem_spec, vmem_spec),
            scratch_shapes=[
                pltpu.VMEM((batch, depth), BF16),
                pltpu.VMEM((depth, cols), BF16),
                pltpu.VMEM((depth, head_dim), BF16),
                pltpu.VMEM((depth, head_dim), BF16),
                pltpu.VMEM(w_out.shape, BF16),
                pltpu.SMEM((batch,), jnp.int32),
                pltpu.VMEM((batch, cols), F32),
                pltpu.VMEM((HALVES, n, half_rows, cols), BF16),
                pltpu.VMEM((HALVES, n, half_rows, cols), BF16),
                pltpu.VMEM((half_rows * heads, half_dim), F32),
                pltpu.VMEM((half_rows * heads, half_dim), F32),
                pltpu.VMEM((half_rows * heads, half_dim), F32),
                pltpu.VMEM((half_rows * heads, half_dim), F32),
                pltpu.VMEM((half_rows * heads, seq_len), F32),
                pltpu.VMEM((half_rows * heads, seq_len), BF16),
                pltpu.VMEM((HALVES, n, half_rows, cols), BF16),
                pltpu.VMEM((HALVES, n, half_rows, cols), BF16),
                pltpu.VMEM((rows, half_dim), F32),
                pltpu.VMEM((rows, half_dim), F32),
                pltpu.VMEM((rows, head_dim), F32),
                pltpu.VMEM((rows, head_dim), F32),
                pltpu.VMEM((HALVES, chips) + piece, F32),
                pltpu.VMEM((HALVES, chips) + piece, BF16),
                pltpu.VMEM((HALVES, chips) + piece, BF16),
                pltpu.VMEM((HALVES, chips - 1) + piece, BF16),
                pltpu.VMEM((HALVES, chips - 1) + piece, BF16),
                dma((1,)),
                dma((K_CHUNKS,)),
                dma((K_CHUNKS,)),
                dma((K_CHUNKS // 2,)),
                dma((K_CHUNKS // 2,)),
                dma((HALVES,)),
                dma((HALVES,)),
                dma((4,)),
                dma((HALVES,)),
                dma((HALVES,)),
                dma((HALVES,)),
                dma((HALVES,)),
                dma((HALVES,)),
                dma((HALVES, chips)),
                dma((HALVES,)),
                dma((HALVES, chips - 1, 2, SUBS)),
            ],
            compiler_params=pltpu.CompilerParams(
                collective_id=0, has_side_effects=True, vmem_limit_bytes=45 * 1024 * 1024
            ),
        )(hidden, w_query, w_key, w_value, w_out, k_cache, v_cache, lengths, inv_freq[None, :])
        y, k_out, v_out = pl.pallas_call(
            write_kernel,
            out_shape=tuple(jax.ShapeDtypeStruct(a.shape, BF16) for a in (y, k_vmem, v_vmem)),
            in_specs=[vmem_spec] * 3,
            out_specs=(hbm_spec,) * 3,
            scratch_shapes=[dma((1 + 2 * WRITES,))],
            compiler_params=pltpu.CompilerParams(vmem_limit_bytes=1024 * 1024),
        )(y, k_vmem, v_vmem)
        return y.reshape(batch, cols), k_out, v_out

    return jax.shard_map(
        local_step,
        mesh=mesh,
        in_specs=(P("dp", None), P(None, "tp"), P(), P(), P("tp", None), cache_spec, cache_spec, P("dp")),
        out_specs=(P("dp", "tp"), cache_spec, cache_spec),
        check_vma=False,
    )
```

```python
import functools

import jax
import jax.numpy as jnp
from jax import lax
from jax.experimental import pallas as pl
from jax.experimental.pallas import tpu as pltpu
from jax.sharding import PartitionSpec as P

MESH = pl.DeviceIdType.MESH
HALVES = 2
K_CHUNKS = 8
AHEAD = 6
WRITES = 4
F32 = jnp.float32
BF16 = jnp.bfloat16


def decode_kernel(
    n, hid_hbm, wq_hbm, wk_hbm, wv_hbm, wo_hbm, kc_hbm, vc_hbm, len_hbm, freq_ref,
    y_ref, kc, vc,
    hid, wq, wk, wv, wo, lens, acc, qs, qr, q_lo, q_hi, o_lo, o_hi, s_buf, e_buf, osend, orecv, cos_ref, sin_ref, kf, vf,
    pm, ps, pr, rs, rr,
    sem_len, sem_h, sem_w, sem_k, sem_v, sem_kc, sem_vc, sem_wo,
    q_ssem, q_rsem, o_ssem, o_rsem, p_ssem, p_rsem, r_ssem, r_rsem,
):
    me = lax.axis_index("tp")
    chips = n // 2
    core = lax.rem(me, 2)
    chip = me // 2
    partner = me + 1 - 2 * core
    neighbours = (lax.rem(me + 2, n), lax.rem(me + n - 2, n))

    batch, depth = hid.shape
    cols = wq.shape[1]
    rows = batch // n
    half_rows = rows // HALVES
    seq_len, head_dim = kc.shape[1:]
    half_dim = head_dim // 2
    dev_heads = cols // head_dim
    heads = dev_heads * n
    block = depth // K_CHUNKS
    part = cols // 2
    out_block = wo.shape[1] // 4
    scale = head_dim ** -0.5

    def load_h(i):
        return pltpu.make_async_copy(hid_hbm.at[:, pl.ds(i * block, block)], hid.at[:, pl.ds(i * block, block)], sem_h.at[i])

    def load_rows(hbm, vmem, sem, size, i):
        return pltpu.make_async_copy(hbm.at[pl.ds(i * size, size)], vmem.at[pl.ds(i * size, size)], sem.at[i])

    def load_w(i):
        return load_rows(wq_hbm, wq, sem_w, block, i)

    def load_k(i):
        return load_rows(wk_hbm, wk, sem_k, 2 * block, i)

    def load_v(i):
        return load_rows(wv_hbm, wv, sem_v, 2 * block, i)

    def load_kc(h):
        return load_rows(kc_hbm, kc, sem_kc, half_rows, h)

    def load_vc(h):
        return load_rows(vc_hbm, vc, sem_vc, half_rows, h)

    def load_o(i):
        span = pl.ds(i * out_block, out_block)
        return pltpu.make_async_copy(wo_hbm.at[:, span], wo.at[:, span], sem_wo.at[i])

    len_copy = pltpu.make_async_copy(len_hbm, lens, sem_len.at[0])
    queue = [(load_h(i), load_w(i)) for i in range(K_CHUNKS)]
    queue += [(load_k(i), load_v(i)) for i in range(K_CHUNKS // 2)]
    queue += [(load_kc(h), load_vc(h)) for h in range(HALVES)]
    queue += [(load_o(i),) for i in range(4)]

    def issue(count):
        for _ in range(count):
            if queue:
                for copy in queue.pop(0):
                    copy.start()

    len_copy.start()
    issue(AHEAD)

    barrier = pltpu.get_barrier_semaphore()
    order = sorted(range(1, n), key=lambda i: (min(i, n - i), i), reverse=True)
    for i in order:
        pl.semaphore_signal(barrier, inc=1, device_id={"tp": lax.rem(me + i, n)}, device_id_type=MESH)

    with jax.named_scope("angles"):
        len_copy.wait()
        for r in range(rows):
            cos_ref[pl.ds(r, 1), :] = lens[me * rows + r].astype(F32) * freq_ref[...]
        angles = cos_ref[...]
        sin_ref[...] = jnp.sin(angles)
        cos_ref[...] = jnp.cos(angles)

    with jax.named_scope("q_mm"):
        for i in range(K_CHUNKS):
            load_h(i).wait()
            load_w(i).wait()
            issue(1)
            span = pl.ds(i * block, block)
            term = jnp.dot(hid[:, span], wq[span, :], preferred_element_type=F32)
            if i == 0:
                acc[...] = term
            elif i < K_CHUNKS - 1:
                acc[...] += term
            else:
                q_all = (acc[...] + term).reshape(n, HALVES, half_rows, cols)
                for h in range(HALVES):
                    qs[h] = q_all[:, h].astype(BF16)

    with jax.named_scope("barrier"):
        pl.semaphore_wait(barrier, n - 1)

    def exchange(src, dst, send_sem, recv_sem, h):
        for i in order:
            peer = lax.rem(me + i, n)
            pltpu.make_async_remote_copy(
                src_ref=src.at[h, peer],
                dst_ref=dst.at[h, me],
                send_sem=send_sem.at[h],
                recv_sem=recv_sem.at[h],
                device_id={"tp": peer},
                device_id_type=MESH,
            ).start()
        dst[h, me] = src[h, me]

    def exchange_wait(buf, sem, h):
        others = buf.at[h, pl.ds(0, n - 1)]
        pltpu.make_async_copy(others, others, sem.at[h]).wait()

    with jax.named_scope("q_send"):
        for h in range(HALVES):
            exchange(qs, qr, q_ssem, q_rsem, h)

    own = pl.ds(pl.multiple_of(me * rows, rows), rows)
    k_sum = jnp.zeros((rows, head_dim), F32)
    v_sum = jnp.zeros((rows, head_dim), F32)
    for i in range(K_CHUNKS // 2):
        with jax.named_scope(f"kv_wait{i}"):
            load_k(i).wait()
            load_v(i).wait()
        issue(1)
        span = pl.ds(i * 2 * block, 2 * block)
        h_own = hid[own, span]
        k_sum += jnp.dot(h_own, wk[span, :], preferred_element_type=F32)
        v_sum += jnp.dot(h_own, wv[span, :], preferred_element_type=F32)
    k_full = k_sum.astype(BF16).astype(F32)
    cosines, sines = cos_ref[...], sin_ref[...]
    k_lo, k_hi = k_full[:, :half_dim], k_full[:, half_dim:]
    k_rot = jnp.concatenate([k_lo * cosines - k_hi * sines, k_hi * cosines + k_lo * sines], axis=-1)
    kf[...] = k_rot.astype(BF16).astype(F32)
    vf[...] = v_sum.astype(BF16).astype(F32)
    issue(len(queue))

    slots = lax.broadcasted_iota(jnp.int32, (heads, seq_len), 1)

    def attend(h):
        with jax.named_scope(f"q_wait{h}"):
            exchange_wait(qr, q_rsem, h)
        with jax.named_scope(f"rope{h}"):
            span = pl.ds(h * half_rows, half_rows)
            cosines, sines = cos_ref[span, :], sin_ref[span, :]
            for src in range(n):
                for j in range(dev_heads):
                    x = qr[h, src, :, pl.ds(j * head_dim, head_dim)].astype(F32)
                    lo, hi = x[:, :half_dim], x[:, half_dim:]
                    place = pl.ds(src * dev_heads + j, half_rows, stride=heads)
                    q_lo[place, :] = lo * cosines - hi * sines
                    q_hi[place, :] = hi * cosines + lo * sines
        with jax.named_scope(f"cache_wait{h}"):
            load_kc(h).wait()
            load_vc(h).wait()
        with jax.named_scope(f"rows{h}"):
            ats = [pl.ds(r * heads, heads) for r in range(half_rows)]
            news = []
            for r, at in enumerate(ats):
                b = h * half_rows + r
                q = jnp.concatenate([q_lo[at, :], q_hi[at, :]], axis=-1).astype(BF16)
                s_buf[at, :] = lax.dot_general(q, kc[b], (((1,), (1,)), ((), ())), preferred_element_type=F32)
                news.append(jnp.sum(q.astype(F32) * kf[pl.ds(b, 1), :], axis=-1, keepdims=True) * scale)
            sums = []
            for r, at in enumerate(ats):
                length = lens[me * rows + h * half_rows + r]
                s = jnp.where(slots < length, s_buf[at, :] * scale, -1e30)
                top = jnp.maximum(jnp.max(s, axis=-1, keepdims=True), news[r])
                e = jnp.where(slots < length, jnp.exp(s - top), 0.0)
                e_new = jnp.exp(news[r] - top)
                e_buf[at, :] = e.astype(BF16)
                sums.append((e_new, jnp.sum(e, axis=-1, keepdims=True) + e_new))
            for r, at in enumerate(ats):
                b = h * half_rows + r
                e_new, total = sums[r]
                o = jnp.dot(e_buf[at, :], vc[b], preferred_element_type=F32)
                o = (o + e_new.astype(BF16).astype(F32) * vf[pl.ds(b, 1), :]) / total
                o_lo[at, :] = o[:, :half_dim]
                o_hi[at, :] = o[:, half_dim:]
        with jax.named_scope(f"opack{h}"):
            for dst in range(n):
                for j in range(dev_heads):
                    place = pl.ds(dst * dev_heads + j, half_rows, stride=heads)
                    osend[h, dst, :, pl.ds(j * head_dim, half_dim)] = o_lo[place, :].astype(BF16)
                    osend[h, dst, :, pl.ds(j * head_dim + half_dim, half_dim)] = o_hi[place, :].astype(BF16)
        with jax.named_scope(f"o_send{h}"):
            exchange(osend, orecv, o_ssem, o_rsem, h)

    for h in range(HALVES):
        attend(h)

    arm = chips // 2

    def partner_copy(h, j):
        return pltpu.make_async_remote_copy(
            src_ref=ps.at[h, j], dst_ref=pr.at[h, j], send_sem=p_ssem.at[h], recv_sem=p_rsem.at[h, j],
            device_id={"tp": partner}, device_id_type=MESH,
        )

    def multiply(h, j):
        o_cols = orecv[h].reshape(n * half_rows, cols)
        shift = (1 - 2 * lax.rem(j + 1, 2)) * (arm - (j + 1) // 2)
        base = lax.rem(chip + shift + chips, chips) * 2

        def product(side):
            first = pl.multiple_of((base + side) * cols, cols)
            return jnp.dot(o_cols, wo[:, pl.ds(first, cols)], preferred_element_type=F32)

        ahead = product(1 - core).astype(BF16)
        for half in range(2):
            ps[h, j, half] = ahead[:, half * part : (half + 1) * part]
        partner_copy(h, j).start()
        kept = product(core)
        for half in range(2):
            pm[h, j, half] = kept[:, half * part : (half + 1) * part]

    def multiplies(h, lo, hi):
        def body(j, carry):
            multiply(h, j)
            return carry

        with jax.named_scope(f"mult{h}_{lo}"):
            lax.fori_loop(lo, hi, body, 0)

    def ring_copy(h, way, slot):
        return pltpu.make_async_remote_copy(
            src_ref=rs.at[h, way, slot], dst_ref=rr.at[h, way, slot],
            send_sem=r_ssem.at[h], recv_sem=r_rsem.at[h, way, slot],
            device_id={"tp": neighbours[way]}, device_id_type=MESH,
        )

    met = set()

    def chip_sum(h, j, half):
        if (h, j) not in met:
            met.add((h, j))
            with jax.named_scope(f"pw{h}_{j}"):
                partner_copy(h, j).wait_recv()
        return pm[h, j, half] + pr[h, j, half].astype(F32)

    def arrived(h, way, slot):
        with jax.named_scope(f"rw{h}_{way}_{slot}"):
            ring_copy(h, way, slot).wait_recv()
        return rr[h, way, slot].astype(F32)

    def pass_on(h, way, long, step):
        hops = (arm if long else arm - 1) - step
        slot = step if long else arm + step
        half = way if long else 1 - way
        value = chip_sum(h, 0 if hops == arm else 1 + 2 * (arm - 1 - hops) + way, half)
        if step > 0:
            value = value + arrived(h, way, slot - 1)
        rs[h, way, slot] = value.astype(BF16)
        ring_copy(h, way, slot).start()

    def reduce_step(h, step):
        for long in (True, False):
            for way in range(2):
                if step < (arm if long else arm - 1):
                    pass_on(h, way, long, step)

    def finish(h):
        for half in range(2):
            value = chip_sum(h, chips - 1, half) + arrived(h, 1 - half, 2 * arm - 2) + arrived(h, half, arm - 1)
            y_ref[:, h, :, pl.ds(half * part, part)] = value.reshape(n, half_rows, part).astype(BF16)

    row_slots = lax.broadcasted_iota(jnp.int32, (seq_len, head_dim), 0)

    def update(b):
        with jax.named_scope(f"update{b}"):
            length = lens[me * rows + b]
            for cache, new in ((kc, kf), (vc, vf)):
                row = jnp.broadcast_to(new[pl.ds(b, 1), :].astype(BF16), (seq_len, head_dim))
                cache[b] = jnp.where(row_slots == length, row, cache[b])

    with jax.named_scope("wo_wait"):
        for i in range(4):
            load_o(i).wait()
    pending = list(range(rows))

    def updates(count):
        for _ in range(count):
            if pending:
                update(pending.pop(0))

    for h in range(HALVES):
        with jax.named_scope(f"o_wait{h}"):
            exchange_wait(orecv, o_rsem, h)
        multiplies(h, 0, 1)
        multiplies(h, 1, 3)
        reduce_step(h, 0)
        if h == 0:
            multiplies(h, 3, chips)
    reduce_step(0, 1)
    for h in range(1, HALVES):
        multiplies(h, 3, chips)
        reduce_step(h, 1)
        updates(3)
    for step in range(2, arm):
        for h in range(HALVES):
            reduce_step(h, step)
            updates(4)
    updates(rows)
    for h in range(HALVES):
        finish(h)

    with jax.named_scope("tail"):
        for h in range(HALVES):
            exchange_wait(qs, q_ssem, h)
            exchange_wait(osend, o_ssem, h)
            pltpu.make_async_copy(ps.at[h], ps.at[h], p_ssem.at[h]).wait()
            pltpu.make_async_copy(rs.at[h], rs.at[h], r_ssem.at[h]).wait()


def write_kernel(y, kc, vc, y_out, k_out, v_out, sem):
    rows = kc.shape[0] // WRITES
    copies = [pltpu.make_async_copy(y, y_out, sem.at[0])]
    for i in range(WRITES):
        span = pl.ds(i * rows, rows)
        copies.append(pltpu.make_async_copy(kc.at[span], k_out.at[span], sem.at[1 + 2 * i]))
        copies.append(pltpu.make_async_copy(vc.at[span], v_out.at[span], sem.at[2 + 2 * i]))
    for copy in copies:
        copy.start()
    for copy in copies:
        copy.wait()


def solution(mesh):
    n = mesh.shape["tp"]
    cache_spec = P(("dp", "tp"), None, None)

    def local_step(hidden, w_query, w_key, w_value, w_out, k_cache, v_cache, lengths):
        rows, seq_len, head_dim = k_cache.shape
        batch, depth = hidden.shape
        cols = w_query.shape[1]
        half_rows = rows // HALVES
        chips = n // 2
        heads = cols * n // head_dim
        half_dim = head_dim // 2
        inv_freq = 10000.0 ** (-(jnp.arange(half_dim, dtype=F32) * 2.0) / head_dim)
        hbm_spec = pl.BlockSpec(memory_space=pltpu.HBM)
        vmem_spec = pl.BlockSpec(memory_space=pltpu.VMEM)
        dma = pltpu.SemaphoreType.DMA
        piece = (n * half_rows, cols // 2)
        y, k_vmem, v_vmem = pl.pallas_call(
            functools.partial(decode_kernel, n),
            out_shape=(
                jax.ShapeDtypeStruct((n, HALVES, half_rows, cols), BF16),
                jax.ShapeDtypeStruct(k_cache.shape, BF16),
                jax.ShapeDtypeStruct(v_cache.shape, BF16),
            ),
            in_specs=[hbm_spec] * 8 + [vmem_spec],
            out_specs=(vmem_spec, vmem_spec, vmem_spec),
            scratch_shapes=[
                pltpu.VMEM((batch, depth), BF16),
                pltpu.VMEM((depth, cols), BF16),
                pltpu.VMEM((depth, head_dim), BF16),
                pltpu.VMEM((depth, head_dim), BF16),
                pltpu.VMEM(w_out.shape, BF16),
                pltpu.SMEM((batch,), jnp.int32),
                pltpu.VMEM((batch, cols), F32),
                pltpu.VMEM((HALVES, n, half_rows, cols), BF16),
                pltpu.VMEM((HALVES, n, half_rows, cols), BF16),
                pltpu.VMEM((half_rows * heads, half_dim), F32),
                pltpu.VMEM((half_rows * heads, half_dim), F32),
                pltpu.VMEM((half_rows * heads, half_dim), F32),
                pltpu.VMEM((half_rows * heads, half_dim), F32),
                pltpu.VMEM((half_rows * heads, seq_len), F32),
                pltpu.VMEM((half_rows * heads, seq_len), BF16),
                pltpu.VMEM((HALVES, n, half_rows, cols), BF16),
                pltpu.VMEM((HALVES, n, half_rows, cols), BF16),
                pltpu.VMEM((rows, half_dim), F32),
                pltpu.VMEM((rows, half_dim), F32),
                pltpu.VMEM((rows, head_dim), F32),
                pltpu.VMEM((rows, head_dim), F32),
                pltpu.VMEM((HALVES, chips, 2) + piece, F32),
                pltpu.VMEM((HALVES, chips, 2) + piece, BF16),
                pltpu.VMEM((HALVES, chips, 2) + piece, BF16),
                pltpu.VMEM((HALVES, 2, chips - 1) + piece, BF16),
                pltpu.VMEM((HALVES, 2, chips - 1) + piece, BF16),
                dma((1,)),
                dma((K_CHUNKS,)),
                dma((K_CHUNKS,)),
                dma((K_CHUNKS // 2,)),
                dma((K_CHUNKS // 2,)),
                dma((HALVES,)),
                dma((HALVES,)),
                dma((4,)),
                dma((HALVES,)),
                dma((HALVES,)),
                dma((HALVES,)),
                dma((HALVES,)),
                dma((HALVES,)),
                dma((HALVES, chips)),
                dma((HALVES,)),
                dma((HALVES, 2, chips - 1)),
            ],
            compiler_params=pltpu.CompilerParams(
                collective_id=0, has_side_effects=True, vmem_limit_bytes=45 * 1024 * 1024
            ),
        )(hidden, w_query, w_key, w_value, w_out, k_cache, v_cache, lengths, inv_freq[None, :])
        y, k_out, v_out = pl.pallas_call(
            write_kernel,
            out_shape=tuple(jax.ShapeDtypeStruct(a.shape, BF16) for a in (y, k_vmem, v_vmem)),
            in_specs=[vmem_spec] * 3,
            out_specs=(hbm_spec,) * 3,
            scratch_shapes=[dma((1 + 2 * WRITES,))],
            compiler_params=pltpu.CompilerParams(vmem_limit_bytes=1024 * 1024),
        )(y, k_vmem, v_vmem)
        return y.reshape(batch, cols), k_out, v_out

    return jax.shard_map(
        local_step,
        mesh=mesh,
        in_specs=(P("dp", None), P(None, "tp"), P(), P(), P("tp", None), cache_spec, cache_spec, P("dp")),
        out_specs=(P("dp", "tp"), cache_spec, cache_spec),
        check_vma=False,
    )
```

```python
import functools

import jax
import jax.numpy as jnp
from jax import lax
from jax.experimental import pallas as pl
from jax.experimental.pallas import tpu as pltpu
from jax.sharding import PartitionSpec as P

MESH = pl.DeviceIdType.MESH
HALVES = 2
K_CHUNKS = 8
AHEAD = 6
WRITES = 4
F32 = jnp.float32
BF16 = jnp.bfloat16


def decode_kernel(
    n, hid_hbm, wq_hbm, wk_hbm, wv_hbm, wo_hbm, kc_hbm, vc_hbm, len_hbm, freq_ref,
    y_ref, kc, vc,
    hid, wq, wk, wv, wo, lens, acc, qs, qr, q_lo, q_hi, o_lo, o_hi, s_buf, e_buf, osend, orecv, oc, cos_ref, sin_ref, kf, vf,
    pm, ps, pr, rs, rr,
    sem_len, sem_q, sem_kv, sem_cache, sem_wo,
    q_ssem, q_rsem, o_ssem, o_rsem, p_ssem, p_rsem, r_ssem, r_rsem,
):
    me = lax.axis_index("tp")
    chips = n // 2
    core = lax.rem(me, 2)
    chip = me // 2
    partner = me + 1 - 2 * core
    neighbours = (lax.rem(me + 2, n), lax.rem(me + n - 2, n))

    batch, depth = hid.shape
    cols = wq.shape[1]
    rows = batch // n
    half_rows = rows // HALVES
    seq_len, head_dim = kc.shape[1:]
    half_dim = head_dim // 2
    dev_heads = cols // head_dim
    heads = dev_heads * n
    block = depth // K_CHUNKS
    part = cols // 2
    out_block = wo.shape[1] // 4
    scale = head_dim ** -0.5

    def rows_of(hbm, vmem, sem, size, i):
        return pltpu.make_async_copy(hbm.at[pl.ds(i * size, size)], vmem.at[pl.ds(i * size, size)], sem)

    def columns_of(hbm, vmem, sem, size, i):
        return pltpu.make_async_copy(hbm.at[:, pl.ds(i * size, size)], vmem.at[:, pl.ds(i * size, size)], sem)

    def wait_for(buf, sem):
        pltpu.make_async_copy(buf, buf, sem).wait()

    len_copy = pltpu.make_async_copy(len_hbm, lens, sem_len.at[0])
    pair = 2 * block
    queue = [
        (columns_of(hid_hbm, hid, sem_q.at[i], block, i), rows_of(wq_hbm, wq, sem_q.at[i], block, i))
        for i in range(K_CHUNKS)
    ]
    queue += [
        (rows_of(wk_hbm, wk, sem_kv.at[i], pair, i), rows_of(wv_hbm, wv, sem_kv.at[i], pair, i))
        for i in range(K_CHUNKS // 2)
    ]
    queue += [
        (rows_of(kc_hbm, kc, sem_cache.at[h], half_rows, h), rows_of(vc_hbm, vc, sem_cache.at[h], half_rows, h))
        for h in range(HALVES)
    ]
    queue += [(columns_of(wo_hbm, wo, sem_wo.at[0], out_block, i),) for i in range(4)]
    q_rows = block + block * batch // cols

    def issue(count):
        for _ in range(count):
            if queue:
                for copy in queue.pop(0):
                    copy.start()

    len_copy.start()
    issue(AHEAD)

    barrier = pltpu.get_barrier_semaphore()
    order = sorted(range(1, n), key=lambda i: (min(i, n - i), i), reverse=True)
    for i in order:
        pl.semaphore_signal(barrier, inc=1, device_id={"tp": lax.rem(me + i, n)}, device_id_type=MESH)

    with jax.named_scope("angles"):
        len_copy.wait()
        for r in range(rows):
            cos_ref[pl.ds(r, 1), :] = lens[me * rows + r].astype(F32) * freq_ref[...]
        angles = cos_ref[...]
        sin_ref[...] = jnp.sin(angles)
        cos_ref[...] = jnp.cos(angles)

    with jax.named_scope("q_mm"):
        for i in range(K_CHUNKS):
            wait_for(wq.at[pl.ds(0, q_rows)], sem_q.at[i])
            issue(1)
            span = pl.ds(i * block, block)
            term = jnp.dot(hid[:, span], wq[span, :], preferred_element_type=F32)
            if i == 0:
                acc[...] = term
            elif i < K_CHUNKS - 1:
                acc[...] += term
            else:
                q_all = (acc[...] + term).reshape(n, HALVES, half_rows, cols)
                for h in range(HALVES):
                    qs[h] = q_all[:, h].astype(BF16)

    with jax.named_scope("barrier"):
        pl.semaphore_wait(barrier, n - 1)

    def exchange(src, dst, send_sem, recv_sem, h):
        for i in order:
            peer = lax.rem(me + i, n)
            pltpu.make_async_remote_copy(
                src_ref=src.at[h, peer],
                dst_ref=dst.at[h, me],
                send_sem=send_sem.at[0],
                recv_sem=recv_sem.at[h],
                device_id={"tp": peer},
                device_id_type=MESH,
            ).start()
        dst[h, me] = src[h, me]

    def exchange_wait(buf, sem, h):
        wait_for(buf.at[h, pl.ds(0, n - 1)], sem.at[h])

    with jax.named_scope("q_send"):
        exchange(qs, qr, q_ssem, q_rsem, 0)

    own = pl.ds(pl.multiple_of(me * rows, rows), rows)
    k_sum = jnp.zeros((rows, head_dim), F32)
    v_sum = jnp.zeros((rows, head_dim), F32)
    for i in range(K_CHUNKS // 2):
        with jax.named_scope(f"kv_wait{i}"):
            wait_for(wk.at[pl.ds(0, 2 * pair)], sem_kv.at[i])
        issue(1)
        span = pl.ds(i * 2 * block, 2 * block)
        h_own = hid[own, span]
        k_sum += jnp.dot(h_own, wk[span, :], preferred_element_type=F32)
        v_sum += jnp.dot(h_own, wv[span, :], preferred_element_type=F32)
    k_full = k_sum.astype(BF16).astype(F32)
    cosines, sines = cos_ref[...], sin_ref[...]
    k_lo, k_hi = k_full[:, :half_dim], k_full[:, half_dim:]
    k_rot = jnp.concatenate([k_lo * cosines - k_hi * sines, k_hi * cosines + k_lo * sines], axis=-1)
    kf[...] = k_rot.astype(BF16).astype(F32)
    vf[...] = v_sum.astype(BF16).astype(F32)
    issue(len(queue))
    with jax.named_scope("q_send1"):
        for h in range(1, HALVES):
            exchange(qs, qr, q_ssem, q_rsem, h)

    slots = lax.broadcasted_iota(jnp.int32, (heads, seq_len), 1)

    def attend(h):
        with jax.named_scope(f"q_wait{h}"):
            exchange_wait(qr, q_rsem, h)
        with jax.named_scope(f"rope{h}"):
            span = pl.ds(h * half_rows, half_rows)
            cosines, sines = cos_ref[span, :], sin_ref[span, :]
            for src in range(n):
                for j in range(dev_heads):
                    x = qr[h, src, :, pl.ds(j * head_dim, head_dim)].astype(F32)
                    lo, hi = x[:, :half_dim], x[:, half_dim:]
                    place = pl.ds(src * dev_heads + j, half_rows, stride=heads)
                    q_lo[place, :] = lo * cosines - hi * sines
                    q_hi[place, :] = hi * cosines + lo * sines
        with jax.named_scope(f"cache_wait{h}"):
            wait_for(kc.at[pl.ds(0, 2 * half_rows)], sem_cache.at[h])
        with jax.named_scope(f"rows{h}"):
            ats = [pl.ds(r * heads, heads) for r in range(half_rows)]
            news = []
            for r, at in enumerate(ats):
                b = h * half_rows + r
                q = jnp.concatenate([q_lo[at, :], q_hi[at, :]], axis=-1).astype(BF16)
                s_buf[at, :] = lax.dot_general(q, kc[b], (((1,), (1,)), ((), ())), preferred_element_type=F32)
                news.append(jnp.sum(q.astype(F32) * kf[pl.ds(b, 1), :], axis=-1, keepdims=True) * scale)
            sums = []
            for r, at in enumerate(ats):
                length = lens[me * rows + h * half_rows + r]
                s = jnp.where(slots < length, s_buf[at, :] * scale, -1e30)
                top = jnp.maximum(jnp.max(s, axis=-1, keepdims=True), news[r])
                e = jnp.where(slots < length, jnp.exp(s - top), 0.0)
                e_new = jnp.exp(news[r] - top)
                e_buf[at, :] = e.astype(BF16)
                sums.append((e_new, jnp.sum(e, axis=-1, keepdims=True) + e_new))
            for r, at in enumerate(ats):
                b = h * half_rows + r
                e_new, total = sums[r]
                o = jnp.dot(e_buf[at, :], vc[b], preferred_element_type=F32)
                o = (o + e_new.astype(BF16).astype(F32) * vf[pl.ds(b, 1), :]) / total
                o_lo[at, :] = o[:, :half_dim]
                o_hi[at, :] = o[:, half_dim:]
        with jax.named_scope(f"opack{h}"):
            for dst in range(n):
                for j in range(dev_heads):
                    place = pl.ds(dst * dev_heads + j, half_rows, stride=heads)
                    osend[h, dst, :, pl.ds(j * head_dim, half_dim)] = o_lo[place, :].astype(BF16)
                    osend[h, dst, :, pl.ds(j * head_dim + half_dim, half_dim)] = o_hi[place, :].astype(BF16)
        with jax.named_scope(f"o_send{h}"):
            exchange(osend, orecv, o_ssem, o_rsem, h)

    for h in range(HALVES):
        attend(h)

    arm = chips // 2

    ahead = 3

    def partner_copy(h, j):
        return pltpu.make_async_remote_copy(
            src_ref=ps.at[h, j], dst_ref=pr.at[h, j], send_sem=p_ssem.at[0], recv_sem=p_rsem.at[h, min(j, ahead)],
            device_id={"tp": partner}, device_id_type=MESH,
        )

    def multiplies(h, lo, hi):
        with jax.named_scope(f"mult{h}_{lo}"):
            o_cols = oc[h]
            for j in range(lo, hi):
                shift = (1 - 2 * ((j + 1) % 2)) * (arm - (j + 1) // 2)
                base = lax.rem(chip + (shift + chips), chips) * 2

                def product(side):
                    first = pl.multiple_of((base + side) * cols, cols)
                    return jnp.dot(o_cols, wo[:, pl.ds(first, cols)], preferred_element_type=F32)

                other = product(1 - core).astype(BF16)
                for half in range(2):
                    ps[h, j, half] = other[:, half * part : (half + 1) * part]
                kept = product(core)
                for half in range(2):
                    pm[h, j, half] = kept[:, half * part : (half + 1) * part]
            for j in range(lo, hi):
                partner_copy(h, j).start()

    def ring_copy(h, way, slot):
        return pltpu.make_async_remote_copy(
            src_ref=rs.at[h, way, slot], dst_ref=rr.at[h, way, slot],
            send_sem=r_ssem.at[0], recv_sem=r_rsem.at[h, way, slot],
            device_id={"tp": neighbours[way]}, device_id_type=MESH,
        )

    met = set()

    def chip_sum(h, j, half):
        if (h, min(j, ahead)) not in met:
            met.add((h, min(j, ahead)))
            with jax.named_scope(f"pw{h}_{j}"):
                if j < ahead:
                    partner_copy(h, j).wait_recv()
                else:
                    wait_for(pr.at[h, pl.ds(ahead, chips - ahead)], p_rsem.at[h, ahead])
        return pm[h, j, half] + pr[h, j, half].astype(F32)

    def arrived(h, way, slot):
        with jax.named_scope(f"rw{h}_{way}_{slot}"):
            ring_copy(h, way, slot).wait_recv()
        return rr[h, way, slot].astype(F32)

    def pass_on(h, way, long, step):
        hops = (arm if long else arm - 1) - step
        slot = step if long else arm + step
        half = way if long else 1 - way
        value = chip_sum(h, 0 if hops == arm else 1 + 2 * (arm - 1 - hops) + way, half)
        if step > 0:
            value = value + arrived(h, way, slot - 1)
        rs[h, way, slot] = value.astype(BF16)
        ring_copy(h, way, slot).start()

    def reduce_step(h, step):
        for long in (True, False):
            for way in range(2):
                if step < (arm if long else arm - 1):
                    pass_on(h, way, long, step)

    def finish(h):
        for half in range(2):
            value = chip_sum(h, chips - 1, half) + arrived(h, 1 - half, 2 * arm - 2) + arrived(h, half, arm - 1)
            y_ref[:, h, :, pl.ds(half * part, part)] = value.reshape(n, half_rows, part).astype(BF16)

    row_slots = lax.broadcasted_iota(jnp.int32, (seq_len, head_dim), 0)

    def update(b):
        with jax.named_scope(f"update{b}"):
            length = lens[me * rows + b]
            for cache, new in ((kc, kf), (vc, vf)):
                row = jnp.broadcast_to(new[pl.ds(b, 1), :].astype(BF16), (seq_len, head_dim))
                cache[b] = jnp.where(row_slots == length, row, cache[b])

    with jax.named_scope("wo_wait"):
        wait_for(wo, sem_wo.at[0])
    pending = list(range(rows))

    def updates(count):
        for _ in range(count):
            if pending:
                update(pending.pop(0))

    for h in range(HALVES):
        with jax.named_scope(f"o_wait{h}"):
            exchange_wait(orecv, o_rsem, h)
        oc[h] = orecv[h].reshape(n * half_rows, cols)
        multiplies(h, 0, ahead)
        reduce_step(h, 0)
        if h == 0:
            multiplies(h, ahead, chips)
    reduce_step(0, 1)
    for h in range(1, HALVES):
        multiplies(h, ahead, chips)
        reduce_step(h, 1)
        updates(3)
    for step in range(2, arm):
        for h in range(HALVES):
            reduce_step(h, step)
            updates(4)
    updates(rows)
    for h in range(HALVES):
        finish(h)

    with jax.named_scope("tail"):
        wait_for(qs.at[:, pl.ds(0, n - 1)], q_ssem.at[0])
        wait_for(osend.at[:, pl.ds(0, n - 1)], o_ssem.at[0])
        wait_for(ps, p_ssem.at[0])
        wait_for(rs, r_ssem.at[0])


def write_kernel(y, kc, vc, y_out, k_out, v_out, sem):
    rows = kc.shape[0] // WRITES
    copies = [pltpu.make_async_copy(y, y_out, sem.at[0])]
    for i in range(WRITES):
        span = pl.ds(i * rows, rows)
        copies.append(pltpu.make_async_copy(kc.at[span], k_out.at[span], sem.at[1 + 2 * i]))
        copies.append(pltpu.make_async_copy(vc.at[span], v_out.at[span], sem.at[2 + 2 * i]))
    for copy in copies:
        copy.start()
    for copy in copies:
        copy.wait()


def solution(mesh):
    n = mesh.shape["tp"]
    cache_spec = P(("dp", "tp"), None, None)

    def local_step(hidden, w_query, w_key, w_value, w_out, k_cache, v_cache, lengths):
        rows, seq_len, head_dim = k_cache.shape
        batch, depth = hidden.shape
        cols = w_query.shape[1]
        half_rows = rows // HALVES
        chips = n // 2
        heads = cols * n // head_dim
        half_dim = head_dim // 2
        inv_freq = 10000.0 ** (-(jnp.arange(half_dim, dtype=F32) * 2.0) / head_dim)
        hbm_spec = pl.BlockSpec(memory_space=pltpu.HBM)
        vmem_spec = pl.BlockSpec(memory_space=pltpu.VMEM)
        dma = pltpu.SemaphoreType.DMA
        piece = (n * half_rows, cols // 2)
        y, k_vmem, v_vmem = pl.pallas_call(
            functools.partial(decode_kernel, n),
            out_shape=(
                jax.ShapeDtypeStruct((n, HALVES, half_rows, cols), BF16),
                jax.ShapeDtypeStruct(k_cache.shape, BF16),
                jax.ShapeDtypeStruct(v_cache.shape, BF16),
            ),
            in_specs=[hbm_spec] * 8 + [vmem_spec],
            out_specs=(vmem_spec, vmem_spec, vmem_spec),
            scratch_shapes=[
                pltpu.VMEM((batch, depth), BF16),
                pltpu.VMEM((depth, cols), BF16),
                pltpu.VMEM((depth, head_dim), BF16),
                pltpu.VMEM((depth, head_dim), BF16),
                pltpu.VMEM(w_out.shape, BF16),
                pltpu.SMEM((batch,), jnp.int32),
                pltpu.VMEM((batch, cols), F32),
                pltpu.VMEM((HALVES, n, half_rows, cols), BF16),
                pltpu.VMEM((HALVES, n, half_rows, cols), BF16),
                pltpu.VMEM((half_rows * heads, half_dim), F32),
                pltpu.VMEM((half_rows * heads, half_dim), F32),
                pltpu.VMEM((half_rows * heads, half_dim), F32),
                pltpu.VMEM((half_rows * heads, half_dim), F32),
                pltpu.VMEM((half_rows * heads, seq_len), F32),
                pltpu.VMEM((half_rows * heads, seq_len), BF16),
                pltpu.VMEM((HALVES, n, half_rows, cols), BF16),
                pltpu.VMEM((HALVES, n, half_rows, cols), BF16),
                pltpu.VMEM((HALVES, n * half_rows, cols), BF16),
                pltpu.VMEM((rows, half_dim), F32),
                pltpu.VMEM((rows, half_dim), F32),
                pltpu.VMEM((rows, head_dim), F32),
                pltpu.VMEM((rows, head_dim), F32),
                pltpu.VMEM((HALVES, chips, 2) + piece, F32),
                pltpu.VMEM((HALVES, chips, 2) + piece, BF16),
                pltpu.VMEM((HALVES, chips, 2) + piece, BF16),
                pltpu.VMEM((HALVES, 2, chips - 1) + piece, BF16),
                pltpu.VMEM((HALVES, 2, chips - 1) + piece, BF16),
                dma((1,)),
                dma((K_CHUNKS,)),
                dma((K_CHUNKS // 2,)),
                dma((HALVES,)),
                dma((1,)),
                dma((1,)),
                dma((HALVES,)),
                dma((1,)),
                dma((HALVES,)),
                dma((1,)),
                dma((HALVES, 4)),
                dma((1,)),
                dma((HALVES, 2, chips - 1)),
            ],
            compiler_params=pltpu.CompilerParams(
                collective_id=0, has_side_effects=True, vmem_limit_bytes=45 * 1024 * 1024
            ),
        )(hidden, w_query, w_key, w_value, w_out, k_cache, v_cache, pltpu.with_memory_space_constraint(lengths, pltpu.HBM), inv_freq[None, :])
        y, k_out, v_out = pl.pallas_call(
            write_kernel,
            out_shape=tuple(jax.ShapeDtypeStruct(a.shape, BF16) for a in (y, k_vmem, v_vmem)),
            in_specs=[vmem_spec] * 3,
            out_specs=(hbm_spec,) * 3,
            scratch_shapes=[dma((1 + 2 * WRITES,))],
            compiler_params=pltpu.CompilerParams(vmem_limit_bytes=1024 * 1024),
        )(y, k_vmem, v_vmem)
        return y.reshape(batch, cols), k_out, v_out

    return jax.shard_map(
        local_step,
        mesh=mesh,
        in_specs=(P("dp", None), P(None, "tp"), P(), P(), P("tp", None), cache_spec, cache_spec, P("dp")),
        out_specs=(P("dp", "tp"), cache_spec, cache_spec),
        check_vma=False,
    )
```

```python
import functools

import jax
import jax.numpy as jnp
from jax import lax
from jax.experimental import pallas as pl
from jax.experimental.pallas import tpu as pltpu
from jax.sharding import PartitionSpec as P

MESH = pl.DeviceIdType.MESH
HALVES = 2
K_CHUNKS = 8
AHEAD = 6
WRITES = 4
F32 = jnp.float32
BF16 = jnp.bfloat16


def decode_kernel(
    n, hid_hbm, wq_hbm, wk_hbm, wv_hbm, wo_hbm, kc_hbm, vc_hbm, len_hbm, freq_ref,
    y_ref, kc, vc,
    hid, wq, wk, wv, wo, lens, acc, qs, qr, q_lo, q_hi, o_lo, o_hi, s_buf, e_buf, osend, orecv, oc, cos_ref, sin_ref, kf, vf,
    pm, ps, pr, rs, rr,
    sem_len, sem_q, sem_kv, sem_cache, sem_wo,
    q_ssem, q_rsem, o_ssem, o_rsem, p_ssem, p_rsem, r_ssem, r_rsem,
):
    me = lax.axis_index("tp")
    chips = n // 2
    core = lax.rem(me, 2)
    chip = me // 2
    partner = me + 1 - 2 * core
    neighbours = (lax.rem(me + 2, n), lax.rem(me + n - 2, n))

    batch, depth = hid.shape
    cols = wq.shape[1]
    rows = batch // n
    half_rows = rows // HALVES
    seq_len, head_dim = kc.shape[1:]
    half_dim = head_dim // 2
    dev_heads = cols // head_dim
    heads = dev_heads * n
    block = depth // K_CHUNKS
    part = cols // 2
    out_block = wo.shape[1] // 4
    scale = head_dim ** -0.5

    def rows_of(hbm, vmem, sem, size, i):
        return pltpu.make_async_copy(hbm.at[pl.ds(i * size, size)], vmem.at[pl.ds(i * size, size)], sem)

    def columns_of(hbm, vmem, sem, size, i):
        return pltpu.make_async_copy(hbm.at[:, pl.ds(i * size, size)], vmem.at[:, pl.ds(i * size, size)], sem)

    def wait_for(buf, sem):
        pltpu.make_async_copy(buf, buf, sem).wait()

    len_copy = pltpu.make_async_copy(len_hbm, lens, sem_len.at[0])
    pair = 2 * block
    queue = [
        (columns_of(hid_hbm, hid, sem_q.at[i], block, i), rows_of(wq_hbm, wq, sem_q.at[i], block, i))
        for i in range(K_CHUNKS)
    ]
    queue += [
        (rows_of(wk_hbm, wk, sem_kv.at[i], pair, i), rows_of(wv_hbm, wv, sem_kv.at[i], pair, i))
        for i in range(K_CHUNKS // 2)
    ]
    queue += [
        (rows_of(kc_hbm, kc, sem_cache.at[h], half_rows, h), rows_of(vc_hbm, vc, sem_cache.at[h], half_rows, h))
        for h in range(HALVES)
    ]
    queue += [(columns_of(wo_hbm, wo, sem_wo.at[0], out_block, i),) for i in range(4)]
    q_rows = block + block * batch // cols

    def issue(count):
        for _ in range(count):
            if queue:
                for copy in queue.pop(0):
                    copy.start()

    len_copy.start()
    issue(AHEAD)

    barrier = pltpu.get_barrier_semaphore()
    order = sorted(range(1, n), key=lambda i: (min(i, n - i), i), reverse=True)
    for i in order:
        pl.semaphore_signal(barrier, inc=1, device_id={"tp": lax.rem(me + i, n)}, device_id_type=MESH)

    with jax.named_scope("q_mm"):
        for i in range(K_CHUNKS):
            wait_for(wq.at[pl.ds(0, q_rows)], sem_q.at[i])
            issue(1)
            span = pl.ds(i * block, block)
            term = jnp.dot(hid[:, span], wq[span, :], preferred_element_type=F32)
            if i == 0:
                acc[...] = term
            elif i < K_CHUNKS - 1:
                acc[...] += term
            else:
                q_all = (acc[...] + term).reshape(n, HALVES, half_rows, cols)
                for h in range(HALVES):
                    qs[h] = q_all[:, h].astype(BF16)

    with jax.named_scope("barrier"):
        pl.semaphore_wait(barrier, n - 1)

    def exchange(src, dst, send_sem, recv_sem, h):
        for i in order:
            peer = lax.rem(me + i, n)
            pltpu.make_async_remote_copy(
                src_ref=src.at[h, peer],
                dst_ref=dst.at[h, me],
                send_sem=send_sem.at[0],
                recv_sem=recv_sem.at[h],
                device_id={"tp": peer},
                device_id_type=MESH,
            ).start()
        dst[h, me] = src[h, me]

    def exchange_wait(buf, sem, h):
        wait_for(buf.at[h, pl.ds(0, n - 1)], sem.at[h])

    with jax.named_scope("q_send"):
        exchange(qs, qr, q_ssem, q_rsem, 0)

    with jax.named_scope("angles"):
        len_copy.wait()
        for r in range(rows):
            cos_ref[pl.ds(r, 1), :] = lens[me * rows + r].astype(F32) * freq_ref[...]
        angles = cos_ref[...]
        sin_ref[...] = jnp.sin(angles)
        cos_ref[...] = jnp.cos(angles)

    own = pl.ds(pl.multiple_of(me * rows, rows), rows)
    k_sum = jnp.zeros((rows, head_dim), F32)
    v_sum = jnp.zeros((rows, head_dim), F32)
    for i in range(K_CHUNKS // 2):
        with jax.named_scope(f"kv_wait{i}"):
            wait_for(wk.at[pl.ds(0, 2 * pair)], sem_kv.at[i])
        issue(1)
        span = pl.ds(i * 2 * block, 2 * block)
        h_own = hid[own, span]
        k_sum += jnp.dot(h_own, wk[span, :], preferred_element_type=F32)
        v_sum += jnp.dot(h_own, wv[span, :], preferred_element_type=F32)
    k_full = k_sum.astype(BF16).astype(F32)
    cosines, sines = cos_ref[...], sin_ref[...]
    k_lo, k_hi = k_full[:, :half_dim], k_full[:, half_dim:]
    k_rot = jnp.concatenate([k_lo * cosines - k_hi * sines, k_hi * cosines + k_lo * sines], axis=-1)
    kf[...] = k_rot.astype(BF16).astype(F32)
    vf[...] = v_sum.astype(BF16).astype(F32)
    issue(len(queue))
    with jax.named_scope("q_send1"):
        for h in range(1, HALVES):
            exchange(qs, qr, q_ssem, q_rsem, h)

    slots = lax.broadcasted_iota(jnp.int32, (heads, seq_len), 1)

    def attend(h):
        with jax.named_scope(f"q_wait{h}"):
            exchange_wait(qr, q_rsem, h)
        with jax.named_scope(f"rope{h}"):
            span = pl.ds(h * half_rows, half_rows)
            cosines, sines = cos_ref[span, :], sin_ref[span, :]
            for src in range(n):
                for j in range(dev_heads):
                    x = qr[h, src, :, pl.ds(j * head_dim, head_dim)].astype(F32)
                    lo, hi = x[:, :half_dim], x[:, half_dim:]
                    place = pl.ds(src * dev_heads + j, half_rows, stride=heads)
                    q_lo[place, :] = lo * cosines - hi * sines
                    q_hi[place, :] = hi * cosines + lo * sines
        with jax.named_scope(f"cache_wait{h}"):
            wait_for(kc.at[pl.ds(0, 2 * half_rows)], sem_cache.at[h])
        with jax.named_scope(f"rows{h}"):
            ats = [pl.ds(r * heads, heads) for r in range(half_rows)]
            news = []
            for r, at in enumerate(ats):
                b = h * half_rows + r
                q = jnp.concatenate([q_lo[at, :], q_hi[at, :]], axis=-1).astype(BF16)
                s_buf[at, :] = lax.dot_general(q, kc[b], (((1,), (1,)), ((), ())), preferred_element_type=F32)
                news.append(jnp.sum(q.astype(F32) * kf[pl.ds(b, 1), :], axis=-1, keepdims=True) * scale)
            sums = []
            for r, at in enumerate(ats):
                length = lens[me * rows + h * half_rows + r]
                s = jnp.where(slots < length, s_buf[at, :] * scale, -1e30)
                top = jnp.maximum(jnp.max(s, axis=-1, keepdims=True), news[r])
                e = jnp.where(slots < length, jnp.exp(s - top), 0.0)
                e_new = jnp.exp(news[r] - top)
                e_buf[at, :] = e.astype(BF16)
                sums.append((e_new, jnp.sum(e, axis=-1, keepdims=True) + e_new))
            for r, at in enumerate(ats):
                b = h * half_rows + r
                e_new, total = sums[r]
                o = jnp.dot(e_buf[at, :], vc[b], preferred_element_type=F32)
                o = (o + e_new.astype(BF16).astype(F32) * vf[pl.ds(b, 1), :]) / total
                o_lo[at, :] = o[:, :half_dim]
                o_hi[at, :] = o[:, half_dim:]
        with jax.named_scope(f"opack{h}"):
            for dst in range(n):
                for j in range(dev_heads):
                    place = pl.ds(dst * dev_heads + j, half_rows, stride=heads)
                    osend[h, dst, :, pl.ds(j * head_dim, half_dim)] = o_lo[place, :].astype(BF16)
                    osend[h, dst, :, pl.ds(j * head_dim + half_dim, half_dim)] = o_hi[place, :].astype(BF16)
        with jax.named_scope(f"o_send{h}"):
            exchange(osend, orecv, o_ssem, o_rsem, h)

    for h in range(HALVES):
        attend(h)

    arm = chips // 2

    ahead = 3

    def partner_copy(h, j):
        return pltpu.make_async_remote_copy(
            src_ref=ps.at[h, j], dst_ref=pr.at[h, j], send_sem=p_ssem.at[0], recv_sem=p_rsem.at[h, min(j, ahead)],
            device_id={"tp": partner}, device_id_type=MESH,
        )

    def multiplies(h, lo, hi):
        with jax.named_scope(f"mult{h}_{lo}"):
            o_cols = oc[h]

            def product(j, side):
                shift = (1 - 2 * ((j + 1) % 2)) * (arm - (j + 1) // 2)
                owner = lax.rem(chip + (shift + chips), chips) * 2 + side
                span = pl.ds(pl.multiple_of(owner * cols, cols), cols)
                return jnp.dot(o_cols, wo[:, span], preferred_element_type=F32)

            for j in range(lo, hi):
                other = product(j, 1 - core).astype(BF16)
                for half in range(2):
                    ps[h, j, half] = other[:, half * part : (half + 1) * part]
                if j == 0:
                    partner_copy(h, j).start()
            for j in range(max(lo, 1), hi):
                partner_copy(h, j).start()
            for j in range(lo, hi):
                kept = product(j, core)
                for half in range(2):
                    pm[h, j, half] = kept[:, half * part : (half + 1) * part]

    def ring_copy(h, way, slot):
        return pltpu.make_async_remote_copy(
            src_ref=rs.at[h, way, slot], dst_ref=rr.at[h, way, slot],
            send_sem=r_ssem.at[0], recv_sem=r_rsem.at[h, way, slot],
            device_id={"tp": neighbours[way]}, device_id_type=MESH,
        )

    met = set()

    def chip_sum(h, j, half):
        if (h, min(j, ahead)) not in met:
            met.add((h, min(j, ahead)))
            with jax.named_scope(f"pw{h}_{j}"):
                if j < ahead:
                    partner_copy(h, j).wait_recv()
                else:
                    wait_for(pr.at[h, pl.ds(ahead, chips - ahead)], p_rsem.at[h, ahead])
        return pm[h, j, half] + pr[h, j, half].astype(F32)

    def arrived(h, way, slot):
        with jax.named_scope(f"rw{h}_{way}_{slot}"):
            ring_copy(h, way, slot).wait_recv()
        return rr[h, way, slot].astype(F32)

    def pass_on(h, way, long, step):
        hops = (arm if long else arm - 1) - step
        slot = step if long else arm + step
        half = way if long else 1 - way
        value = chip_sum(h, 0 if hops == arm else 1 + 2 * (arm - 1 - hops) + way, half)
        if step > 0:
            value = value + arrived(h, way, slot - 1)
        rs[h, way, slot] = value.astype(BF16)
        ring_copy(h, way, slot).start()

    def reduce_step(h, step):
        for long in (True, False):
            for way in range(2):
                if step < (arm if long else arm - 1):
                    pass_on(h, way, long, step)

    def finish(h):
        for half in range(2):
            value = chip_sum(h, chips - 1, half) + arrived(h, 1 - half, 2 * arm - 2) + arrived(h, half, arm - 1)
            y_ref[:, h, :, pl.ds(half * part, part)] = value.reshape(n, half_rows, part).astype(BF16)

    row_slots = lax.broadcasted_iota(jnp.int32, (seq_len, head_dim), 0)

    def update(b):
        with jax.named_scope(f"update{b}"):
            length = lens[me * rows + b]
            for cache, new in ((kc, kf), (vc, vf)):
                row = jnp.broadcast_to(new[pl.ds(b, 1), :].astype(BF16), (seq_len, head_dim))
                cache[b] = jnp.where(row_slots == length, row, cache[b])

    with jax.named_scope("wo_wait"):
        wait_for(wo, sem_wo.at[0])
    pending = list(range(rows))

    def updates(count):
        for _ in range(count):
            if pending:
                update(pending.pop(0))

    for h in range(HALVES):
        with jax.named_scope(f"o_wait{h}"):
            exchange_wait(orecv, o_rsem, h)
        oc[h] = orecv[h].reshape(n * half_rows, cols)
        multiplies(h, 0, ahead)
        if h == 1:
            multiplies(0, ahead, chips)
        reduce_step(h, 0)
    reduce_step(0, 1)
    for h in range(1, HALVES):
        multiplies(h, ahead, chips)
        reduce_step(h, 1)
        updates(3)
    for step in range(2, arm):
        for h in range(HALVES):
            reduce_step(h, step)
            updates(4)
    updates(rows)
    for h in range(HALVES):
        finish(h)

    with jax.named_scope("tail"):
        wait_for(qs.at[:, pl.ds(0, n - 1)], q_ssem.at[0])
        wait_for(osend.at[:, pl.ds(0, n - 1)], o_ssem.at[0])
        wait_for(ps, p_ssem.at[0])
        wait_for(rs, r_ssem.at[0])


def write_kernel(y, kc, vc, y_out, k_out, v_out, sem):
    rows = kc.shape[0] // WRITES
    copies = [pltpu.make_async_copy(y, y_out, sem.at[0])]
    for i in range(WRITES):
        span = pl.ds(i * rows, rows)
        copies.append(pltpu.make_async_copy(kc.at[span], k_out.at[span], sem.at[1 + 2 * i]))
        copies.append(pltpu.make_async_copy(vc.at[span], v_out.at[span], sem.at[2 + 2 * i]))
    for copy in copies:
        copy.start()
    for copy in copies:
        copy.wait()


def solution(mesh):
    n = mesh.shape["tp"]
    cache_spec = P(("dp", "tp"), None, None)

    def local_step(hidden, w_query, w_key, w_value, w_out, k_cache, v_cache, lengths):
        rows, seq_len, head_dim = k_cache.shape
        batch, depth = hidden.shape
        cols = w_query.shape[1]
        half_rows = rows // HALVES
        chips = n // 2
        heads = cols * n // head_dim
        half_dim = head_dim // 2
        inv_freq = 10000.0 ** (-(jnp.arange(half_dim, dtype=F32) * 2.0) / head_dim)
        hbm_spec = pl.BlockSpec(memory_space=pltpu.HBM)
        vmem_spec = pl.BlockSpec(memory_space=pltpu.VMEM)
        dma = pltpu.SemaphoreType.DMA
        piece = (n * half_rows, cols // 2)
        y, k_vmem, v_vmem = pl.pallas_call(
            functools.partial(decode_kernel, n),
            out_shape=(
                jax.ShapeDtypeStruct((n, HALVES, half_rows, cols), BF16),
                jax.ShapeDtypeStruct(k_cache.shape, BF16),
                jax.ShapeDtypeStruct(v_cache.shape, BF16),
            ),
            in_specs=[hbm_spec] * 8 + [vmem_spec],
            out_specs=(vmem_spec, vmem_spec, vmem_spec),
            scratch_shapes=[
                pltpu.VMEM((batch, depth), BF16),
                pltpu.VMEM((depth, cols), BF16),
                pltpu.VMEM((depth, head_dim), BF16),
                pltpu.VMEM((depth, head_dim), BF16),
                pltpu.VMEM(w_out.shape, BF16),
                pltpu.SMEM((batch,), jnp.int32),
                pltpu.VMEM((batch, cols), F32),
                pltpu.VMEM((HALVES, n, half_rows, cols), BF16),
                pltpu.VMEM((HALVES, n, half_rows, cols), BF16),
                pltpu.VMEM((half_rows * heads, half_dim), F32),
                pltpu.VMEM((half_rows * heads, half_dim), F32),
                pltpu.VMEM((half_rows * heads, half_dim), F32),
                pltpu.VMEM((half_rows * heads, half_dim), F32),
                pltpu.VMEM((half_rows * heads, seq_len), F32),
                pltpu.VMEM((half_rows * heads, seq_len), BF16),
                pltpu.VMEM((HALVES, n, half_rows, cols), BF16),
                pltpu.VMEM((HALVES, n, half_rows, cols), BF16),
                pltpu.VMEM((HALVES, n * half_rows, cols), BF16),
                pltpu.VMEM((rows, half_dim), F32),
                pltpu.VMEM((rows, half_dim), F32),
                pltpu.VMEM((rows, head_dim), F32),
                pltpu.VMEM((rows, head_dim), F32),
                pltpu.VMEM((HALVES, chips, 2) + piece, F32),
                pltpu.VMEM((HALVES, chips, 2) + piece, BF16),
                pltpu.VMEM((HALVES, chips, 2) + piece, BF16),
                pltpu.VMEM((HALVES, 2, chips - 1) + piece, BF16),
                pltpu.VMEM((HALVES, 2, chips - 1) + piece, BF16),
                dma((1,)),
                dma((K_CHUNKS,)),
                dma((K_CHUNKS // 2,)),
                dma((HALVES,)),
                dma((1,)),
                dma((1,)),
                dma((HALVES,)),
                dma((1,)),
                dma((HALVES,)),
                dma((1,)),
                dma((HALVES, 4)),
                dma((1,)),
                dma((HALVES, 2, chips - 1)),
            ],
            compiler_params=pltpu.CompilerParams(
                collective_id=0, has_side_effects=True, vmem_limit_bytes=45 * 1024 * 1024
            ),
        )(hidden, w_query, w_key, w_value, w_out, k_cache, v_cache, pltpu.with_memory_space_constraint(lengths, pltpu.HBM), inv_freq[None, :])
        y, k_out, v_out = pl.pallas_call(
            write_kernel,
            out_shape=tuple(jax.ShapeDtypeStruct(a.shape, BF16) for a in (y, k_vmem, v_vmem)),
            in_specs=[vmem_spec] * 3,
            out_specs=(hbm_spec,) * 3,
            scratch_shapes=[dma((1 + 2 * WRITES,))],
            compiler_params=pltpu.CompilerParams(vmem_limit_bytes=1024 * 1024),
        )(y, k_vmem, v_vmem)
        return y.reshape(batch, cols), k_out, v_out

    return jax.shard_map(
        local_step,
        mesh=mesh,
        in_specs=(P("dp", None), P(None, "tp"), P(), P(), P("tp", None), cache_spec, cache_spec, P("dp")),
        out_specs=(P("dp", "tp"), cache_spec, cache_spec),
        check_vma=False,
    )
```

```python
import functools

import jax
import jax.numpy as jnp
from jax import lax
from jax.experimental import pallas as pl
from jax.experimental.pallas import tpu as pltpu
from jax.sharding import PartitionSpec as P

MESH = pl.DeviceIdType.MESH
HALVES = 2
K_CHUNKS = 8
AHEAD = 8
WRITES = 4
F32 = jnp.float32
BF16 = jnp.bfloat16


def decode_kernel(
    n, hid_hbm, wq_hbm, wk_hbm, wv_hbm, wo_hbm, kc_hbm, vc_hbm, len_hbm, freq_ref,
    y_ref, kc, vc,
    hid, wq, wk, wv, wo, lens, acc, qs, qr, q_lo, q_hi, o_lo, o_hi, s_buf, e_buf, osend, orecv, oc, cos_ref, sin_ref, kf, vf,
    pm, ps, pr, rs, rr,
    sem_len, sem_q, sem_kv, sem_cache, sem_wo,
    q_ssem, q_rsem, o_ssem, o_rsem, p_ssem, p_rsem, r_ssem, r_rsem,
):
    me = lax.axis_index("tp")
    chips = n // 2
    core = lax.rem(me, 2)
    chip = me // 2
    partner = me + 1 - 2 * core
    neighbours = (lax.rem(me + 2, n), lax.rem(me + n - 2, n))

    batch, depth = hid.shape
    cols = wq.shape[1]
    rows = batch // n
    half_rows = rows // HALVES
    seq_len, head_dim = kc.shape[1:]
    half_dim = head_dim // 2
    dev_heads = cols // head_dim
    heads = dev_heads * n
    block = depth // K_CHUNKS
    part = cols // 2
    out_block = wo.shape[1] // 4
    scale = head_dim ** -0.5

    def rows_of(hbm, vmem, sem, size, i):
        return pltpu.make_async_copy(hbm.at[pl.ds(i * size, size)], vmem.at[pl.ds(i * size, size)], sem)

    def columns_of(hbm, vmem, sem, size, i):
        return pltpu.make_async_copy(hbm.at[:, pl.ds(i * size, size)], vmem.at[:, pl.ds(i * size, size)], sem)

    def wait_for(buf, sem):
        pltpu.make_async_copy(buf, buf, sem).wait()

    len_copy = pltpu.make_async_copy(len_hbm, lens, sem_len.at[0])
    pair = 2 * block

    def load_q(j, size, i):
        at = (pl.ds(i * size, size), pl.ds(j * head_dim, head_dim))
        return pltpu.make_async_copy(wq_hbm.at[at], wq.at[at], sem_q.at[j, i])

    queue = [(columns_of(hid_hbm, hid, sem_q.at[0, i], block, i), load_q(0, block, i)) for i in range(K_CHUNKS)]
    queue += [(load_q(j, pair, i),) for j in range(1, dev_heads) for i in range(K_CHUNKS // 2)]
    queue += [
        (rows_of(wk_hbm, wk, sem_kv.at[i], pair, i), rows_of(wv_hbm, wv, sem_kv.at[i], pair, i))
        for i in range(K_CHUNKS // 2)
    ]
    queue += [
        (rows_of(kc_hbm, kc, sem_cache.at[h], half_rows, h), rows_of(vc_hbm, vc, sem_cache.at[h], half_rows, h))
        for h in range(HALVES)
    ]
    queue += [(columns_of(wo_hbm, wo, sem_wo.at[0], out_block, i),) for i in range(4)]
    first_rows = block // dev_heads + block * batch // cols

    def issue(count):
        for _ in range(count):
            if queue:
                for copy in queue.pop(0):
                    copy.start()

    len_copy.start()
    issue(AHEAD)

    barrier = pltpu.get_barrier_semaphore()
    order = sorted(range(1, n), key=lambda i: (min(i, n - i), i), reverse=True)
    for i in order:
        pl.semaphore_signal(barrier, inc=1, device_id={"tp": lax.rem(me + i, n)}, device_id_type=MESH)

    def exchange(src, dst, send_sem, recv_sem, *at):
        for i in order:
            peer = lax.rem(me + i, n)
            pltpu.make_async_remote_copy(
                src_ref=src.at[(*at, peer)],
                dst_ref=dst.at[(*at, me)],
                send_sem=send_sem.at[0],
                recv_sem=recv_sem.at[at[0]],
                device_id={"tp": peer},
                device_id_type=MESH,
            ).start()
        dst[(*at, me)] = src[(*at, me)]

    for j in range(dev_heads):
        size, count = (block, K_CHUNKS) if j == 0 else (pair, K_CHUNKS // 2)
        with jax.named_scope(f"q_mm{j}"):
            for i in range(count):
                wait_for(wq.at[pl.ds(0, first_rows if j == 0 else pair // dev_heads)], sem_q.at[j, i])
                issue(1)
                span = pl.ds(i * size, size)
                term = jnp.dot(hid[:, span], wq[span, pl.ds(j * head_dim, head_dim)], preferred_element_type=F32)
                if i == 0:
                    acc[...] = term
                elif i < count - 1:
                    acc[...] += term
                else:
                    q_all = (acc[...] + term).reshape(n, HALVES, half_rows, head_dim)
                    for h in range(HALVES):
                        qs[h, j] = q_all[:, h].astype(BF16)
        with jax.named_scope(f"q_send{j}"):
            if j == 0:
                pl.semaphore_wait(barrier, n - 1)
            exchange(qs, qr, q_ssem, q_rsem, 0, j)

    with jax.named_scope("angles"):
        len_copy.wait()
        for r in range(rows):
            cos_ref[pl.ds(r, 1), :] = lens[me * rows + r].astype(F32) * freq_ref[...]
        angles = cos_ref[...]
        sin_ref[...] = jnp.sin(angles)
        cos_ref[...] = jnp.cos(angles)

    def exchange_wait(buf, sem, h):
        wait_for(buf.at[h, pl.ds(0, n - 1)], sem.at[h])

    own = pl.ds(pl.multiple_of(me * rows, rows), rows)
    k_sum = jnp.zeros((rows, head_dim), F32)
    v_sum = jnp.zeros((rows, head_dim), F32)
    for i in range(K_CHUNKS // 2):
        with jax.named_scope(f"kv_wait{i}"):
            wait_for(wk.at[pl.ds(0, 2 * pair)], sem_kv.at[i])
        issue(1)
        span = pl.ds(i * 2 * block, 2 * block)
        h_own = hid[own, span]
        k_sum += jnp.dot(h_own, wk[span, :], preferred_element_type=F32)
        v_sum += jnp.dot(h_own, wv[span, :], preferred_element_type=F32)
    k_full = k_sum.astype(BF16).astype(F32)
    cosines, sines = cos_ref[...], sin_ref[...]
    k_lo, k_hi = k_full[:, :half_dim], k_full[:, half_dim:]
    k_rot = jnp.concatenate([k_lo * cosines - k_hi * sines, k_hi * cosines + k_lo * sines], axis=-1)
    kf[...] = k_rot.astype(BF16).astype(F32)
    vf[...] = v_sum.astype(BF16).astype(F32)
    issue(len(queue))
    with jax.named_scope("q_sendB"):
        for h in range(1, HALVES):
            for j in range(dev_heads):
                exchange(qs, qr, q_ssem, q_rsem, h, j)

    slots = lax.broadcasted_iota(jnp.int32, (heads, seq_len), 1)

    def attend(h):
        with jax.named_scope(f"q_wait{h}"):
            wait_for(qr.at[h, :, pl.ds(0, n - 1)], q_rsem.at[h])
        with jax.named_scope(f"rope{h}"):
            span = pl.ds(h * half_rows, half_rows)
            cosines, sines = cos_ref[span, :], sin_ref[span, :]
            for src in range(n):
                for j in range(dev_heads):
                    x = qr[h, j, src].astype(F32)
                    lo, hi = x[:, :half_dim], x[:, half_dim:]
                    place = pl.ds(src * dev_heads + j, half_rows, stride=heads)
                    q_lo[place, :] = lo * cosines - hi * sines
                    q_hi[place, :] = hi * cosines + lo * sines
        with jax.named_scope(f"cache_wait{h}"):
            wait_for(kc.at[pl.ds(0, 2 * half_rows)], sem_cache.at[h])
        with jax.named_scope(f"rows{h}"):
            ats = [pl.ds(r * heads, heads) for r in range(half_rows)]
            news = []
            for r, at in enumerate(ats):
                b = h * half_rows + r
                q = jnp.concatenate([q_lo[at, :], q_hi[at, :]], axis=-1).astype(BF16)
                s_buf[at, :] = lax.dot_general(q, kc[b], (((1,), (1,)), ((), ())), preferred_element_type=F32)
                news.append(jnp.sum(q.astype(F32) * kf[pl.ds(b, 1), :], axis=-1, keepdims=True) * scale)
            sums = []
            for r, at in enumerate(ats):
                length = lens[me * rows + h * half_rows + r]
                s = jnp.where(slots < length, s_buf[at, :] * scale, -1e30)
                top = jnp.maximum(jnp.max(s, axis=-1, keepdims=True), news[r])
                e = jnp.where(slots < length, jnp.exp(s - top), 0.0)
                e_new = jnp.exp(news[r] - top)
                e_buf[at, :] = e.astype(BF16)
                sums.append((e_new, jnp.sum(e, axis=-1, keepdims=True) + e_new))
            for r, at in enumerate(ats):
                b = h * half_rows + r
                e_new, total = sums[r]
                o = jnp.dot(e_buf[at, :], vc[b], preferred_element_type=F32)
                o = (o + e_new.astype(BF16).astype(F32) * vf[pl.ds(b, 1), :]) / total
                o_lo[at, :] = o[:, :half_dim]
                o_hi[at, :] = o[:, half_dim:]
        with jax.named_scope(f"opack{h}"):
            for dst in range(n):
                for j in range(dev_heads):
                    place = pl.ds(dst * dev_heads + j, half_rows, stride=heads)
                    osend[h, dst, :, pl.ds(j * head_dim, half_dim)] = o_lo[place, :].astype(BF16)
                    osend[h, dst, :, pl.ds(j * head_dim + half_dim, half_dim)] = o_hi[place, :].astype(BF16)
        with jax.named_scope(f"o_send{h}"):
            exchange(osend, orecv, o_ssem, o_rsem, h)

    for h in range(HALVES):
        attend(h)

    arm = chips // 2

    first_group = ((0, 0), (0, 1), (1, 1), (2, 0))
    last_group = ((1, 0), (2, 1)) + tuple((j, half) for j in range(3, chips) for half in range(2))

    def partner_copy(h, group, j, half=None):
        at = (h, j) if half is None else (h, j, half)
        return pltpu.make_async_remote_copy(
            src_ref=ps.at[at], dst_ref=pr.at[at], send_sem=p_ssem.at[0], recv_sem=p_rsem.at[h, group],
            device_id={"tp": partner}, device_id_type=MESH,
        )

    def multiplies(h, group):
        with jax.named_scope(f"mult{h}_{group[0][0]}"):
            o_cols = oc[h]

            def products(side, store):
                left = list(group)
                while left:
                    j, half = left.pop(0)
                    whole = bool(left) and left[0][0] == j
                    shift = (1 - 2 * ((j + 1) % 2)) * (arm - (j + 1) // 2)
                    first = (lax.rem(chip + (shift + chips), chips) * 2 + side) * cols + half * part
                    width = cols if whole else part
                    value = jnp.dot(o_cols, wo[:, pl.ds(pl.multiple_of(first, part), width)], preferred_element_type=F32)
                    store(j, half, value[:, :part])
                    if whole:
                        left.pop(0)
                        store(j, 1, value[:, part:])
                        if j == 0 and side is other:
                            partner_copy(h, 0, 0).start()

            def store_other(j, half, value):
                ps[h, j, half] = value.astype(BF16)

            def store_mine(j, half, value):
                pm[h, j, half] = value

            other = 1 - core
            products(other, store_other)
            if group is first_group:
                partner_copy(h, 1, 1, 1).start()
                partner_copy(h, 2, 2, 0).start()
            else:
                partner_copy(h, 3, 1, 0).start()
                partner_copy(h, 3, 2, 1).start()
                for j in range(3, chips):
                    partner_copy(h, 3, j).start()
            products(core, store_mine)

    def ring_copy(h, way, slot):
        return pltpu.make_async_remote_copy(
            src_ref=rs.at[h, way, slot], dst_ref=rr.at[h, way, slot],
            send_sem=r_ssem.at[0], recv_sem=r_rsem.at[h, way, slot],
            device_id={"tp": neighbours[way]}, device_id_type=MESH,
        )

    met = set()

    def chip_sum(h, j, half):
        group = {(0, 0): 0, (0, 1): 0, (1, 1): 1, (2, 0): 2}.get((j, half), 3)
        if (h, group) not in met:
            met.add((h, group))
            with jax.named_scope(f"pw{h}_{group}"):
                if group == 0:
                    partner_copy(h, 0, 0).wait_recv()
                elif group < 3:
                    partner_copy(h, group, j, half).wait_recv()
                else:
                    wait_for(pr.at[h, pl.ds(0, len(last_group) // 2)], p_rsem.at[h, 3])
        return pm[h, j, half] + pr[h, j, half].astype(F32)

    def arrived(h, way, slot):
        with jax.named_scope(f"rw{h}_{way}_{slot}"):
            ring_copy(h, way, slot).wait_recv()
        return rr[h, way, slot].astype(F32)

    def pass_on(h, way, long, step):
        hops = (arm if long else arm - 1) - step
        slot = step if long else arm + step
        half = way if long else 1 - way
        value = chip_sum(h, 0 if hops == arm else 1 + 2 * (arm - 1 - hops) + way, half)
        if step > 0:
            value = value + arrived(h, way, slot - 1)
        rs[h, way, slot] = value.astype(BF16)
        ring_copy(h, way, slot).start()

    def reduce_step(h, step):
        for long in (True, False):
            for way in range(2):
                if step < (arm if long else arm - 1):
                    pass_on(h, way, long, step)

    def finish(h):
        for half in range(2):
            value = chip_sum(h, chips - 1, half) + arrived(h, 1 - half, 2 * arm - 2) + arrived(h, half, arm - 1)
            y_ref[:, h, :, pl.ds(half * part, part)] = value.reshape(n, half_rows, part).astype(BF16)

    row_slots = lax.broadcasted_iota(jnp.int32, (seq_len, head_dim), 0)

    def update(b):
        with jax.named_scope(f"update{b}"):
            length = lens[me * rows + b]
            for cache, new in ((kc, kf), (vc, vf)):
                row = jnp.broadcast_to(new[pl.ds(b, 1), :].astype(BF16), (seq_len, head_dim))
                cache[b] = jnp.where(row_slots == length, row, cache[b])

    with jax.named_scope("wo_wait"):
        wait_for(wo, sem_wo.at[0])
    pending = list(range(rows))

    def updates(count):
        for _ in range(count):
            if pending:
                update(pending.pop(0))

    for h in range(HALVES):
        with jax.named_scope(f"o_wait{h}"):
            exchange_wait(orecv, o_rsem, h)
        oc[h] = orecv[h].reshape(n * half_rows, cols)
        multiplies(h, first_group)
        if h == 1:
            multiplies(0, last_group)
        reduce_step(h, 0)
    reduce_step(0, 1)
    for h in range(1, HALVES):
        multiplies(h, last_group)
        reduce_step(h, 1)
        updates(3)
    for step in range(2, arm):
        for h in range(HALVES):
            reduce_step(h, step)
            updates(4)
    updates(rows)
    for h in range(HALVES):
        finish(h)

    with jax.named_scope("tail"):
        wait_for(qs.at[:, :, pl.ds(0, n - 1)], q_ssem.at[0])
        wait_for(osend.at[:, pl.ds(0, n - 1)], o_ssem.at[0])
        wait_for(ps, p_ssem.at[0])
        wait_for(rs, r_ssem.at[0])


def write_kernel(y, kc, vc, y_out, k_out, v_out, sem):
    rows = kc.shape[0] // WRITES
    copies = [pltpu.make_async_copy(y, y_out, sem.at[0])]
    for i in range(WRITES):
        span = pl.ds(i * rows, rows)
        copies.append(pltpu.make_async_copy(kc.at[span], k_out.at[span], sem.at[1 + 2 * i]))
        copies.append(pltpu.make_async_copy(vc.at[span], v_out.at[span], sem.at[2 + 2 * i]))
    for copy in copies:
        copy.start()
    for copy in copies:
        copy.wait()


def solution(mesh):
    n = mesh.shape["tp"]
    cache_spec = P(("dp", "tp"), None, None)

    def local_step(hidden, w_query, w_key, w_value, w_out, k_cache, v_cache, lengths):
        rows, seq_len, head_dim = k_cache.shape
        batch, depth = hidden.shape
        cols = w_query.shape[1]
        half_rows = rows // HALVES
        chips = n // 2
        heads = cols * n // head_dim
        half_dim = head_dim // 2
        inv_freq = 10000.0 ** (-(jnp.arange(half_dim, dtype=F32) * 2.0) / head_dim)
        hbm_spec = pl.BlockSpec(memory_space=pltpu.HBM)
        vmem_spec = pl.BlockSpec(memory_space=pltpu.VMEM)
        dma = pltpu.SemaphoreType.DMA
        piece = (n * half_rows, cols // 2)
        y, k_vmem, v_vmem = pl.pallas_call(
            functools.partial(decode_kernel, n),
            out_shape=(
                jax.ShapeDtypeStruct((n, HALVES, half_rows, cols), BF16),
                jax.ShapeDtypeStruct(k_cache.shape, BF16),
                jax.ShapeDtypeStruct(v_cache.shape, BF16),
            ),
            in_specs=[hbm_spec] * 8 + [vmem_spec],
            out_specs=(vmem_spec, vmem_spec, vmem_spec),
            scratch_shapes=[
                pltpu.VMEM((batch, depth), BF16),
                pltpu.VMEM((depth, cols), BF16),
                pltpu.VMEM((depth, head_dim), BF16),
                pltpu.VMEM((depth, head_dim), BF16),
                pltpu.VMEM(w_out.shape, BF16),
                pltpu.SMEM((batch,), jnp.int32),
                pltpu.VMEM((batch, head_dim), F32),
                pltpu.VMEM((HALVES, cols // head_dim, n, half_rows, head_dim), BF16),
                pltpu.VMEM((HALVES, cols // head_dim, n, half_rows, head_dim), BF16),
                pltpu.VMEM((half_rows * heads, half_dim), F32),
                pltpu.VMEM((half_rows * heads, half_dim), F32),
                pltpu.VMEM((half_rows * heads, half_dim), F32),
                pltpu.VMEM((half_rows * heads, half_dim), F32),
                pltpu.VMEM((half_rows * heads, seq_len), F32),
                pltpu.VMEM((half_rows * heads, seq_len), BF16),
                pltpu.VMEM((HALVES, n, half_rows, cols), BF16),
                pltpu.VMEM((HALVES, n, half_rows, cols), BF16),
                pltpu.VMEM((HALVES, n * half_rows, cols), BF16),
                pltpu.VMEM((rows, half_dim), F32),
                pltpu.VMEM((rows, half_dim), F32),
                pltpu.VMEM((rows, head_dim), F32),
                pltpu.VMEM((rows, head_dim), F32),
                pltpu.VMEM((HALVES, chips, 2) + piece, F32),
                pltpu.VMEM((HALVES, chips, 2) + piece, BF16),
                pltpu.VMEM((HALVES, chips, 2) + piece, BF16),
                pltpu.VMEM((HALVES, 2, chips - 1) + piece, BF16),
                pltpu.VMEM((HALVES, 2, chips - 1) + piece, BF16),
                dma((1,)),
                dma((cols // head_dim, K_CHUNKS)),
                dma((K_CHUNKS // 2,)),
                dma((HALVES,)),
                dma((1,)),
                dma((1,)),
                dma((HALVES,)),
                dma((1,)),
                dma((HALVES,)),
                dma((1,)),
                dma((HALVES, 4)),
                dma((1,)),
                dma((HALVES, 2, chips - 1)),
            ],
            compiler_params=pltpu.CompilerParams(
                collective_id=0, has_side_effects=True, vmem_limit_bytes=45 * 1024 * 1024
            ),
        )(hidden, w_query, w_key, w_value, w_out, k_cache, v_cache, pltpu.with_memory_space_constraint(lengths, pltpu.HBM), inv_freq[None, :])
        y, k_out, v_out = pl.pallas_call(
            write_kernel,
            out_shape=tuple(jax.ShapeDtypeStruct(a.shape, BF16) for a in (y, k_vmem, v_vmem)),
            in_specs=[vmem_spec] * 3,
            out_specs=(hbm_spec,) * 3,
            scratch_shapes=[dma((1 + 2 * WRITES,))],
            compiler_params=pltpu.CompilerParams(vmem_limit_bytes=1024 * 1024),
        )(y, k_vmem, v_vmem)
        return y.reshape(batch, cols), k_out, v_out

    return jax.shard_map(
        local_step,
        mesh=mesh,
        in_specs=(P("dp", None), P(None, "tp"), P(), P(), P("tp", None), cache_spec, cache_spec, P("dp")),
        out_specs=(P("dp", "tp"), cache_spec, cache_spec),
        check_vma=False,
    )
```

```python
import functools

import jax
import jax.numpy as jnp
from jax import lax
from jax.experimental import pallas as pl
from jax.experimental.pallas import tpu as pltpu
from jax.sharding import PartitionSpec as P

MESH = pl.DeviceIdType.MESH
HALVES = 2
K_CHUNKS = 8
AHEAD = 8
WRITES = 4
F32 = jnp.float32
BF16 = jnp.bfloat16


def decode_kernel(
    n, hid_hbm, wq_hbm, wk_hbm, wv_hbm, wo_hbm, kc_hbm, vc_hbm, len_hbm, freq_ref,
    y_ref, kc, vc,
    hid, wq, wk, wv, wo, lens, acc, qs, qr, q_lo, q_hi, o_lo, o_hi, s_buf, e_buf, osend, orecv, oc, cos_ref, sin_ref, kf, vf,
    pm, ps, pr, rs, rr,
    sem_len, sem_q, sem_kv, sem_cache, sem_wo,
    q_ssem, q_rsem, o_ssem, o_rsem, p_ssem, p_rsem, r_ssem, r_rsem,
):
    me = lax.axis_index("tp")
    chips = n // 2
    core = lax.rem(me, 2)
    chip = me // 2
    partner = me + 1 - 2 * core
    neighbours = (lax.rem(me + 2, n), lax.rem(me + n - 2, n))

    batch, depth = hid.shape
    cols = wq.shape[1]
    rows = batch // n
    half_rows = rows // HALVES
    seq_len, head_dim = kc.shape[1:]
    half_dim = head_dim // 2
    dev_heads = cols // head_dim
    heads = dev_heads * n
    block = depth // K_CHUNKS
    part = cols // 2
    out_block = wo.shape[1] // 4
    scale = head_dim ** -0.5

    def rows_of(hbm, vmem, sem, size, i):
        return pltpu.make_async_copy(hbm.at[pl.ds(i * size, size)], vmem.at[pl.ds(i * size, size)], sem)

    def columns_of(hbm, vmem, sem, size, i):
        return pltpu.make_async_copy(hbm.at[:, pl.ds(i * size, size)], vmem.at[:, pl.ds(i * size, size)], sem)

    def wait_for(buf, sem):
        pltpu.make_async_copy(buf, buf, sem).wait()

    len_copy = pltpu.make_async_copy(len_hbm, lens, sem_len.at[0])
    pair = 2 * block

    def load_q(j, size, i):
        at = (pl.ds(i * size, size), pl.ds(j * head_dim, head_dim))
        return pltpu.make_async_copy(wq_hbm.at[at], wq.at[at], sem_q.at[j, i])

    queue = [(columns_of(hid_hbm, hid, sem_q.at[0, i], block, i), load_q(0, block, i)) for i in range(K_CHUNKS)]
    queue += [(load_q(j, pair, i),) for j in range(1, dev_heads) for i in range(K_CHUNKS // 2)]
    queue += [
        (rows_of(wk_hbm, wk, sem_kv.at[i], pair, i), rows_of(wv_hbm, wv, sem_kv.at[i], pair, i))
        for i in range(K_CHUNKS // 2)
    ]
    queue += [
        (rows_of(kc_hbm, kc, sem_cache.at[h], half_rows, h), rows_of(vc_hbm, vc, sem_cache.at[h], half_rows, h))
        for h in range(HALVES)
    ]
    queue += [(columns_of(wo_hbm, wo, sem_wo.at[0], out_block, i),) for i in range(4)]
    first_rows = block // dev_heads + block * batch // cols

    def issue(count):
        for _ in range(count):
            if queue:
                for copy in queue.pop(0):
                    copy.start()

    len_copy.start()
    issue(AHEAD)

    barrier = pltpu.get_barrier_semaphore()
    order = sorted(range(1, n), key=lambda i: (min(i, n - i), i), reverse=True)
    for i in order:
        pl.semaphore_signal(barrier, inc=1, device_id={"tp": lax.rem(me + i, n)}, device_id_type=MESH)

    def exchange(src, dst, send_sem, recv_sem, *at):
        for i in order:
            peer = lax.rem(me + i, n)
            pltpu.make_async_remote_copy(
                src_ref=src.at[(*at, peer)],
                dst_ref=dst.at[(*at, me)],
                send_sem=send_sem.at[0],
                recv_sem=recv_sem.at[at[0]],
                device_id={"tp": peer},
                device_id_type=MESH,
            ).start()
        dst[(*at, me)] = src[(*at, me)]

    for j in range(dev_heads):
        size, count = (block, K_CHUNKS) if j == 0 else (pair, K_CHUNKS // 2)
        with jax.named_scope(f"q_mm{j}"):
            for i in range(count):
                wait_for(wq.at[pl.ds(0, first_rows if j == 0 else pair // dev_heads)], sem_q.at[j, i])
                issue(1)
                terms = []
                for way in range(2):
                    span = pl.ds(i * size + way * (size // 2), size // 2)
                    terms.append(jnp.dot(hid[:, span], wq[span, pl.ds(j * head_dim, head_dim)], preferred_element_type=F32))
                if i < count - 1:
                    for way in range(2):
                        acc[way] = terms[way] if i == 0 else acc[way] + terms[way]
                else:
                    q_all = ((acc[0] + terms[0]) + (acc[1] + terms[1])).reshape(n, HALVES, half_rows, head_dim)
                    for h in range(HALVES):
                        qs[h, j] = q_all[:, h].astype(BF16)
        with jax.named_scope(f"q_send{j}"):
            if j == 0:
                pl.semaphore_wait(barrier, n - 1)
            exchange(qs, qr, q_ssem, q_rsem, 0, j)

    with jax.named_scope("angles"):
        len_copy.wait()
        for r in range(rows):
            cos_ref[pl.ds(r, 1), :] = lens[me * rows + r].astype(F32) * freq_ref[...]
        angles = cos_ref[...]
        sin_ref[...] = jnp.sin(angles)
        cos_ref[...] = jnp.cos(angles)

    def exchange_wait(buf, sem, h):
        wait_for(buf.at[h, pl.ds(0, n - 1)], sem.at[h])

    own = pl.ds(pl.multiple_of(me * rows, rows), rows)
    k_sum = jnp.zeros((rows, head_dim), F32)
    v_sum = jnp.zeros((rows, head_dim), F32)
    for i in range(K_CHUNKS // 2):
        with jax.named_scope(f"kv_wait{i}"):
            wait_for(wk.at[pl.ds(0, 2 * pair)], sem_kv.at[i])
        issue(1)
        span = pl.ds(i * 2 * block, 2 * block)
        h_own = hid[own, span]
        k_sum += jnp.dot(h_own, wk[span, :], preferred_element_type=F32)
        v_sum += jnp.dot(h_own, wv[span, :], preferred_element_type=F32)
    k_full = k_sum.astype(BF16).astype(F32)
    cosines, sines = cos_ref[...], sin_ref[...]
    k_lo, k_hi = k_full[:, :half_dim], k_full[:, half_dim:]
    k_rot = jnp.concatenate([k_lo * cosines - k_hi * sines, k_hi * cosines + k_lo * sines], axis=-1)
    kf[...] = k_rot.astype(BF16).astype(F32)
    vf[...] = v_sum.astype(BF16).astype(F32)
    issue(len(queue))
    with jax.named_scope("q_sendB"):
        for h in range(1, HALVES):
            for j in range(dev_heads):
                exchange(qs, qr, q_ssem, q_rsem, h, j)

    slots = lax.broadcasted_iota(jnp.int32, (heads, seq_len), 1)

    def attend(h):
        with jax.named_scope(f"q_wait{h}"):
            wait_for(qr.at[h, :, pl.ds(0, n - 1)], q_rsem.at[h])
        with jax.named_scope(f"rope{h}"):
            span = pl.ds(h * half_rows, half_rows)
            cosines, sines = cos_ref[span, :], sin_ref[span, :]
            for src in range(n):
                for j in range(dev_heads):
                    x = qr[h, j, src].astype(F32)
                    lo, hi = x[:, :half_dim], x[:, half_dim:]
                    place = pl.ds(src * dev_heads + j, half_rows, stride=heads)
                    q_lo[place, :] = lo * cosines - hi * sines
                    q_hi[place, :] = hi * cosines + lo * sines
        with jax.named_scope(f"cache_wait{h}"):
            wait_for(kc.at[pl.ds(0, 2 * half_rows)], sem_cache.at[h])
        with jax.named_scope(f"rows{h}"):
            ats = [pl.ds(r * heads, heads) for r in range(half_rows)]
            news = []
            for r, at in enumerate(ats):
                b = h * half_rows + r
                q = jnp.concatenate([q_lo[at, :], q_hi[at, :]], axis=-1).astype(BF16)
                s_buf[at, :] = lax.dot_general(q, kc[b], (((1,), (1,)), ((), ())), preferred_element_type=F32)
                news.append(jnp.sum(q.astype(F32) * kf[pl.ds(b, 1), :], axis=-1, keepdims=True) * scale)
            sums = []
            for r, at in enumerate(ats):
                length = lens[me * rows + h * half_rows + r]
                s = jnp.where(slots < length, s_buf[at, :] * scale, -1e30)
                top = jnp.maximum(jnp.max(s, axis=-1, keepdims=True), news[r])
                e = jnp.where(slots < length, jnp.exp(s - top), 0.0)
                e_new = jnp.exp(news[r] - top)
                e_buf[at, :] = e.astype(BF16)
                sums.append((e_new, jnp.sum(e, axis=-1, keepdims=True) + e_new))
            for r, at in enumerate(ats):
                b = h * half_rows + r
                e_new, total = sums[r]
                o = jnp.dot(e_buf[at, :], vc[b], preferred_element_type=F32)
                o = (o + e_new.astype(BF16).astype(F32) * vf[pl.ds(b, 1), :]) / total
                o_lo[at, :] = o[:, :half_dim]
                o_hi[at, :] = o[:, half_dim:]
        with jax.named_scope(f"opack{h}"):
            for dst in range(n):
                for j in range(dev_heads):
                    place = pl.ds(dst * dev_heads + j, half_rows, stride=heads)
                    osend[h, dst, :, pl.ds(j * head_dim, half_dim)] = o_lo[place, :].astype(BF16)
                    osend[h, dst, :, pl.ds(j * head_dim + half_dim, half_dim)] = o_hi[place, :].astype(BF16)
        with jax.named_scope(f"o_send{h}"):
            exchange(osend, orecv, o_ssem, o_rsem, h)

    for h in range(HALVES):
        attend(h)

    arm = chips // 2

    first_group = ((0, 0), (0, 1), (1, 1), (2, 0))
    last_group = ((1, 0), (2, 1)) + tuple((j, half) for j in range(3, chips) for half in range(2))

    def partner_copy(h, group, j, half=None):
        at = (h, j) if half is None else (h, j, half)
        return pltpu.make_async_remote_copy(
            src_ref=ps.at[at], dst_ref=pr.at[at], send_sem=p_ssem.at[0], recv_sem=p_rsem.at[h, group],
            device_id={"tp": partner}, device_id_type=MESH,
        )

    def multiplies(h, group):
        with jax.named_scope(f"mult{h}_{group[0][0]}"):
            o_cols = oc[h]

            def products(side, store):
                left = list(group)
                while left:
                    j, half = left.pop(0)
                    whole = bool(left) and left[0][0] == j
                    shift = (1 - 2 * ((j + 1) % 2)) * (arm - (j + 1) // 2)
                    first = (lax.rem(chip + (shift + chips), chips) * 2 + side) * cols + half * part
                    width = cols if whole else part
                    value = jnp.dot(o_cols, wo[:, pl.ds(pl.multiple_of(first, part), width)], preferred_element_type=F32)
                    store(j, half, value[:, :part])
                    if whole:
                        left.pop(0)
                        store(j, 1, value[:, part:])
                        if j == 0 and side is other:
                            partner_copy(h, 0, 0).start()

            def store_other(j, half, value):
                ps[h, j, half] = value.astype(BF16)

            def store_mine(j, half, value):
                pm[h, j, half] = value

            other = 1 - core
            products(other, store_other)
            if group is first_group:
                partner_copy(h, 1, 1, 1).start()
                partner_copy(h, 2, 2, 0).start()
            else:
                partner_copy(h, 3, 1, 0).start()
                partner_copy(h, 3, 2, 1).start()
                for j in range(3, chips):
                    partner_copy(h, 3, j).start()
            products(core, store_mine)

    def ring_copy(h, way, slot):
        return pltpu.make_async_remote_copy(
            src_ref=rs.at[h, way, slot], dst_ref=rr.at[h, way, slot],
            send_sem=r_ssem.at[0], recv_sem=r_rsem.at[h, way, slot],
            device_id={"tp": neighbours[way]}, device_id_type=MESH,
        )

    met = set()

    def chip_sum(h, j, half):
        group = {(0, 0): 0, (0, 1): 0, (1, 1): 1, (2, 0): 2}.get((j, half), 3)
        if (h, group) not in met:
            met.add((h, group))
            with jax.named_scope(f"pw{h}_{group}"):
                if group == 0:
                    partner_copy(h, 0, 0).wait_recv()
                elif group < 3:
                    partner_copy(h, group, j, half).wait_recv()
                else:
                    wait_for(pr.at[h, pl.ds(0, len(last_group) // 2)], p_rsem.at[h, 3])
        return pm[h, j, half] + pr[h, j, half].astype(F32)

    def arrived(h, way, slot):
        with jax.named_scope(f"rw{h}_{way}_{slot}"):
            ring_copy(h, way, slot).wait_recv()
        return rr[h, way, slot].astype(F32)

    def pass_on(h, way, long, step):
        hops = (arm if long else arm - 1) - step
        slot = step if long else arm + step
        half = way if long else 1 - way
        value = chip_sum(h, 0 if hops == arm else 1 + 2 * (arm - 1 - hops) + way, half)
        if step > 0:
            value = value + arrived(h, way, slot - 1)
        rs[h, way, slot] = value.astype(BF16)
        ring_copy(h, way, slot).start()

    def reduce_step(h, step):
        for long in (True, False):
            for way in range(2):
                if step < (arm if long else arm - 1):
                    pass_on(h, way, long, step)

    def finish(h):
        for half in range(2):
            value = chip_sum(h, chips - 1, half) + arrived(h, 1 - half, 2 * arm - 2) + arrived(h, half, arm - 1)
            y_ref[:, h, :, pl.ds(half * part, part)] = value.reshape(n, half_rows, part).astype(BF16)

    row_slots = lax.broadcasted_iota(jnp.int32, (seq_len, head_dim), 0)

    def update(b):
        with jax.named_scope(f"update{b}"):
            length = lens[me * rows + b]
            for cache, new in ((kc, kf), (vc, vf)):
                row = jnp.broadcast_to(new[pl.ds(b, 1), :].astype(BF16), (seq_len, head_dim))
                cache[b] = jnp.where(row_slots == length, row, cache[b])

    with jax.named_scope("wo_wait"):
        wait_for(wo, sem_wo.at[0])
    pending = list(range(rows))

    def updates(count):
        for _ in range(count):
            if pending:
                update(pending.pop(0))

    for h in range(HALVES):
        with jax.named_scope(f"o_wait{h}"):
            exchange_wait(orecv, o_rsem, h)
        oc[h] = orecv[h].reshape(n * half_rows, cols)
        multiplies(h, first_group)
        reduce_step(h, 0)
        if h == 0:
            multiplies(h, last_group)
    reduce_step(0, 1)
    for h in range(1, HALVES):
        multiplies(h, last_group)
        reduce_step(h, 1)
        updates(3)
    for step in range(2, arm):
        for h in range(HALVES):
            reduce_step(h, step)
            updates(4)
    updates(rows)
    for h in range(HALVES):
        finish(h)

    with jax.named_scope("tail"):
        wait_for(qs.at[:, :, pl.ds(0, n - 1)], q_ssem.at[0])
        wait_for(osend.at[:, pl.ds(0, n - 1)], o_ssem.at[0])
        wait_for(ps, p_ssem.at[0])
        wait_for(rs, r_ssem.at[0])


def write_kernel(y, kc, vc, y_out, k_out, v_out, sem):
    rows = kc.shape[0] // WRITES
    copies = [pltpu.make_async_copy(y, y_out, sem.at[0])]
    for i in range(WRITES):
        span = pl.ds(i * rows, rows)
        copies.append(pltpu.make_async_copy(kc.at[span], k_out.at[span], sem.at[1 + 2 * i]))
        copies.append(pltpu.make_async_copy(vc.at[span], v_out.at[span], sem.at[2 + 2 * i]))
    for copy in copies:
        copy.start()
    for copy in copies:
        copy.wait()


def solution(mesh):
    n = mesh.shape["tp"]
    cache_spec = P(("dp", "tp"), None, None)

    def local_step(hidden, w_query, w_key, w_value, w_out, k_cache, v_cache, lengths):
        rows, seq_len, head_dim = k_cache.shape
        batch, depth = hidden.shape
        cols = w_query.shape[1]
        half_rows = rows // HALVES
        chips = n // 2
        heads = cols * n // head_dim
        half_dim = head_dim // 2
        inv_freq = 10000.0 ** (-(jnp.arange(half_dim, dtype=F32) * 2.0) / head_dim)
        hbm_spec = pl.BlockSpec(memory_space=pltpu.HBM)
        vmem_spec = pl.BlockSpec(memory_space=pltpu.VMEM)
        dma = pltpu.SemaphoreType.DMA
        piece = (n * half_rows, cols // 2)
        y, k_vmem, v_vmem = pl.pallas_call(
            functools.partial(decode_kernel, n),
            out_shape=(
                jax.ShapeDtypeStruct((n, HALVES, half_rows, cols), BF16),
                jax.ShapeDtypeStruct(k_cache.shape, BF16),
                jax.ShapeDtypeStruct(v_cache.shape, BF16),
            ),
            in_specs=[hbm_spec] * 8 + [vmem_spec],
            out_specs=(vmem_spec, vmem_spec, vmem_spec),
            scratch_shapes=[
                pltpu.VMEM((batch, depth), BF16),
                pltpu.VMEM((depth, cols), BF16),
                pltpu.VMEM((depth, head_dim), BF16),
                pltpu.VMEM((depth, head_dim), BF16),
                pltpu.VMEM(w_out.shape, BF16),
                pltpu.SMEM((batch,), jnp.int32),
                pltpu.VMEM((2, batch, head_dim), F32),
                pltpu.VMEM((HALVES, cols // head_dim, n, half_rows, head_dim), BF16),
                pltpu.VMEM((HALVES, cols // head_dim, n, half_rows, head_dim), BF16),
                pltpu.VMEM((half_rows * heads, half_dim), F32),
                pltpu.VMEM((half_rows * heads, half_dim), F32),
                pltpu.VMEM((half_rows * heads, half_dim), F32),
                pltpu.VMEM((half_rows * heads, half_dim), F32),
                pltpu.VMEM((half_rows * heads, seq_len), F32),
                pltpu.VMEM((half_rows * heads, seq_len), BF16),
                pltpu.VMEM((HALVES, n, half_rows, cols), BF16),
                pltpu.VMEM((HALVES, n, half_rows, cols), BF16),
                pltpu.VMEM((HALVES, n * half_rows, cols), BF16),
                pltpu.VMEM((rows, half_dim), F32),
                pltpu.VMEM((rows, half_dim), F32),
                pltpu.VMEM((rows, head_dim), F32),
                pltpu.VMEM((rows, head_dim), F32),
                pltpu.VMEM((HALVES, chips, 2) + piece, F32),
                pltpu.VMEM((HALVES, chips, 2) + piece, BF16),
                pltpu.VMEM((HALVES, chips, 2) + piece, BF16),
                pltpu.VMEM((HALVES, 2, chips - 1) + piece, BF16),
                pltpu.VMEM((HALVES, 2, chips - 1) + piece, BF16),
                dma((1,)),
                dma((cols // head_dim, K_CHUNKS)),
                dma((K_CHUNKS // 2,)),
                dma((HALVES,)),
                dma((1,)),
                dma((1,)),
                dma((HALVES,)),
                dma((1,)),
                dma((HALVES,)),
                dma((1,)),
                dma((HALVES, 4)),
                dma((1,)),
                dma((HALVES, 2, chips - 1)),
            ],
            compiler_params=pltpu.CompilerParams(
                collective_id=0, has_side_effects=True, vmem_limit_bytes=45 * 1024 * 1024
            ),
        )(hidden, w_query, w_key, w_value, w_out, k_cache, v_cache, pltpu.with_memory_space_constraint(lengths, pltpu.HBM), inv_freq[None, :])
        y, k_out, v_out = pl.pallas_call(
            write_kernel,
            out_shape=tuple(jax.ShapeDtypeStruct(a.shape, BF16) for a in (y, k_vmem, v_vmem)),
            in_specs=[vmem_spec] * 3,
            out_specs=(hbm_spec,) * 3,
            scratch_shapes=[dma((1 + 2 * WRITES,))],
            compiler_params=pltpu.CompilerParams(vmem_limit_bytes=1024 * 1024),
        )(y, k_vmem, v_vmem)
        return y.reshape(batch, cols), k_out, v_out

    return jax.shard_map(
        local_step,
        mesh=mesh,
        in_specs=(P("dp", None), P(None, "tp"), P(), P(), P("tp", None), cache_spec, cache_spec, P("dp")),
        out_specs=(P("dp", "tp"), cache_spec, cache_spec),
        check_vma=False,
    )
```

```python
import functools

import jax
import jax.numpy as jnp
from jax import lax
from jax.experimental import pallas as pl
from jax.experimental.pallas import tpu as pltpu
from jax.sharding import PartitionSpec as P

MESH = pl.DeviceIdType.MESH
HALVES = 2
K_CHUNKS = 8
IN_FLIGHT = 5 * 1024 * 1024
WRITES = 4
F32 = jnp.float32
BF16 = jnp.bfloat16


def decode_kernel(
    n, hid_hbm, wq_hbm, wk_hbm, wv_hbm, wo_hbm, kc_hbm, vc_hbm, len_hbm, freq_ref,
    y_ref, kc, vc,
    hid, wq, wk, wv, wo, lens, acc, qs, qr, q_lo, q_hi, o_lo, o_hi, s_buf, e_buf, osend, orecv, oc, cos_ref, sin_ref, kf, vf,
    pm, ps, pr, rs, rr,
    sem_len, sem_q, sem_kv, sem_cache, sem_wo,
    q_ssem, q_rsem, o_ssem, o_rsem, p_ssem, p_rsem, r_ssem, r_rsem,
):
    me = lax.axis_index("tp")
    chips = n // 2
    core = lax.rem(me, 2)
    chip = me // 2
    partner = me + 1 - 2 * core
    neighbours = (lax.rem(me + 2, n), lax.rem(me + n - 2, n))

    batch, depth = hid.shape
    cols = wq.shape[1]
    rows = batch // n
    half_rows = rows // HALVES
    seq_len, head_dim = kc.shape[1:]
    half_dim = head_dim // 2
    dev_heads = cols // head_dim
    heads = dev_heads * n
    block = depth // K_CHUNKS
    part = cols // 2
    out_block = wo.shape[1] // 4
    scale = head_dim ** -0.5

    def rows_of(hbm, vmem, sem, size, i):
        return pltpu.make_async_copy(hbm.at[pl.ds(i * size, size)], vmem.at[pl.ds(i * size, size)], sem)

    def columns_of(hbm, vmem, sem, size, i):
        return pltpu.make_async_copy(hbm.at[:, pl.ds(i * size, size)], vmem.at[:, pl.ds(i * size, size)], sem)

    def wait_for(buf, sem):
        pltpu.make_async_copy(buf, buf, sem).wait()

    len_copy = pltpu.make_async_copy(len_hbm, lens, sem_len.at[0])
    pair = 2 * block

    def load_q(j, size, i):
        at = (pl.ds(i * size, size), pl.ds(j * head_dim, head_dim))
        return pltpu.make_async_copy(wq_hbm.at[at], wq.at[at], sem_q.at[j, i])

    weight_bytes = 2 * block * head_dim
    queue = [
        (weight_bytes + 2 * batch * block, columns_of(hid_hbm, hid, sem_q.at[0, i], block, i), load_q(0, block, i))
        for i in range(K_CHUNKS)
    ]
    queue += [(2 * weight_bytes, load_q(j, pair, i)) for j in range(1, dev_heads) for i in range(K_CHUNKS // 2)]
    queue += [
        (4 * weight_bytes, rows_of(wk_hbm, wk, sem_kv.at[i], pair, i), rows_of(wv_hbm, wv, sem_kv.at[i], pair, i))
        for i in range(K_CHUNKS // 2)
    ]
    queue += [
        (4 * half_rows * seq_len * head_dim, rows_of(kc_hbm, kc, sem_cache.at[h], half_rows, h), rows_of(vc_hbm, vc, sem_cache.at[h], half_rows, h))
        for h in range(HALVES)
    ]
    queue += [(2 * cols * out_block, columns_of(wo_hbm, wo, sem_wo.at[0], out_block, i)) for i in range(4)]
    first_rows = block // dev_heads + block * batch // cols

    flight = []

    def issue(everything=False):
        while queue and (everything or sum(flight) + queue[0][0] <= IN_FLIGHT):
            size, *copies = queue.pop(0)
            flight.append(size)
            for copy in copies:
                copy.start()

    def landed():
        flight.pop(0)
        issue()

    len_copy.start()
    issue()

    barrier = pltpu.get_barrier_semaphore()
    order = sorted(range(1, n), key=lambda i: (min(i, n - i), i), reverse=True)
    for i in order:
        pl.semaphore_signal(barrier, inc=1, device_id={"tp": lax.rem(me + i, n)}, device_id_type=MESH)

    def exchange(src, dst, send_sem, recv_sem, *at):
        for i in order:
            peer = lax.rem(me + i, n)
            pltpu.make_async_remote_copy(
                src_ref=src.at[(*at, peer)],
                dst_ref=dst.at[(*at, me)],
                send_sem=send_sem.at[0],
                recv_sem=recv_sem.at[at[0]],
                device_id={"tp": peer},
                device_id_type=MESH,
            ).start()
        dst[(*at, me)] = src[(*at, me)]

    for j in range(dev_heads):
        size, count = (block, K_CHUNKS) if j == 0 else (pair, K_CHUNKS // 2)
        with jax.named_scope(f"q_mm{j}"):
            for i in range(count):
                wait_for(wq.at[pl.ds(0, first_rows if j == 0 else pair // dev_heads)], sem_q.at[j, i])
                landed()
                terms = []
                for way in range(2):
                    span = pl.ds(i * size + way * (size // 2), size // 2)
                    terms.append(jnp.dot(hid[:, span], wq[span, pl.ds(j * head_dim, head_dim)], preferred_element_type=F32))
                if i < count - 1:
                    for way in range(2):
                        acc[way] = terms[way] if i == 0 else acc[way] + terms[way]
                else:
                    q_all = ((acc[0] + terms[0]) + (acc[1] + terms[1])).reshape(n, HALVES, half_rows, head_dim)
                    for h in range(HALVES):
                        qs[h, j] = q_all[:, h].astype(BF16)
        with jax.named_scope(f"q_send{j}"):
            if j == 0:
                pl.semaphore_wait(barrier, n - 1)
            exchange(qs, qr, q_ssem, q_rsem, 0, j)

    with jax.named_scope("angles"):
        len_copy.wait()
        for r in range(rows):
            cos_ref[pl.ds(r, 1), :] = lens[me * rows + r].astype(F32) * freq_ref[...]
        angles = cos_ref[...]
        sin_ref[...] = jnp.sin(angles)
        cos_ref[...] = jnp.cos(angles)

    def exchange_wait(buf, sem, h):
        wait_for(buf.at[h, pl.ds(0, n - 1)], sem.at[h])

    own = pl.ds(pl.multiple_of(me * rows, rows), rows)
    k_sum = jnp.zeros((rows, head_dim), F32)
    v_sum = jnp.zeros((rows, head_dim), F32)
    for i in range(K_CHUNKS // 2):
        with jax.named_scope(f"kv_wait{i}"):
            wait_for(wk.at[pl.ds(0, 2 * pair)], sem_kv.at[i])
        landed()
        span = pl.ds(i * 2 * block, 2 * block)
        h_own = hid[own, span]
        k_sum += jnp.dot(h_own, wk[span, :], preferred_element_type=F32)
        v_sum += jnp.dot(h_own, wv[span, :], preferred_element_type=F32)
        if i == 1:
            with jax.named_scope("q_sendB"):
                for h in range(1, HALVES):
                    for j in range(dev_heads):
                        exchange(qs, qr, q_ssem, q_rsem, h, j)
    k_full = k_sum.astype(BF16).astype(F32)
    cosines, sines = cos_ref[...], sin_ref[...]
    k_lo, k_hi = k_full[:, :half_dim], k_full[:, half_dim:]
    k_rot = jnp.concatenate([k_lo * cosines - k_hi * sines, k_hi * cosines + k_lo * sines], axis=-1)
    kf[...] = k_rot.astype(BF16).astype(F32)
    vf[...] = v_sum.astype(BF16).astype(F32)
    issue(everything=True)
    slots = lax.broadcasted_iota(jnp.int32, (heads, seq_len), 1)

    def attend(h):
        with jax.named_scope(f"q_wait{h}"):
            wait_for(qr.at[h, :, pl.ds(0, n - 1)], q_rsem.at[h])
        with jax.named_scope(f"rope{h}"):
            span = pl.ds(h * half_rows, half_rows)
            cosines, sines = cos_ref[span, :], sin_ref[span, :]
            for src in range(n):
                for j in range(dev_heads):
                    x = qr[h, j, src].astype(F32)
                    lo, hi = x[:, :half_dim], x[:, half_dim:]
                    place = pl.ds(src * dev_heads + j, half_rows, stride=heads)
                    q_lo[place, :] = lo * cosines - hi * sines
                    q_hi[place, :] = hi * cosines + lo * sines
        with jax.named_scope(f"cache_wait{h}"):
            wait_for(kc.at[pl.ds(0, 2 * half_rows)], sem_cache.at[h])
        with jax.named_scope(f"rows{h}"):
            ats = [pl.ds(r * heads, heads) for r in range(half_rows)]
            news = []
            for r, at in enumerate(ats):
                b = h * half_rows + r
                q = jnp.concatenate([q_lo[at, :], q_hi[at, :]], axis=-1).astype(BF16)
                s_buf[at, :] = lax.dot_general(q, kc[b], (((1,), (1,)), ((), ())), preferred_element_type=F32)
                news.append(jnp.sum(q.astype(F32) * kf[pl.ds(b, 1), :], axis=-1, keepdims=True) * scale)
            sums = []
            for r, at in enumerate(ats):
                length = lens[me * rows + h * half_rows + r]
                s = jnp.where(slots < length, s_buf[at, :] * scale, -1e30)
                top = jnp.maximum(jnp.max(s, axis=-1, keepdims=True), news[r])
                e = jnp.where(slots < length, jnp.exp(s - top), 0.0)
                e_new = jnp.exp(news[r] - top)
                e_buf[at, :] = e.astype(BF16)
                sums.append((e_new, jnp.sum(e, axis=-1, keepdims=True) + e_new))
            for r, at in enumerate(ats):
                b = h * half_rows + r
                e_new, total = sums[r]
                o = jnp.dot(e_buf[at, :], vc[b], preferred_element_type=F32)
                o = (o + e_new.astype(BF16).astype(F32) * vf[pl.ds(b, 1), :]) / total
                o_lo[at, :] = o[:, :half_dim]
                o_hi[at, :] = o[:, half_dim:]
        with jax.named_scope(f"opack{h}"):
            for dst in range(n):
                for j in range(dev_heads):
                    place = pl.ds(dst * dev_heads + j, half_rows, stride=heads)
                    osend[h, dst, :, pl.ds(j * head_dim, half_dim)] = o_lo[place, :].astype(BF16)
                    osend[h, dst, :, pl.ds(j * head_dim + half_dim, half_dim)] = o_hi[place, :].astype(BF16)
        with jax.named_scope(f"o_send{h}"):
            exchange(osend, orecv, o_ssem, o_rsem, h)

    for h in range(HALVES):
        attend(h)

    arm = chips // 2

    first_group = ((0, 0), (0, 1), (1, 1), (2, 0))
    last_group = ((1, 0), (2, 1)) + tuple((j, half) for j in range(3, chips) for half in range(2))

    def partner_copy(h, group, j, half=None):
        at = (h, j) if half is None else (h, j, half)
        return pltpu.make_async_remote_copy(
            src_ref=ps.at[at], dst_ref=pr.at[at], send_sem=p_ssem.at[0], recv_sem=p_rsem.at[h, group],
            device_id={"tp": partner}, device_id_type=MESH,
        )

    def multiplies(h, group, own):
        with jax.named_scope(f"mult{h}_{group[0][0]}_{int(own)}"):
            o_cols = oc[h]

            def products(side, store):
                left = list(group)
                while left:
                    j, half = left.pop(0)
                    whole = bool(left) and left[0][0] == j
                    shift = (1 - 2 * ((j + 1) % 2)) * (arm - (j + 1) // 2)
                    first = (lax.rem(chip + (shift + chips), chips) * 2 + side) * cols + half * part
                    width = cols if whole else part
                    value = jnp.dot(o_cols, wo[:, pl.ds(pl.multiple_of(first, part), width)], preferred_element_type=F32)
                    store(j, half, value[:, :part])
                    if whole:
                        left.pop(0)
                        store(j, 1, value[:, part:])
                        if j == 0 and not own:
                            partner_copy(h, 0, 0).start()

            def store_other(j, half, value):
                ps[h, j, half] = value.astype(BF16)

            def store_mine(j, half, value):
                pm[h, j, half] = value

            if own:
                products(core, store_mine)
                return
            products(1 - core, store_other)
            if group is first_group:
                partner_copy(h, 1, 1, 1).start()
                partner_copy(h, 2, 2, 0).start()
            else:
                partner_copy(h, 3, 1, 0).start()
                partner_copy(h, 3, 2, 1).start()
                for j in range(3, chips):
                    partner_copy(h, 3, j).start()

    def ring_copy(h, way, slot):
        return pltpu.make_async_remote_copy(
            src_ref=rs.at[h, way, slot], dst_ref=rr.at[h, way, slot],
            send_sem=r_ssem.at[0], recv_sem=r_rsem.at[h, way, slot],
            device_id={"tp": neighbours[way]}, device_id_type=MESH,
        )

    met = set()

    def chip_sum(h, j, half):
        group = {(0, 0): 0, (0, 1): 0, (1, 1): 1, (2, 0): 2}.get((j, half), 3)
        if (h, group) not in met:
            met.add((h, group))
            with jax.named_scope(f"pw{h}_{group}"):
                if group == 0:
                    partner_copy(h, 0, 0).wait_recv()
                elif group < 3:
                    partner_copy(h, group, j, half).wait_recv()
                else:
                    wait_for(pr.at[h, pl.ds(0, len(last_group) // 2)], p_rsem.at[h, 3])
        return pm[h, j, half] + pr[h, j, half].astype(F32)

    def arrived(h, way, slot):
        with jax.named_scope(f"rw{h}_{way}_{slot}"):
            ring_copy(h, way, slot).wait_recv()
        return rr[h, way, slot].astype(F32)

    def pass_on(h, way, long, step):
        hops = (arm if long else arm - 1) - step
        slot = step if long else arm + step
        half = way if long else 1 - way
        value = chip_sum(h, 0 if hops == arm else 1 + 2 * (arm - 1 - hops) + way, half)
        if step > 0:
            value = value + arrived(h, way, slot - 1)
        rs[h, way, slot] = value.astype(BF16)
        ring_copy(h, way, slot).start()

    def reduce_step(h, step):
        for long in (True, False):
            for way in range(2):
                if step < (arm if long else arm - 1):
                    pass_on(h, way, long, step)

    def finish(h):
        for half in range(2):
            value = chip_sum(h, chips - 1, half) + arrived(h, 1 - half, 2 * arm - 2) + arrived(h, half, arm - 1)
            y_ref[:, h, :, pl.ds(half * part, part)] = value.reshape(n, half_rows, part).astype(BF16)

    row_slots = lax.broadcasted_iota(jnp.int32, (seq_len, head_dim), 0)

    def update(b):
        with jax.named_scope(f"update{b}"):
            length = lens[me * rows + b]
            for cache, new in ((kc, kf), (vc, vf)):
                row = jnp.broadcast_to(new[pl.ds(b, 1), :].astype(BF16), (seq_len, head_dim))
                cache[b] = jnp.where(row_slots == length, row, cache[b])

    with jax.named_scope("wo_wait"):
        wait_for(wo, sem_wo.at[0])
    pending = list(range(rows))

    def updates(count):
        for _ in range(count):
            if pending:
                update(pending.pop(0))

    for h in range(HALVES):
        with jax.named_scope(f"o_wait{h}"):
            exchange_wait(orecv, o_rsem, h)
        oc[h] = orecv[h].reshape(n * half_rows, cols)
        multiplies(h, first_group, False)
        multiplies(h, first_group, True)
        multiplies(h, last_group, False)
        reduce_step(h, 0)
        if h == 0:
            multiplies(h, last_group, True)
    reduce_step(0, 1)
    for h in range(1, HALVES):
        multiplies(h, last_group, True)
        reduce_step(h, 1)
        updates(3)
    for step in range(2, arm):
        for h in range(HALVES):
            reduce_step(h, step)
            updates(4)
    updates(rows)
    for h in range(HALVES):
        finish(h)

    with jax.named_scope("tail"):
        wait_for(qs.at[:, :, pl.ds(0, n - 1)], q_ssem.at[0])
        wait_for(osend.at[:, pl.ds(0, n - 1)], o_ssem.at[0])
        wait_for(ps, p_ssem.at[0])
        wait_for(rs, r_ssem.at[0])


def write_kernel(y, kc, vc, y_out, k_out, v_out, sem):
    rows = kc.shape[0] // WRITES
    copies = [pltpu.make_async_copy(y, y_out, sem.at[0])]
    for i in range(WRITES):
        span = pl.ds(i * rows, rows)
        copies.append(pltpu.make_async_copy(kc.at[span], k_out.at[span], sem.at[1 + 2 * i]))
        copies.append(pltpu.make_async_copy(vc.at[span], v_out.at[span], sem.at[2 + 2 * i]))
    for copy in copies:
        copy.start()
    for copy in copies:
        copy.wait()


def solution(mesh):
    n = mesh.shape["tp"]
    cache_spec = P(("dp", "tp"), None, None)

    def local_step(hidden, w_query, w_key, w_value, w_out, k_cache, v_cache, lengths):
        rows, seq_len, head_dim = k_cache.shape
        batch, depth = hidden.shape
        cols = w_query.shape[1]
        half_rows = rows // HALVES
        chips = n // 2
        heads = cols * n // head_dim
        half_dim = head_dim // 2
        inv_freq = 10000.0 ** (-(jnp.arange(half_dim, dtype=F32) * 2.0) / head_dim)
        hbm_spec = pl.BlockSpec(memory_space=pltpu.HBM)
        vmem_spec = pl.BlockSpec(memory_space=pltpu.VMEM)
        dma = pltpu.SemaphoreType.DMA
        piece = (n * half_rows, cols // 2)
        y, k_vmem, v_vmem = pl.pallas_call(
            functools.partial(decode_kernel, n),
            out_shape=(
                jax.ShapeDtypeStruct((n, HALVES, half_rows, cols), BF16),
                jax.ShapeDtypeStruct(k_cache.shape, BF16),
                jax.ShapeDtypeStruct(v_cache.shape, BF16),
            ),
            in_specs=[hbm_spec] * 8 + [vmem_spec],
            out_specs=(vmem_spec, vmem_spec, vmem_spec),
            scratch_shapes=[
                pltpu.VMEM((batch, depth), BF16),
                pltpu.VMEM((depth, cols), BF16),
                pltpu.VMEM((depth, head_dim), BF16),
                pltpu.VMEM((depth, head_dim), BF16),
                pltpu.VMEM(w_out.shape, BF16),
                pltpu.SMEM((batch,), jnp.int32),
                pltpu.VMEM((2, batch, head_dim), F32),
                pltpu.VMEM((HALVES, cols // head_dim, n, half_rows, head_dim), BF16),
                pltpu.VMEM((HALVES, cols // head_dim, n, half_rows, head_dim), BF16),
                pltpu.VMEM((half_rows * heads, half_dim), F32),
                pltpu.VMEM((half_rows * heads, half_dim), F32),
                pltpu.VMEM((half_rows * heads, half_dim), F32),
                pltpu.VMEM((half_rows * heads, half_dim), F32),
                pltpu.VMEM((half_rows * heads, seq_len), F32),
                pltpu.VMEM((half_rows * heads, seq_len), BF16),
                pltpu.VMEM((HALVES, n, half_rows, cols), BF16),
                pltpu.VMEM((HALVES, n, half_rows, cols), BF16),
                pltpu.VMEM((HALVES, n * half_rows, cols), BF16),
                pltpu.VMEM((rows, half_dim), F32),
                pltpu.VMEM((rows, half_dim), F32),
                pltpu.VMEM((rows, head_dim), F32),
                pltpu.VMEM((rows, head_dim), F32),
                pltpu.VMEM((HALVES, chips, 2) + piece, F32),
                pltpu.VMEM((HALVES, chips, 2) + piece, BF16),
                pltpu.VMEM((HALVES, chips, 2) + piece, BF16),
                pltpu.VMEM((HALVES, 2, chips - 1) + piece, BF16),
                pltpu.VMEM((HALVES, 2, chips - 1) + piece, BF16),
                dma((1,)),
                dma((cols // head_dim, K_CHUNKS)),
                dma((K_CHUNKS // 2,)),
                dma((HALVES,)),
                dma((1,)),
                dma((1,)),
                dma((HALVES,)),
                dma((1,)),
                dma((HALVES,)),
                dma((1,)),
                dma((HALVES, 4)),
                dma((1,)),
                dma((HALVES, 2, chips - 1)),
            ],
            compiler_params=pltpu.CompilerParams(
                collective_id=0, has_side_effects=True, vmem_limit_bytes=45 * 1024 * 1024
            ),
        )(hidden, w_query, w_key, w_value, w_out, k_cache, v_cache, pltpu.with_memory_space_constraint(lengths, pltpu.HBM), inv_freq[None, :])
        y, k_out, v_out = pl.pallas_call(
            write_kernel,
            out_shape=tuple(jax.ShapeDtypeStruct(a.shape, BF16) for a in (y, k_vmem, v_vmem)),
            in_specs=[vmem_spec] * 3,
            out_specs=(hbm_spec,) * 3,
            scratch_shapes=[dma((1 + 2 * WRITES,))],
            compiler_params=pltpu.CompilerParams(vmem_limit_bytes=1024 * 1024),
        )(y, k_vmem, v_vmem)
        return y.reshape(batch, cols), k_out, v_out

    return jax.shard_map(
        local_step,
        mesh=mesh,
        in_specs=(P("dp", None), P(None, "tp"), P(), P(), P("tp", None), cache_spec, cache_spec, P("dp")),
        out_specs=(P("dp", "tp"), cache_spec, cache_spec),
        check_vma=False,
    )
```

```python
import functools

import jax
import jax.numpy as jnp
from jax import lax
from jax.experimental import pallas as pl
from jax.experimental.pallas import tpu as pltpu
from jax.sharding import PartitionSpec as P

MESH = pl.DeviceIdType.MESH
HALVES = 2
K_CHUNKS = 8
IN_FLIGHT = 10 * 1024 * 1024
WRITES = 4
F32 = jnp.float32
BF16 = jnp.bfloat16


def decode_kernel(
    n, hid_hbm, wq_hbm, wk_hbm, wv_hbm, wo_hbm, kc_hbm, vc_hbm, len_hbm, freq_ref,
    y_ref, kc, vc,
    hid, wq, wk, wv, wo, lens, acc, qs, qr, q_lo, q_hi, o_lo, o_hi, s_buf, e_buf, osend, orecv, oc, cos_ref, sin_ref, kf, vf,
    pm, ps, pr, rs, rr,
    sem_len, sem_q, sem_kv, sem_cache, sem_wo,
    q_ssem, q_rsem, o_ssem, o_rsem, p_ssem, p_rsem, r_ssem, r_rsem,
):
    me = lax.axis_index("tp")
    chips = n // 2
    core = lax.rem(me, 2)
    chip = me // 2
    partner = me + 1 - 2 * core
    neighbours = (lax.rem(me + 2, n), lax.rem(me + n - 2, n))

    batch, depth = hid.shape
    cols = wq.shape[1]
    rows = batch // n
    half_rows = rows // HALVES
    seq_len, head_dim = kc.shape[1:]
    half_dim = head_dim // 2
    dev_heads = cols // head_dim
    heads = dev_heads * n
    block = depth // K_CHUNKS
    part = cols // 2
    out_block = wo.shape[1] // 4
    scale = head_dim ** -0.5

    def rows_of(hbm, vmem, sem, size, i):
        return pltpu.make_async_copy(hbm.at[pl.ds(i * size, size)], vmem.at[pl.ds(i * size, size)], sem)

    def columns_of(hbm, vmem, sem, size, i):
        return pltpu.make_async_copy(hbm.at[:, pl.ds(i * size, size)], vmem.at[:, pl.ds(i * size, size)], sem)

    def wait_for(buf, sem):
        pltpu.make_async_copy(buf, buf, sem).wait()

    len_copy = pltpu.make_async_copy(len_hbm, lens, sem_len.at[0])
    pair = 2 * block

    weight_bytes = 2 * block * head_dim
    queue = [
        (2 * (batch + cols) * block, columns_of(hid_hbm, hid, sem_q.at[i], block, i), rows_of(wq_hbm, wq, sem_q.at[i], block, i))
        for i in range(K_CHUNKS)
    ]
    queue += [
        (4 * weight_bytes, rows_of(wk_hbm, wk, sem_kv.at[i], pair, i), rows_of(wv_hbm, wv, sem_kv.at[i], pair, i))
        for i in range(K_CHUNKS // 2)
    ]
    queue += [
        (4 * half_rows * seq_len * head_dim, rows_of(kc_hbm, kc, sem_cache.at[h], half_rows, h), rows_of(vc_hbm, vc, sem_cache.at[h], half_rows, h))
        for h in range(HALVES)
    ]
    queue += [(2 * cols * out_block, columns_of(wo_hbm, wo, sem_wo.at[0], out_block, i)) for i in range(4)]
    q_rows = block + block * batch // cols

    flight = []

    def issue(everything=False):
        while queue and (everything or sum(flight) + queue[0][0] <= IN_FLIGHT):
            size, *copies = queue.pop(0)
            flight.append(size)
            for copy in copies:
                copy.start()

    def landed():
        flight.pop(0)
        issue()

    len_copy.start()
    issue()

    barrier = pltpu.get_barrier_semaphore()
    order = sorted(range(1, n), key=lambda i: (min(i, n - i), i), reverse=True)
    for i in order:
        pl.semaphore_signal(barrier, inc=1, device_id={"tp": lax.rem(me + i, n)}, device_id_type=MESH)

    def exchange(src, dst, send_sem, recv_sem, *at):
        for i in order:
            peer = lax.rem(me + i, n)
            pltpu.make_async_remote_copy(
                src_ref=src.at[(*at, peer)],
                dst_ref=dst.at[(*at, me)],
                send_sem=send_sem.at[0],
                recv_sem=recv_sem.at[at[0]],
                device_id={"tp": peer},
                device_id_type=MESH,
            ).start()
        dst[(*at, me)] = src[(*at, me)]

    with jax.named_scope("q_mm"):
        for i in range(K_CHUNKS):
            wait_for(wq.at[pl.ds(0, q_rows)], sem_q.at[i])
            landed()
            span = pl.ds(i * block, block)
            term = jnp.dot(hid[:, span], wq[span, :], preferred_element_type=F32)
            if i == 0:
                acc[...] = term
            elif i < K_CHUNKS - 1:
                acc[...] += term
            else:
                q_all = (acc[...] + term).reshape(n, HALVES, half_rows, cols)
                for h in range(HALVES):
                    qs[h] = q_all[:, h].astype(BF16)

    with jax.named_scope("q_send0"):
        pl.semaphore_wait(barrier, n - 1)
        exchange(qs, qr, q_ssem, q_rsem, 0)

    with jax.named_scope("angles"):
        len_copy.wait()
        for r in range(rows):
            cos_ref[pl.ds(r, 1), :] = lens[me * rows + r].astype(F32) * freq_ref[...]
        angles = cos_ref[...]
        sin_ref[...] = jnp.sin(angles)
        cos_ref[...] = jnp.cos(angles)

    def exchange_wait(buf, sem, h):
        wait_for(buf.at[h, pl.ds(0, n - 1)], sem.at[h])

    own = pl.ds(pl.multiple_of(me * rows, rows), rows)
    k_sum = jnp.zeros((rows, head_dim), F32)
    v_sum = jnp.zeros((rows, head_dim), F32)
    for i in range(K_CHUNKS // 2):
        with jax.named_scope(f"kv_wait{i}"):
            wait_for(wk.at[pl.ds(0, 2 * pair)], sem_kv.at[i])
        landed()
        span = pl.ds(i * 2 * block, 2 * block)
        h_own = hid[own, span]
        k_sum += jnp.dot(h_own, wk[span, :], preferred_element_type=F32)
        v_sum += jnp.dot(h_own, wv[span, :], preferred_element_type=F32)
        if i == 1:
            with jax.named_scope("q_sendB"):
                for h in range(1, HALVES):
                    exchange(qs, qr, q_ssem, q_rsem, h)
    k_full = k_sum.astype(BF16).astype(F32)
    cosines, sines = cos_ref[...], sin_ref[...]
    k_lo, k_hi = k_full[:, :half_dim], k_full[:, half_dim:]
    k_rot = jnp.concatenate([k_lo * cosines - k_hi * sines, k_hi * cosines + k_lo * sines], axis=-1)
    kf[...] = k_rot.astype(BF16).astype(F32)
    vf[...] = v_sum.astype(BF16).astype(F32)
    issue(everything=True)
    slots = lax.broadcasted_iota(jnp.int32, (heads, seq_len), 1)

    def attend(h):
        with jax.named_scope(f"q_wait{h}"):
            exchange_wait(qr, q_rsem, h)
        with jax.named_scope(f"rope{h}"):
            span = pl.ds(h * half_rows, half_rows)
            cosines, sines = cos_ref[span, :], sin_ref[span, :]
            for src in range(n):
                for j in range(dev_heads):
                    x = qr[h, src, :, pl.ds(j * head_dim, head_dim)].astype(F32)
                    lo, hi = x[:, :half_dim], x[:, half_dim:]
                    place = pl.ds(src * dev_heads + j, half_rows, stride=heads)
                    q_lo[place, :] = lo * cosines - hi * sines
                    q_hi[place, :] = hi * cosines + lo * sines
        with jax.named_scope(f"cache_wait{h}"):
            wait_for(kc.at[pl.ds(0, 2 * half_rows)], sem_cache.at[h])
        with jax.named_scope(f"rows{h}"):
            ats = [pl.ds(r * heads, heads) for r in range(half_rows)]
            news = []
            for r, at in enumerate(ats):
                b = h * half_rows + r
                q = jnp.concatenate([q_lo[at, :], q_hi[at, :]], axis=-1).astype(BF16)
                s_buf[at, :] = lax.dot_general(q, kc[b], (((1,), (1,)), ((), ())), preferred_element_type=F32)
                news.append(jnp.sum(q.astype(F32) * kf[pl.ds(b, 1), :], axis=-1, keepdims=True) * scale)
            sums = []
            for r, at in enumerate(ats):
                length = lens[me * rows + h * half_rows + r]
                s = jnp.where(slots < length, s_buf[at, :] * scale, -1e30)
                top = jnp.maximum(jnp.max(s, axis=-1, keepdims=True), news[r])
                e = jnp.where(slots < length, jnp.exp(s - top), 0.0)
                e_new = jnp.exp(news[r] - top)
                e_buf[at, :] = e.astype(BF16)
                sums.append((e_new, jnp.sum(e, axis=-1, keepdims=True) + e_new))
            for r, at in enumerate(ats):
                b = h * half_rows + r
                e_new, total = sums[r]
                o = jnp.dot(e_buf[at, :], vc[b], preferred_element_type=F32)
                o = (o + e_new.astype(BF16).astype(F32) * vf[pl.ds(b, 1), :]) / total
                o_lo[at, :] = o[:, :half_dim]
                o_hi[at, :] = o[:, half_dim:]
        with jax.named_scope(f"opack{h}"):
            for dst in range(n):
                for j in range(dev_heads):
                    place = pl.ds(dst * dev_heads + j, half_rows, stride=heads)
                    osend[h, dst, :, pl.ds(j * head_dim, half_dim)] = o_lo[place, :].astype(BF16)
                    osend[h, dst, :, pl.ds(j * head_dim + half_dim, half_dim)] = o_hi[place, :].astype(BF16)
        with jax.named_scope(f"o_send{h}"):
            exchange(osend, orecv, o_ssem, o_rsem, h)

    for h in range(HALVES):
        attend(h)

    arm = chips // 2

    first_group = ((0, 0), (0, 1), (1, 1), (2, 0))
    last_group = ((1, 0), (2, 1)) + tuple((j, half) for j in range(3, chips) for half in range(2))

    def partner_copy(h, group, j, half=None):
        at = (h, j) if half is None else (h, j, half)
        return pltpu.make_async_remote_copy(
            src_ref=ps.at[at], dst_ref=pr.at[at], send_sem=p_ssem.at[0], recv_sem=p_rsem.at[h, group],
            device_id={"tp": partner}, device_id_type=MESH,
        )

    def multiplies(h, group, own):
        with jax.named_scope(f"mult{h}_{group[0][0]}_{int(own)}"):
            o_cols = oc[h]

            def products(side, store):
                left = list(group)
                while left:
                    j, half = left.pop(0)
                    whole = bool(left) and left[0][0] == j
                    shift = (1 - 2 * ((j + 1) % 2)) * (arm - (j + 1) // 2)
                    first = (lax.rem(chip + (shift + chips), chips) * 2 + side) * cols + half * part
                    width = cols if whole else part
                    value = jnp.dot(o_cols, wo[:, pl.ds(pl.multiple_of(first, part), width)], preferred_element_type=F32)
                    store(j, half, value[:, :part])
                    if whole:
                        left.pop(0)
                        store(j, 1, value[:, part:])
                        if j == 0 and not own:
                            partner_copy(h, 0, 0).start()

            def store_other(j, half, value):
                ps[h, j, half] = value.astype(BF16)

            def store_mine(j, half, value):
                pm[h, j, half] = value

            if own:
                products(core, store_mine)
                return
            products(1 - core, store_other)
            if group is first_group:
                partner_copy(h, 1, 1, 1).start()
                partner_copy(h, 2, 2, 0).start()
            else:
                partner_copy(h, 3, 1, 0).start()
                partner_copy(h, 3, 2, 1).start()
                for j in range(3, chips):
                    partner_copy(h, 3, j).start()

    def ring_copy(h, way, slot):
        return pltpu.make_async_remote_copy(
            src_ref=rs.at[h, way, slot], dst_ref=rr.at[h, way, slot],
            send_sem=r_ssem.at[0], recv_sem=r_rsem.at[h, way, slot],
            device_id={"tp": neighbours[way]}, device_id_type=MESH,
        )

    met = set()

    def chip_sum(h, j, half):
        group = {(0, 0): 0, (0, 1): 0, (1, 1): 1, (2, 0): 2}.get((j, half), 3)
        if (h, group) not in met:
            met.add((h, group))
            with jax.named_scope(f"pw{h}_{group}"):
                if group == 0:
                    partner_copy(h, 0, 0).wait_recv()
                elif group < 3:
                    partner_copy(h, group, j, half).wait_recv()
                else:
                    wait_for(pr.at[h, pl.ds(0, len(last_group) // 2)], p_rsem.at[h, 3])
        return pm[h, j, half] + pr[h, j, half].astype(F32)

    def arrived(h, way, slot):
        with jax.named_scope(f"rw{h}_{way}_{slot}"):
            ring_copy(h, way, slot).wait_recv()
        return rr[h, way, slot].astype(F32)

    def pass_on(h, way, long, step):
        hops = (arm if long else arm - 1) - step
        slot = step if long else arm + step
        half = way if long else 1 - way
        value = chip_sum(h, 0 if hops == arm else 1 + 2 * (arm - 1 - hops) + way, half)
        if step > 0:
            value = value + arrived(h, way, slot - 1)
        rs[h, way, slot] = value.astype(BF16)
        ring_copy(h, way, slot).start()

    def reduce_step(h, step):
        for long in (True, False):
            for way in range(2):
                if step < (arm if long else arm - 1):
                    pass_on(h, way, long, step)

    def finish(h):
        for half in range(2):
            value = chip_sum(h, chips - 1, half) + arrived(h, 1 - half, 2 * arm - 2) + arrived(h, half, arm - 1)
            y_ref[:, h, :, pl.ds(half * part, part)] = value.reshape(n, half_rows, part).astype(BF16)

    row_slots = lax.broadcasted_iota(jnp.int32, (seq_len, head_dim), 0)

    def update(b):
        with jax.named_scope(f"update{b}"):
            length = lens[me * rows + b]
            for cache, new in ((kc, kf), (vc, vf)):
                row = jnp.broadcast_to(new[pl.ds(b, 1), :].astype(BF16), (seq_len, head_dim))
                cache[b] = jnp.where(row_slots == length, row, cache[b])

    with jax.named_scope("wo_wait"):
        wait_for(wo, sem_wo.at[0])
    pending = list(range(rows))

    def updates(count):
        for _ in range(count):
            if pending:
                update(pending.pop(0))

    for h in range(HALVES):
        with jax.named_scope(f"o_wait{h}"):
            exchange_wait(orecv, o_rsem, h)
        oc[h] = orecv[h].reshape(n * half_rows, cols)
        multiplies(h, first_group, False)
        multiplies(h, first_group, True)
        if h == 0:
            reduce_step(h, 0)
            multiplies(h, last_group, False)
            multiplies(h, last_group, True)
        else:
            multiplies(h, last_group, False)
            reduce_step(h, 0)
    reduce_step(0, 1)
    for h in range(1, HALVES):
        multiplies(h, last_group, True)
        reduce_step(h, 1)
        updates(3)
    for step in range(2, arm):
        for h in range(HALVES):
            reduce_step(h, step)
            updates(4)
    updates(rows)
    for h in range(HALVES):
        finish(h)

    with jax.named_scope("tail"):
        wait_for(qs.at[:, pl.ds(0, n - 1)], q_ssem.at[0])
        wait_for(osend.at[:, pl.ds(0, n - 1)], o_ssem.at[0])
        wait_for(ps, p_ssem.at[0])
        wait_for(rs, r_ssem.at[0])


def write_kernel(y, kc, vc, y_out, k_out, v_out, sem):
    rows = kc.shape[0] // WRITES
    copies = [pltpu.make_async_copy(y, y_out, sem.at[0])]
    for i in range(WRITES):
        span = pl.ds(i * rows, rows)
        copies.append(pltpu.make_async_copy(kc.at[span], k_out.at[span], sem.at[1 + 2 * i]))
        copies.append(pltpu.make_async_copy(vc.at[span], v_out.at[span], sem.at[2 + 2 * i]))
    for copy in copies:
        copy.start()
    for copy in copies:
        copy.wait()


def solution(mesh):
    n = mesh.shape["tp"]
    cache_spec = P(("dp", "tp"), None, None)

    def local_step(hidden, w_query, w_key, w_value, w_out, k_cache, v_cache, lengths):
        rows, seq_len, head_dim = k_cache.shape
        batch, depth = hidden.shape
        cols = w_query.shape[1]
        half_rows = rows // HALVES
        chips = n // 2
        heads = cols * n // head_dim
        half_dim = head_dim // 2
        inv_freq = 10000.0 ** (-(jnp.arange(half_dim, dtype=F32) * 2.0) / head_dim)
        hbm_spec = pl.BlockSpec(memory_space=pltpu.HBM)
        vmem_spec = pl.BlockSpec(memory_space=pltpu.VMEM)
        dma = pltpu.SemaphoreType.DMA
        piece = (n * half_rows, cols // 2)
        y, k_vmem, v_vmem = pl.pallas_call(
            functools.partial(decode_kernel, n),
            out_shape=(
                jax.ShapeDtypeStruct((n, HALVES, half_rows, cols), BF16),
                jax.ShapeDtypeStruct(k_cache.shape, BF16),
                jax.ShapeDtypeStruct(v_cache.shape, BF16),
            ),
            in_specs=[hbm_spec] * 8 + [vmem_spec],
            out_specs=(vmem_spec, vmem_spec, vmem_spec),
            scratch_shapes=[
                pltpu.VMEM((batch, depth), BF16),
                pltpu.VMEM((depth, cols), BF16),
                pltpu.VMEM((depth, head_dim), BF16),
                pltpu.VMEM((depth, head_dim), BF16),
                pltpu.VMEM(w_out.shape, BF16),
                pltpu.SMEM((batch,), jnp.int32),
                pltpu.VMEM((batch, cols), F32),
                pltpu.VMEM((HALVES, n, half_rows, cols), BF16),
                pltpu.VMEM((HALVES, n, half_rows, cols), BF16),
                pltpu.VMEM((half_rows * heads, half_dim), F32),
                pltpu.VMEM((half_rows * heads, half_dim), F32),
                pltpu.VMEM((half_rows * heads, half_dim), F32),
                pltpu.VMEM((half_rows * heads, half_dim), F32),
                pltpu.VMEM((half_rows * heads, seq_len), F32),
                pltpu.VMEM((half_rows * heads, seq_len), BF16),
                pltpu.VMEM((HALVES, n, half_rows, cols), BF16),
                pltpu.VMEM((HALVES, n, half_rows, cols), BF16),
                pltpu.VMEM((HALVES, n * half_rows, cols), BF16),
                pltpu.VMEM((rows, half_dim), F32),
                pltpu.VMEM((rows, half_dim), F32),
                pltpu.VMEM((rows, head_dim), F32),
                pltpu.VMEM((rows, head_dim), F32),
                pltpu.VMEM((HALVES, chips, 2) + piece, F32),
                pltpu.VMEM((HALVES, chips, 2) + piece, BF16),
                pltpu.VMEM((HALVES, chips, 2) + piece, BF16),
                pltpu.VMEM((HALVES, 2, chips - 1) + piece, BF16),
                pltpu.VMEM((HALVES, 2, chips - 1) + piece, BF16),
                dma((1,)),
                dma((K_CHUNKS,)),
                dma((K_CHUNKS // 2,)),
                dma((HALVES,)),
                dma((1,)),
                dma((1,)),
                dma((HALVES,)),
                dma((1,)),
                dma((HALVES,)),
                dma((1,)),
                dma((HALVES, 4)),
                dma((1,)),
                dma((HALVES, 2, chips - 1)),
            ],
            compiler_params=pltpu.CompilerParams(
                collective_id=0, has_side_effects=True, vmem_limit_bytes=45 * 1024 * 1024
            ),
        )(hidden, w_query, w_key, w_value, w_out, k_cache, v_cache, pltpu.with_memory_space_constraint(lengths, pltpu.HBM), inv_freq[None, :])
        y, k_out, v_out = pl.pallas_call(
            write_kernel,
            out_shape=tuple(jax.ShapeDtypeStruct(a.shape, BF16) for a in (y, k_vmem, v_vmem)),
            in_specs=[vmem_spec] * 3,
            out_specs=(hbm_spec,) * 3,
            scratch_shapes=[dma((1 + 2 * WRITES,))],
            compiler_params=pltpu.CompilerParams(vmem_limit_bytes=1024 * 1024),
        )(y, k_vmem, v_vmem)
        return y.reshape(batch, cols), k_out, v_out

    return jax.shard_map(
        local_step,
        mesh=mesh,
        in_specs=(P("dp", None), P(None, "tp"), P(), P(), P("tp", None), cache_spec, cache_spec, P("dp")),
        out_specs=(P("dp", "tp"), cache_spec, cache_spec),
        check_vma=False,
    )
```

```python
import functools

import jax
import jax.numpy as jnp
from jax import lax
from jax.experimental import pallas as pl
from jax.experimental.pallas import tpu as pltpu
from jax.sharding import PartitionSpec as P

MESH = pl.DeviceIdType.MESH
HALVES = 2
K_CHUNKS = 8
IN_FLIGHT = 10 * 1024 * 1024
WRITES = 4
F32 = jnp.float32
BF16 = jnp.bfloat16


def decode_kernel(
    n, hid_hbm, wq_hbm, wk_hbm, wv_hbm, wo_hbm, kc_hbm, vc_hbm, len_hbm, freq_ref,
    y_ref, kc, vc,
    hid, wq, wk, wv, wo, lens, acc, qs, qr, q_lo, q_hi, o_lo, o_hi, s_buf, e_buf, osend, orecv, oc, cos_ref, sin_ref, kf, vf,
    pm, ps, pr, rs, rr,
    sem_len, sem_q, sem_kv, sem_cache, sem_wo,
    q_ssem, q_rsem, o_ssem, o_rsem, p_ssem, p_rsem, r_ssem, r_rsem,
):
    me = lax.axis_index("tp")
    chips = n // 2
    core = lax.rem(me, 2)
    chip = me // 2
    partner = me + 1 - 2 * core
    neighbours = (lax.rem(me + 2, n), lax.rem(me + n - 2, n))

    batch, depth = hid.shape
    cols = wq.shape[1]
    rows = batch // n
    half_rows = rows // HALVES
    seq_len, head_dim = kc.shape[1:]
    half_dim = head_dim // 2
    dev_heads = cols // head_dim
    heads = dev_heads * n
    block = depth // K_CHUNKS
    part = cols // 2
    out_block = wo.shape[1] // 4
    scale = head_dim ** -0.5

    def rows_of(hbm, vmem, sem, size, i):
        return pltpu.make_async_copy(hbm.at[pl.ds(i * size, size)], vmem.at[pl.ds(i * size, size)], sem)

    def columns_of(hbm, vmem, sem, size, i):
        return pltpu.make_async_copy(hbm.at[:, pl.ds(i * size, size)], vmem.at[:, pl.ds(i * size, size)], sem)

    def wait_for(buf, sem):
        pltpu.make_async_copy(buf, buf, sem).wait()

    len_copy = pltpu.make_async_copy(len_hbm, lens, sem_len.at[0])
    pair = 2 * block

    weight_bytes = 2 * block * head_dim
    lone = K_CHUNKS // 2
    tail_columns = pl.ds(head_dim, cols - head_dim)

    def load_q(i, columns, size, sem):
        at = (pl.ds(i * size, size), columns)
        return pltpu.make_async_copy(wq_hbm.at[at], wq.at[at], sem)

    queue = []
    for i in range(K_CHUNKS):
        width = head_dim if i < lone else cols
        queue.append((
            2 * (batch + width) * block,
            columns_of(hid_hbm, hid, sem_q.at[i], block, i),
            load_q(i, pl.ds(0, width), block, sem_q.at[i]),
        ))
    for i in range(lone // 2):
        queue.append((2 * pair * (cols - head_dim), load_q(i, tail_columns, pair, sem_q.at[K_CHUNKS + i])))
    queue += [
        (4 * weight_bytes, rows_of(wk_hbm, wk, sem_kv.at[i], pair, i), rows_of(wv_hbm, wv, sem_kv.at[i], pair, i))
        for i in range(K_CHUNKS // 2)
    ]
    queue += [
        (4 * half_rows * seq_len * head_dim, rows_of(kc_hbm, kc, sem_cache.at[h], half_rows, h), rows_of(vc_hbm, vc, sem_cache.at[h], half_rows, h))
        for h in range(HALVES)
    ]
    queue += [(2 * cols * out_block, columns_of(wo_hbm, wo, sem_wo.at[0], out_block, i)) for i in range(4)]

    flight = []

    def issue(everything=False):
        while queue and (everything or sum(flight) + queue[0][0] <= IN_FLIGHT):
            size, *copies = queue.pop(0)
            flight.append(size)
            for copy in copies:
                copy.start()

    def landed():
        flight.pop(0)
        issue()

    len_copy.start()
    issue()

    barrier = pltpu.get_barrier_semaphore()
    order = sorted(range(1, n), key=lambda i: (min(i, n - i), i), reverse=True)
    for i in order:
        pl.semaphore_signal(barrier, inc=1, device_id={"tp": lax.rem(me + i, n)}, device_id_type=MESH)

    def exchange(src, dst, send_sem, recv_sem, h, *at):
        for i in order:
            peer = lax.rem(me + i, n)
            pltpu.make_async_remote_copy(
                src_ref=src.at[(h, *at, peer)],
                dst_ref=dst.at[(h, *at, me)],
                send_sem=send_sem.at[0],
                recv_sem=recv_sem.at[h],
                device_id={"tp": peer},
                device_id_type=MESH,
            ).start()
        dst[(h, *at, me)] = src[(h, *at, me)]

    def exchange_wait(buf, sem, h):
        wait_for(buf.at[h, pl.ds(0, n - 1)], sem.at[h])

    def pack_q(j, value):
        value = value.reshape(n, HALVES, half_rows, head_dim)
        for h in range(HALVES):
            qs[h, j] = value[:, h].astype(BF16)

    with jax.named_scope("q_mm0"):
        for i in range(K_CHUNKS):
            width = head_dim if i < lone else cols
            wait_for(wq.at[pl.ds(0, block * (batch + width) // cols)], sem_q.at[i])
            landed()
            span = pl.ds(i * block, block)
            term = jnp.dot(hid[:, span], wq[span, pl.ds(0, width)], preferred_element_type=F32)
            if i == 0:
                acc[:, pl.ds(0, width)] = term
            elif i < lone:
                acc[:, pl.ds(0, width)] += term
            else:
                head = acc[:, pl.ds(0, head_dim)] + term[:, :head_dim]
                if i < K_CHUNKS - 1:
                    acc[:, pl.ds(0, head_dim)] = head
                else:
                    pack_q(0, head)
                rest = term[:, head_dim:]
                acc[:, tail_columns] = rest if i == lone else acc[:, tail_columns] + rest
    with jax.named_scope("q_send0"):
        pl.semaphore_wait(barrier, n - 1)
        exchange(qs, qr, q_ssem, q_rsem, 0, 0)
    with jax.named_scope("q_mm1"):
        for i in range(lone // 2):
            wait_for(wq.at[pl.ds(0, pair * (cols - head_dim) // cols)], sem_q.at[K_CHUNKS + i])
            landed()
            span = pl.ds(i * pair, pair)
            acc[:, tail_columns] += jnp.dot(hid[:, span], wq[span, tail_columns], preferred_element_type=F32)
        for j in range(1, dev_heads):
            pack_q(j, acc[:, pl.ds(j * head_dim, head_dim)])
    with jax.named_scope("q_send1"):
        for j in range(1, dev_heads):
            exchange(qs, qr, q_ssem, q_rsem, 0, j)

    with jax.named_scope("angles"):
        len_copy.wait()
        for r in range(rows):
            cos_ref[pl.ds(r, 1), :] = lens[me * rows + r].astype(F32) * freq_ref[...]
        angles = cos_ref[...]
        sin_ref[...] = jnp.sin(angles)
        cos_ref[...] = jnp.cos(angles)

    def exchange_wait(buf, sem, h):
        wait_for(buf.at[h, pl.ds(0, n - 1)], sem.at[h])

    own = pl.ds(pl.multiple_of(me * rows, rows), rows)
    k_sum = jnp.zeros((rows, head_dim), F32)
    v_sum = jnp.zeros((rows, head_dim), F32)
    for i in range(K_CHUNKS // 2):
        with jax.named_scope(f"kv_wait{i}"):
            wait_for(wk.at[pl.ds(0, 2 * pair)], sem_kv.at[i])
        landed()
        span = pl.ds(i * 2 * block, 2 * block)
        h_own = hid[own, span]
        k_sum += jnp.dot(h_own, wk[span, :], preferred_element_type=F32)
        v_sum += jnp.dot(h_own, wv[span, :], preferred_element_type=F32)
    k_full = k_sum.astype(BF16).astype(F32)
    cosines, sines = cos_ref[...], sin_ref[...]
    k_lo, k_hi = k_full[:, :half_dim], k_full[:, half_dim:]
    k_rot = jnp.concatenate([k_lo * cosines - k_hi * sines, k_hi * cosines + k_lo * sines], axis=-1)
    kf[...] = k_rot.astype(BF16).astype(F32)
    vf[...] = v_sum.astype(BF16).astype(F32)
    issue(everything=True)
    with jax.named_scope("q_sendB"):
        for h in range(1, HALVES):
            exchange(qs, qr, q_ssem, q_rsem, h, slice(None))

    slots = lax.broadcasted_iota(jnp.int32, (heads, seq_len), 1)

    def attend(h):
        with jax.named_scope(f"q_wait{h}"):
            wait_for(qr.at[h, :, pl.ds(0, n - 1)], q_rsem.at[h])
        with jax.named_scope(f"rope{h}"):
            span = pl.ds(h * half_rows, half_rows)
            cosines, sines = cos_ref[span, :], sin_ref[span, :]
            for src in range(n):
                for j in range(dev_heads):
                    x = qr[h, j, src].astype(F32)
                    lo, hi = x[:, :half_dim], x[:, half_dim:]
                    place = pl.ds(src * dev_heads + j, half_rows, stride=heads)
                    q_lo[place, :] = lo * cosines - hi * sines
                    q_hi[place, :] = hi * cosines + lo * sines
        with jax.named_scope(f"cache_wait{h}"):
            wait_for(kc.at[pl.ds(0, 2 * half_rows)], sem_cache.at[h])
        with jax.named_scope(f"rows{h}"):
            ats = [pl.ds(r * heads, heads) for r in range(half_rows)]
            news = []
            for r, at in enumerate(ats):
                b = h * half_rows + r
                q = jnp.concatenate([q_lo[at, :], q_hi[at, :]], axis=-1).astype(BF16)
                s_buf[at, :] = lax.dot_general(q, kc[b], (((1,), (1,)), ((), ())), preferred_element_type=F32)
                news.append(jnp.sum(q.astype(F32) * kf[pl.ds(b, 1), :], axis=-1, keepdims=True) * scale)
            sums = []
            for r, at in enumerate(ats):
                length = lens[me * rows + h * half_rows + r]
                s = jnp.where(slots < length, s_buf[at, :] * scale, -1e30)
                top = jnp.maximum(jnp.max(s, axis=-1, keepdims=True), news[r])
                e = jnp.where(slots < length, jnp.exp(s - top), 0.0)
                e_new = jnp.exp(news[r] - top)
                e_buf[at, :] = e.astype(BF16)
                sums.append((e_new, jnp.sum(e, axis=-1, keepdims=True) + e_new))
            for r, at in enumerate(ats):
                b = h * half_rows + r
                e_new, total = sums[r]
                o = jnp.dot(e_buf[at, :], vc[b], preferred_element_type=F32)
                o = (o + e_new.astype(BF16).astype(F32) * vf[pl.ds(b, 1), :]) / total
                o_lo[at, :] = o[:, :half_dim]
                o_hi[at, :] = o[:, half_dim:]
        with jax.named_scope(f"opack{h}"):
            for dst in range(n):
                for j in range(dev_heads):
                    place = pl.ds(dst * dev_heads + j, half_rows, stride=heads)
                    osend[h, dst, :, pl.ds(j * head_dim, half_dim)] = o_lo[place, :].astype(BF16)
                    osend[h, dst, :, pl.ds(j * head_dim + half_dim, half_dim)] = o_hi[place, :].astype(BF16)
        with jax.named_scope(f"o_send{h}"):
            exchange(osend, orecv, o_ssem, o_rsem, h)

    for h in range(HALVES):
        attend(h)

    arm = chips // 2

    first_group = ((0, 0), (0, 1), (1, 1), (2, 0))
    last_group = ((1, 0), (2, 1)) + tuple((j, half) for j in range(3, chips) for half in range(2))

    def partner_copy(h, group, j, half=None):
        at = (h, j) if half is None else (h, j, half)
        return pltpu.make_async_remote_copy(
            src_ref=ps.at[at], dst_ref=pr.at[at], send_sem=p_ssem.at[0], recv_sem=p_rsem.at[h, group],
            device_id={"tp": partner}, device_id_type=MESH,
        )

    def multiplies(h, group, own):
        with jax.named_scope(f"mult{h}_{group[0][0]}_{int(own)}"):
            o_cols = oc[h]

            def products(side, store):
                left = list(group)
                while left:
                    j, half = left.pop(0)
                    whole = bool(left) and left[0][0] == j
                    shift = (1 - 2 * ((j + 1) % 2)) * (arm - (j + 1) // 2)
                    first = (lax.rem(chip + (shift + chips), chips) * 2 + side) * cols + half * part
                    width = cols if whole else part
                    value = jnp.dot(o_cols, wo[:, pl.ds(pl.multiple_of(first, part), width)], preferred_element_type=F32)
                    store(j, half, value[:, :part])
                    if whole:
                        left.pop(0)
                        store(j, 1, value[:, part:])
                        if j == 0 and not own:
                            partner_copy(h, 0, 0).start()

            def store_other(j, half, value):
                ps[h, j, half] = value.astype(BF16)

            def store_mine(j, half, value):
                pm[h, j, half] = value

            if own:
                products(core, store_mine)
                return
            products(1 - core, store_other)
            if group is first_group:
                partner_copy(h, 1, 1, 1).start()
                partner_copy(h, 2, 2, 0).start()
            else:
                partner_copy(h, 3, 1, 0).start()
                partner_copy(h, 3, 2, 1).start()
                for j in range(3, chips):
                    partner_copy(h, 3, j).start()

    def ring_copy(h, way, slot):
        return pltpu.make_async_remote_copy(
            src_ref=rs.at[h, way, slot], dst_ref=rr.at[h, way, slot],
            send_sem=r_ssem.at[0], recv_sem=r_rsem.at[h, way, slot],
            device_id={"tp": neighbours[way]}, device_id_type=MESH,
        )

    met = set()

    def chip_sum(h, j, half):
        group = {(0, 0): 0, (0, 1): 0, (1, 1): 1, (2, 0): 2}.get((j, half), 3)
        if (h, group) not in met:
            met.add((h, group))
            with jax.named_scope(f"pw{h}_{group}"):
                if group == 0:
                    partner_copy(h, 0, 0).wait_recv()
                elif group < 3:
                    partner_copy(h, group, j, half).wait_recv()
                else:
                    wait_for(pr.at[h, pl.ds(0, len(last_group) // 2)], p_rsem.at[h, 3])
        return pm[h, j, half] + pr[h, j, half].astype(F32)

    def arrived(h, way, slot):
        with jax.named_scope(f"rw{h}_{way}_{slot}"):
            ring_copy(h, way, slot).wait_recv()
        return rr[h, way, slot].astype(F32)

    def pass_on(h, way, long, step):
        hops = (arm if long else arm - 1) - step
        slot = step if long else arm + step
        half = way if long else 1 - way
        value = chip_sum(h, 0 if hops == arm else 1 + 2 * (arm - 1 - hops) + way, half)
        if step > 0:
            value = value + arrived(h, way, slot - 1)
        rs[h, way, slot] = value.astype(BF16)
        ring_copy(h, way, slot).start()

    def reduce_step(h, step):
        for long in (True, False):
            for way in range(2):
                if step < (arm if long else arm - 1):
                    pass_on(h, way, long, step)

    def finish(h):
        for half in range(2):
            value = chip_sum(h, chips - 1, half) + arrived(h, 1 - half, 2 * arm - 2) + arrived(h, half, arm - 1)
            y_ref[:, h, :, pl.ds(half * part, part)] = value.reshape(n, half_rows, part).astype(BF16)

    row_slots = lax.broadcasted_iota(jnp.int32, (seq_len, head_dim), 0)

    def update(b):
        with jax.named_scope(f"update{b}"):
            length = lens[me * rows + b]
            for cache, new in ((kc, kf), (vc, vf)):
                row = jnp.broadcast_to(new[pl.ds(b, 1), :].astype(BF16), (seq_len, head_dim))
                cache[b] = jnp.where(row_slots == length, row, cache[b])

    with jax.named_scope("wo_wait"):
        wait_for(wo, sem_wo.at[0])
    pending = list(range(rows))

    def updates(count):
        for _ in range(count):
            if pending:
                update(pending.pop(0))

    for h in range(HALVES):
        with jax.named_scope(f"o_wait{h}"):
            exchange_wait(orecv, o_rsem, h)
        oc[h] = orecv[h].reshape(n * half_rows, cols)
        multiplies(h, first_group, False)
        multiplies(h, first_group, True)
        if h == 0:
            reduce_step(h, 0)
            multiplies(h, last_group, False)
            multiplies(h, last_group, True)
        else:
            multiplies(h, last_group, False)
            reduce_step(h, 0)
    reduce_step(0, 1)
    for h in range(1, HALVES):
        multiplies(h, last_group, True)
        reduce_step(h, 1)
        updates(3)
    for step in range(2, arm):
        for h in range(HALVES):
            reduce_step(h, step)
            updates(4)
    updates(rows)
    for h in range(HALVES):
        finish(h)

    with jax.named_scope("tail"):
        wait_for(qs.at[:, :, pl.ds(0, n - 1)], q_ssem.at[0])
        wait_for(osend.at[:, pl.ds(0, n - 1)], o_ssem.at[0])
        wait_for(ps, p_ssem.at[0])
        wait_for(rs, r_ssem.at[0])


def write_kernel(y, kc, vc, y_out, k_out, v_out, sem):
    rows = kc.shape[0] // WRITES
    copies = [pltpu.make_async_copy(y, y_out, sem.at[0])]
    for i in range(WRITES):
        span = pl.ds(i * rows, rows)
        copies.append(pltpu.make_async_copy(kc.at[span], k_out.at[span], sem.at[1 + 2 * i]))
        copies.append(pltpu.make_async_copy(vc.at[span], v_out.at[span], sem.at[2 + 2 * i]))
    for copy in copies:
        copy.start()
    for copy in copies:
        copy.wait()


def solution(mesh):
    n = mesh.shape["tp"]
    cache_spec = P(("dp", "tp"), None, None)

    def local_step(hidden, w_query, w_key, w_value, w_out, k_cache, v_cache, lengths):
        rows, seq_len, head_dim = k_cache.shape
        batch, depth = hidden.shape
        cols = w_query.shape[1]
        half_rows = rows // HALVES
        chips = n // 2
        heads = cols * n // head_dim
        half_dim = head_dim // 2
        inv_freq = 10000.0 ** (-(jnp.arange(half_dim, dtype=F32) * 2.0) / head_dim)
        hbm_spec = pl.BlockSpec(memory_space=pltpu.HBM)
        vmem_spec = pl.BlockSpec(memory_space=pltpu.VMEM)
        dma = pltpu.SemaphoreType.DMA
        piece = (n * half_rows, cols // 2)
        y, k_vmem, v_vmem = pl.pallas_call(
            functools.partial(decode_kernel, n),
            out_shape=(
                jax.ShapeDtypeStruct((n, HALVES, half_rows, cols), BF16),
                jax.ShapeDtypeStruct(k_cache.shape, BF16),
                jax.ShapeDtypeStruct(v_cache.shape, BF16),
            ),
            in_specs=[hbm_spec] * 8 + [vmem_spec],
            out_specs=(vmem_spec, vmem_spec, vmem_spec),
            scratch_shapes=[
                pltpu.VMEM((batch, depth), BF16),
                pltpu.VMEM((depth, cols), BF16),
                pltpu.VMEM((depth, head_dim), BF16),
                pltpu.VMEM((depth, head_dim), BF16),
                pltpu.VMEM(w_out.shape, BF16),
                pltpu.SMEM((batch,), jnp.int32),
                pltpu.VMEM((batch, cols), F32),
                pltpu.VMEM((HALVES, cols // head_dim, n, half_rows, head_dim), BF16),
                pltpu.VMEM((HALVES, cols // head_dim, n, half_rows, head_dim), BF16),
                pltpu.VMEM((half_rows * heads, half_dim), F32),
                pltpu.VMEM((half_rows * heads, half_dim), F32),
                pltpu.VMEM((half_rows * heads, half_dim), F32),
                pltpu.VMEM((half_rows * heads, half_dim), F32),
                pltpu.VMEM((half_rows * heads, seq_len), F32),
                pltpu.VMEM((half_rows * heads, seq_len), BF16),
                pltpu.VMEM((HALVES, n, half_rows, cols), BF16),
                pltpu.VMEM((HALVES, n, half_rows, cols), BF16),
                pltpu.VMEM((HALVES, n * half_rows, cols), BF16),
                pltpu.VMEM((rows, half_dim), F32),
                pltpu.VMEM((rows, half_dim), F32),
                pltpu.VMEM((rows, head_dim), F32),
                pltpu.VMEM((rows, head_dim), F32),
                pltpu.VMEM((HALVES, chips, 2) + piece, F32),
                pltpu.VMEM((HALVES, chips, 2) + piece, BF16),
                pltpu.VMEM((HALVES, chips, 2) + piece, BF16),
                pltpu.VMEM((HALVES, 2, chips - 1) + piece, BF16),
                pltpu.VMEM((HALVES, 2, chips - 1) + piece, BF16),
                dma((1,)),
                dma((K_CHUNKS + K_CHUNKS // 4,)),
                dma((K_CHUNKS // 2,)),
                dma((HALVES,)),
                dma((1,)),
                dma((1,)),
                dma((HALVES,)),
                dma((1,)),
                dma((HALVES,)),
                dma((1,)),
                dma((HALVES, 4)),
                dma((1,)),
                dma((HALVES, 2, chips - 1)),
            ],
            compiler_params=pltpu.CompilerParams(
                collective_id=0, has_side_effects=True, vmem_limit_bytes=45 * 1024 * 1024
            ),
        )(hidden, w_query, w_key, w_value, w_out, k_cache, v_cache, pltpu.with_memory_space_constraint(lengths, pltpu.HBM), inv_freq[None, :])
        y, k_out, v_out = pl.pallas_call(
            write_kernel,
            out_shape=tuple(jax.ShapeDtypeStruct(a.shape, BF16) for a in (y, k_vmem, v_vmem)),
            in_specs=[vmem_spec] * 3,
            out_specs=(hbm_spec,) * 3,
            scratch_shapes=[dma((1 + 2 * WRITES,))],
            compiler_params=pltpu.CompilerParams(vmem_limit_bytes=1024 * 1024),
        )(y, k_vmem, v_vmem)
        return y.reshape(batch, cols), k_out, v_out

    return jax.shard_map(
        local_step,
        mesh=mesh,
        in_specs=(P("dp", None), P(None, "tp"), P(), P(), P("tp", None), cache_spec, cache_spec, P("dp")),
        out_specs=(P("dp", "tp"), cache_spec, cache_spec),
        check_vma=False,
    )
```

```python
import functools

import jax
import jax.numpy as jnp
from jax import lax
from jax.experimental import pallas as pl
from jax.experimental.pallas import tpu as pltpu
from jax.sharding import PartitionSpec as P

MESH = pl.DeviceIdType.MESH
HALVES = 2
K_CHUNKS = 8
IN_FLIGHT = 10 * 1024 * 1024
WRITES = 4
F32 = jnp.float32
BF16 = jnp.bfloat16


def decode_kernel(
    n, hid_hbm, wq_hbm, wk_hbm, wv_hbm, wo_hbm, kc_hbm, vc_hbm, len_hbm, freq_ref,
    y_ref, kc, vc,
    hid, wq, wk, wv, wo, lens, acc, qs, qr, q_lo, q_hi, o_lo, o_hi, s_buf, e_buf, osend, orecv, oc, cos_ref, sin_ref, kf, vf,
    pm, ps, pr, rs, rr,
    sem_len, sem_q, sem_kv, sem_cache, sem_wo,
    q_ssem, q_rsem, o_ssem, o_rsem, p_ssem, p_rsem, r_ssem, r_rsem,
):
    me = lax.axis_index("tp")
    chips = n // 2
    core = lax.rem(me, 2)
    chip = me // 2
    partner = me + 1 - 2 * core
    neighbours = (lax.rem(me + 2, n), lax.rem(me + n - 2, n))

    batch, depth = hid.shape
    cols = wq.shape[1]
    rows = batch // n
    half_rows = rows // HALVES
    seq_len, head_dim = kc.shape[1:]
    half_dim = head_dim // 2
    dev_heads = cols // head_dim
    heads = dev_heads * n
    block = depth // K_CHUNKS
    part = cols // 2
    out_block = wo.shape[1] // 4
    scale = head_dim ** -0.5

    def rows_of(hbm, vmem, sem, size, i):
        return pltpu.make_async_copy(hbm.at[pl.ds(i * size, size)], vmem.at[pl.ds(i * size, size)], sem)

    def columns_of(hbm, vmem, sem, size, i):
        return pltpu.make_async_copy(hbm.at[:, pl.ds(i * size, size)], vmem.at[:, pl.ds(i * size, size)], sem)

    def wait_for(buf, sem):
        pltpu.make_async_copy(buf, buf, sem).wait()

    len_copy = pltpu.make_async_copy(len_hbm, lens, sem_len.at[0])
    pair = 2 * block

    weight_bytes = 2 * block * head_dim
    lone = K_CHUNKS // 2
    tail_columns = pl.ds(head_dim, cols - head_dim)

    def load_q(i, columns, size, sem):
        at = (pl.ds(i * size, size), columns)
        return pltpu.make_async_copy(wq_hbm.at[at], wq.at[at], sem)

    queue = []
    for i in range(K_CHUNKS):
        width = head_dim if i < lone else cols
        queue.append((
            2 * (batch + width) * block,
            columns_of(hid_hbm, hid, sem_q.at[i], block, i),
            load_q(i, pl.ds(0, width), block, sem_q.at[i]),
        ))
    for i in range(lone // 2):
        queue.append((2 * pair * (cols - head_dim), load_q(i, tail_columns, pair, sem_q.at[K_CHUNKS + i])))
    queue += [
        (4 * weight_bytes, rows_of(wk_hbm, wk, sem_kv.at[i], pair, i), rows_of(wv_hbm, wv, sem_kv.at[i], pair, i))
        for i in range(K_CHUNKS // 2)
    ]
    queue += [
        (4 * half_rows * seq_len * head_dim, rows_of(kc_hbm, kc, sem_cache.at[h], half_rows, h), rows_of(vc_hbm, vc, sem_cache.at[h], half_rows, h))
        for h in range(HALVES)
    ]
    queue += [(2 * cols * out_block, columns_of(wo_hbm, wo, sem_wo.at[0], out_block, i)) for i in range(4)]

    flight = []

    def issue(everything=False):
        while queue and (everything or sum(flight) + queue[0][0] <= IN_FLIGHT):
            size, *copies = queue.pop(0)
            flight.append(size)
            for copy in copies:
                copy.start()

    def landed():
        flight.pop(0)
        issue()

    len_copy.start()
    issue()

    barrier = pltpu.get_barrier_semaphore()
    order = sorted(range(1, n), key=lambda i: (min(i, n - i), i), reverse=True)
    for i in order:
        pl.semaphore_signal(barrier, inc=1, device_id={"tp": lax.rem(me + i, n)}, device_id_type=MESH)

    def exchange(src, dst, send_sem, recv_sem, h, *at):
        for i in order:
            peer = lax.rem(me + i, n)
            pltpu.make_async_remote_copy(
                src_ref=src.at[(h, *at, peer)],
                dst_ref=dst.at[(h, *at, me)],
                send_sem=send_sem.at[0],
                recv_sem=recv_sem.at[h],
                device_id={"tp": peer},
                device_id_type=MESH,
            ).start()
        dst[(h, *at, me)] = src[(h, *at, me)]

    def exchange_wait(buf, sem, h):
        wait_for(buf.at[h, pl.ds(0, n - 1)], sem.at[h])

    def pack_q(j, value):
        value = value.reshape(n, HALVES, half_rows, head_dim)
        for h in range(HALVES):
            qs[h, j] = value[:, h].astype(BF16)

    with jax.named_scope("q_mm0"):
        for i in range(K_CHUNKS):
            width = head_dim if i < lone else cols
            wait_for(wq.at[pl.ds(0, block * (batch + width) // cols)], sem_q.at[i])
            landed()
            span = pl.ds(i * block, block)
            term = jnp.dot(hid[:, span], wq[span, pl.ds(0, width)], preferred_element_type=F32)
            if i == 0:
                acc[:, pl.ds(0, width)] = term
            elif i < lone:
                acc[:, pl.ds(0, width)] += term
            else:
                head = acc[:, pl.ds(0, head_dim)] + term[:, :head_dim]
                if i < K_CHUNKS - 1:
                    acc[:, pl.ds(0, head_dim)] = head
                else:
                    pack_q(0, head)
                rest = term[:, head_dim:]
                acc[:, tail_columns] = rest if i == lone else acc[:, tail_columns] + rest
    with jax.named_scope("q_send0"):
        pl.semaphore_wait(barrier, n - 1)
        exchange(qs, qr, q_ssem, q_rsem, 0, 0)
    with jax.named_scope("q_mm1"):
        for i in range(lone // 2):
            wait_for(wq.at[pl.ds(0, pair * (cols - head_dim) // cols)], sem_q.at[K_CHUNKS + i])
            landed()
            span = pl.ds(i * pair, pair)
            acc[:, tail_columns] += jnp.dot(hid[:, span], wq[span, tail_columns], preferred_element_type=F32)
        for j in range(1, dev_heads):
            pack_q(j, acc[:, pl.ds(j * head_dim, head_dim)])
    with jax.named_scope("q_send1"):
        for j in range(1, dev_heads):
            exchange(qs, qr, q_ssem, q_rsem, 0, j)

    with jax.named_scope("angles"):
        len_copy.wait()
        for r in range(rows):
            cos_ref[pl.ds(r, 1), :] = lens[me * rows + r].astype(F32) * freq_ref[...]
        angles = cos_ref[...]
        sin_ref[...] = jnp.sin(angles)
        cos_ref[...] = jnp.cos(angles)

    def exchange_wait(buf, sem, h):
        wait_for(buf.at[h, pl.ds(0, n - 1)], sem.at[h])

    own = pl.ds(pl.multiple_of(me * rows, rows), rows)
    k_sum = jnp.zeros((rows, head_dim), F32)
    v_sum = jnp.zeros((rows, head_dim), F32)
    for i in range(K_CHUNKS // 2):
        with jax.named_scope(f"kv_wait{i}"):
            wait_for(wk.at[pl.ds(0, 2 * pair)], sem_kv.at[i])
        landed()
        span = pl.ds(i * 2 * block, 2 * block)
        h_own = hid[own, span]
        k_sum += jnp.dot(h_own, wk[span, :], preferred_element_type=F32)
        v_sum += jnp.dot(h_own, wv[span, :], preferred_element_type=F32)
    k_full = k_sum.astype(BF16).astype(F32)
    cosines, sines = cos_ref[...], sin_ref[...]
    k_lo, k_hi = k_full[:, :half_dim], k_full[:, half_dim:]
    k_rot = jnp.concatenate([k_lo * cosines - k_hi * sines, k_hi * cosines + k_lo * sines], axis=-1)
    kf[...] = k_rot.astype(BF16).astype(F32)
    vf[...] = v_sum.astype(BF16).astype(F32)
    issue(everything=True)
    with jax.named_scope("q_sendB"):
        for h in range(1, HALVES):
            for j in range(dev_heads):
                exchange(qs, qr, q_ssem, q_rsem, h, j)

    slots = lax.broadcasted_iota(jnp.int32, (heads, seq_len), 1)

    def attend(h):
        with jax.named_scope(f"q_wait{h}"):
            wait_for(qr.at[h, :, pl.ds(0, n - 1)], q_rsem.at[h])
        with jax.named_scope(f"rope{h}"):
            span = pl.ds(h * half_rows, half_rows)
            cosines, sines = cos_ref[span, :], sin_ref[span, :]
            for src in range(n):
                for j in range(dev_heads):
                    x = qr[h, j, src].astype(F32)
                    lo, hi = x[:, :half_dim], x[:, half_dim:]
                    place = pl.ds(src * dev_heads + j, half_rows, stride=heads)
                    q_lo[place, :] = lo * cosines - hi * sines
                    q_hi[place, :] = hi * cosines + lo * sines
        with jax.named_scope(f"cache_wait{h}"):
            wait_for(kc.at[pl.ds(0, 2 * half_rows)], sem_cache.at[h])
        with jax.named_scope(f"rows{h}"):
            ats = [pl.ds(r * heads, heads) for r in range(half_rows)]
            news = []
            for r, at in enumerate(ats):
                b = h * half_rows + r
                q = jnp.concatenate([q_lo[at, :], q_hi[at, :]], axis=-1).astype(BF16)
                s_buf[at, :] = lax.dot_general(q, kc[b], (((1,), (1,)), ((), ())), preferred_element_type=F32)
                news.append(jnp.sum(q.astype(F32) * kf[pl.ds(b, 1), :], axis=-1, keepdims=True) * scale)
            sums = []
            for r, at in enumerate(ats):
                length = lens[me * rows + h * half_rows + r]
                s = jnp.where(slots < length, s_buf[at, :] * scale, -1e30)
                top = jnp.maximum(jnp.max(s, axis=-1, keepdims=True), news[r])
                e = jnp.where(slots < length, jnp.exp(s - top), 0.0)
                e_new = jnp.exp(news[r] - top)
                e_buf[at, :] = e.astype(BF16)
                sums.append((e_new, jnp.sum(e, axis=-1, keepdims=True) + e_new))
            for r, at in enumerate(ats):
                b = h * half_rows + r
                e_new, total = sums[r]
                o = jnp.dot(e_buf[at, :], vc[b], preferred_element_type=F32)
                o = (o + e_new.astype(BF16).astype(F32) * vf[pl.ds(b, 1), :]) / total
                o_lo[at, :] = o[:, :half_dim]
                o_hi[at, :] = o[:, half_dim:]
        with jax.named_scope(f"opack{h}"):
            for dst in range(n):
                for j in range(dev_heads):
                    place = pl.ds(dst * dev_heads + j, half_rows, stride=heads)
                    osend[h, dst, :, pl.ds(j * head_dim, half_dim)] = o_lo[place, :].astype(BF16)
                    osend[h, dst, :, pl.ds(j * head_dim + half_dim, half_dim)] = o_hi[place, :].astype(BF16)
        with jax.named_scope(f"o_send{h}"):
            exchange(osend, orecv, o_ssem, o_rsem, h)

    for h in range(HALVES):
        attend(h)

    arm = chips // 2

    first_group = ((0, 0), (0, 1), (1, 1), (2, 0))
    last_group = ((1, 0), (2, 1)) + tuple((j, half) for j in range(3, chips) for half in range(2))

    def partner_copy(h, group, j, half=None):
        at = (h, j) if half is None else (h, j, half)
        return pltpu.make_async_remote_copy(
            src_ref=ps.at[at], dst_ref=pr.at[at], send_sem=p_ssem.at[0], recv_sem=p_rsem.at[h, group],
            device_id={"tp": partner}, device_id_type=MESH,
        )

    def multiplies(h, group, own):
        with jax.named_scope(f"mult{h}_{group[0][0]}_{int(own)}"):
            o_cols = oc[h]

            def products(side, store):
                left = list(group)
                while left:
                    j, half = left.pop(0)
                    whole = bool(left) and left[0][0] == j
                    shift = (1 - 2 * ((j + 1) % 2)) * (arm - (j + 1) // 2)
                    first = (lax.rem(chip + (shift + chips), chips) * 2 + side) * cols + half * part
                    width = cols if whole else part
                    value = jnp.dot(o_cols, wo[:, pl.ds(pl.multiple_of(first, part), width)], preferred_element_type=F32)
                    store(j, half, value[:, :part])
                    if whole:
                        left.pop(0)
                        store(j, 1, value[:, part:])
                        if j == 0 and not own:
                            partner_copy(h, 0, 0).start()

            def store_other(j, half, value):
                ps[h, j, half] = value.astype(BF16)

            def store_mine(j, half, value):
                pm[h, j, half] = value

            if own:
                products(core, store_mine)
                return
            products(1 - core, store_other)
            if group is first_group:
                partner_copy(h, 1, 1, 1).start()
                partner_copy(h, 2, 2, 0).start()
            else:
                partner_copy(h, 3, 1, 0).start()
                partner_copy(h, 3, 2, 1).start()
                for j in range(3, chips):
                    partner_copy(h, 3, j).start()

    def ring_copy(h, way, slot):
        return pltpu.make_async_remote_copy(
            src_ref=rs.at[h, way, slot], dst_ref=rr.at[h, way, slot],
            send_sem=r_ssem.at[0], recv_sem=r_rsem.at[h, way, slot],
            device_id={"tp": neighbours[way]}, device_id_type=MESH,
        )

    met = set()

    def chip_sum(h, j, half):
        group = {(0, 0): 0, (0, 1): 0, (1, 1): 1, (2, 0): 2}.get((j, half), 3)
        if (h, group) not in met:
            met.add((h, group))
            with jax.named_scope(f"pw{h}_{group}"):
                if group == 0:
                    partner_copy(h, 0, 0).wait_recv()
                elif group < 3:
                    partner_copy(h, group, j, half).wait_recv()
                else:
                    wait_for(pr.at[h, pl.ds(0, len(last_group) // 2)], p_rsem.at[h, 3])
        return pm[h, j, half] + pr[h, j, half].astype(F32)

    def arrived(h, way, slot):
        with jax.named_scope(f"rw{h}_{way}_{slot}"):
            ring_copy(h, way, slot).wait_recv()
        return rr[h, way, slot].astype(F32)

    def pass_on(h, way, long, step):
        hops = (arm if long else arm - 1) - step
        slot = step if long else arm + step
        half = way if long else 1 - way
        value = chip_sum(h, 0 if hops == arm else 1 + 2 * (arm - 1 - hops) + way, half)
        if step > 0:
            value = value + arrived(h, way, slot - 1)
        rs[h, way, slot] = value.astype(BF16)
        ring_copy(h, way, slot).start()

    def reduce_step(h, step):
        for long in (True, False):
            for way in range(2):
                if step < (arm if long else arm - 1):
                    pass_on(h, way, long, step)

    def finish(h):
        for half in range(2):
            value = chip_sum(h, chips - 1, half) + arrived(h, 1 - half, 2 * arm - 2) + arrived(h, half, arm - 1)
            y_ref[:, h, :, pl.ds(half * part, part)] = value.reshape(n, half_rows, part).astype(BF16)

    row_slots = lax.broadcasted_iota(jnp.int32, (seq_len, head_dim), 0)

    def update(b):
        with jax.named_scope(f"update{b}"):
            length = lens[me * rows + b]
            for cache, new in ((kc, kf), (vc, vf)):
                row = jnp.broadcast_to(new[pl.ds(b, 1), :].astype(BF16), (seq_len, head_dim))
                cache[b] = jnp.where(row_slots == length, row, cache[b])

    with jax.named_scope("wo_wait"):
        wait_for(wo, sem_wo.at[0])
    pending = list(range(rows))

    def updates(count):
        for _ in range(count):
            if pending:
                update(pending.pop(0))

    for h in range(HALVES):
        with jax.named_scope(f"o_wait{h}"):
            exchange_wait(orecv, o_rsem, h)
        oc[h] = orecv[h].reshape(n * half_rows, cols)
        multiplies(h, first_group, False)
        multiplies(h, first_group, True)
        if h == 0:
            reduce_step(h, 0)
            multiplies(h, last_group, False)
            multiplies(h, last_group, True)
        else:
            multiplies(h, last_group, False)
            reduce_step(h, 0)
    reduce_step(0, 1)
    for h in range(1, HALVES):
        multiplies(h, last_group, True)
        reduce_step(h, 1)
        updates(3)
    for step in range(2, arm):
        for h in range(HALVES):
            reduce_step(h, step)
            updates(4)
    updates(rows)
    for h in range(HALVES):
        finish(h)

    with jax.named_scope("tail"):
        wait_for(qs.at[:, :, pl.ds(0, n - 1)], q_ssem.at[0])
        wait_for(osend.at[:, pl.ds(0, n - 1)], o_ssem.at[0])
        wait_for(ps, p_ssem.at[0])
        wait_for(rs, r_ssem.at[0])


def write_kernel(y, kc, vc, y_out, k_out, v_out, sem):
    rows = kc.shape[0] // WRITES
    copies = [pltpu.make_async_copy(y, y_out, sem.at[0])]
    for i in range(WRITES):
        span = pl.ds(i * rows, rows)
        copies.append(pltpu.make_async_copy(kc.at[span], k_out.at[span], sem.at[1 + 2 * i]))
        copies.append(pltpu.make_async_copy(vc.at[span], v_out.at[span], sem.at[2 + 2 * i]))
    for copy in copies:
        copy.start()
    for copy in copies:
        copy.wait()


def solution(mesh):
    n = mesh.shape["tp"]
    cache_spec = P(("dp", "tp"), None, None)

    def local_step(hidden, w_query, w_key, w_value, w_out, k_cache, v_cache, lengths):
        rows, seq_len, head_dim = k_cache.shape
        batch, depth = hidden.shape
        cols = w_query.shape[1]
        half_rows = rows // HALVES
        chips = n // 2
        heads = cols * n // head_dim
        half_dim = head_dim // 2
        inv_freq = 10000.0 ** (-(jnp.arange(half_dim, dtype=F32) * 2.0) / head_dim)
        hbm_spec = pl.BlockSpec(memory_space=pltpu.HBM)
        vmem_spec = pl.BlockSpec(memory_space=pltpu.VMEM)
        dma = pltpu.SemaphoreType.DMA
        piece = (n * half_rows, cols // 2)
        y, k_vmem, v_vmem = pl.pallas_call(
            functools.partial(decode_kernel, n),
            out_shape=(
                jax.ShapeDtypeStruct((n, HALVES, half_rows, cols), BF16),
                jax.ShapeDtypeStruct(k_cache.shape, BF16),
                jax.ShapeDtypeStruct(v_cache.shape, BF16),
            ),
            in_specs=[hbm_spec] * 8 + [vmem_spec],
            out_specs=(vmem_spec, vmem_spec, vmem_spec),
            scratch_shapes=[
                pltpu.VMEM((batch, depth), BF16),
                pltpu.VMEM((depth, cols), BF16),
                pltpu.VMEM((depth, head_dim), BF16),
                pltpu.VMEM((depth, head_dim), BF16),
                pltpu.VMEM(w_out.shape, BF16),
                pltpu.SMEM((batch,), jnp.int32),
                pltpu.VMEM((batch, cols), F32),
                pltpu.VMEM((HALVES, cols // head_dim, n, half_rows, head_dim), BF16),
                pltpu.VMEM((HALVES, cols // head_dim, n, half_rows, head_dim), BF16),
                pltpu.VMEM((half_rows * heads, half_dim), F32),
                pltpu.VMEM((half_rows * heads, half_dim), F32),
                pltpu.VMEM((half_rows * heads, half_dim), F32),
                pltpu.VMEM((half_rows * heads, half_dim), F32),
                pltpu.VMEM((half_rows * heads, seq_len), F32),
                pltpu.VMEM((half_rows * heads, seq_len), BF16),
                pltpu.VMEM((HALVES, n, half_rows, cols), BF16),
                pltpu.VMEM((HALVES, n, half_rows, cols), BF16),
                pltpu.VMEM((HALVES, n * half_rows, cols), BF16),
                pltpu.VMEM((rows, half_dim), F32),
                pltpu.VMEM((rows, half_dim), F32),
                pltpu.VMEM((rows, head_dim), F32),
                pltpu.VMEM((rows, head_dim), F32),
                pltpu.VMEM((HALVES, chips, 2) + piece, F32),
                pltpu.VMEM((HALVES, chips, 2) + piece, BF16),
                pltpu.VMEM((HALVES, chips, 2) + piece, BF16),
                pltpu.VMEM((HALVES, 2, chips - 1) + piece, BF16),
                pltpu.VMEM((HALVES, 2, chips - 1) + piece, BF16),
                dma((1,)),
                dma((K_CHUNKS + K_CHUNKS // 4,)),
                dma((K_CHUNKS // 2,)),
                dma((HALVES,)),
                dma((1,)),
                dma((1,)),
                dma((HALVES,)),
                dma((1,)),
                dma((HALVES,)),
                dma((1,)),
                dma((HALVES, 4)),
                dma((1,)),
                dma((HALVES, 2, chips - 1)),
            ],
            compiler_params=pltpu.CompilerParams(
                collective_id=0, has_side_effects=True, vmem_limit_bytes=45 * 1024 * 1024
            ),
        )(hidden, w_query, w_key, w_value, w_out, k_cache, v_cache, pltpu.with_memory_space_constraint(lengths, pltpu.HBM), inv_freq[None, :])
        y, k_out, v_out = pl.pallas_call(
            write_kernel,
            out_shape=tuple(jax.ShapeDtypeStruct(a.shape, BF16) for a in (y, k_vmem, v_vmem)),
            in_specs=[vmem_spec] * 3,
            out_specs=(hbm_spec,) * 3,
            scratch_shapes=[dma((1 + 2 * WRITES,))],
            compiler_params=pltpu.CompilerParams(vmem_limit_bytes=1024 * 1024),
        )(y, k_vmem, v_vmem)
        return y.reshape(batch, cols), k_out, v_out

    return jax.shard_map(
        local_step,
        mesh=mesh,
        in_specs=(P("dp", None), P(None, "tp"), P(), P(), P("tp", None), cache_spec, cache_spec, P("dp")),
        out_specs=(P("dp", "tp"), cache_spec, cache_spec),
        check_vma=False,
    )
```

```python
import functools

import jax
import jax.numpy as jnp
from jax import lax
from jax.experimental import pallas as pl
from jax.experimental.pallas import tpu as pltpu
from jax.sharding import PartitionSpec as P

MESH = pl.DeviceIdType.MESH
HALVES = 2
K_CHUNKS = 8
AHEAD = 8
WRITES = 8
F32 = jnp.float32
BF16 = jnp.bfloat16


def decode_kernel(
    n, hid_hbm, wq_hbm, wk_hbm, wv_hbm, wo_hbm, kc_hbm, vc_hbm, len_hbm, freq_ref,
    y_ref, kc, vc,
    hid, wq, wk, wv, wo, lens, acc, qs, qr, q_lo, q_hi, o_lo, o_hi, s_buf, e_buf, osend, orecv, oc, cos_ref, sin_ref, kf, vf,
    pm, ps, pr, rs, rr,
    sem_len, sem_q, sem_kv, sem_cache, sem_wo,
    q_ssem, q_rsem, o_ssem, o_rsem, p_ssem, p_rsem, r_ssem, r_rsem,
):
    me = lax.axis_index("tp")
    chips = n // 2
    core = lax.rem(me, 2)
    chip = me // 2
    partner = me + 1 - 2 * core
    neighbours = (lax.rem(me + 2, n), lax.rem(me + n - 2, n))

    batch, depth = hid.shape
    cols = wq.shape[1]
    rows = batch // n
    half_rows = rows // HALVES
    seq_len, head_dim = kc.shape[1:]
    half_dim = head_dim // 2
    dev_heads = cols // head_dim
    heads = dev_heads * n
    block = depth // K_CHUNKS
    part = cols // 2
    out_block = wo.shape[1] // 4
    scale = head_dim ** -0.5

    def rows_of(hbm, vmem, sem, size, i):
        return pltpu.make_async_copy(hbm.at[pl.ds(i * size, size)], vmem.at[pl.ds(i * size, size)], sem)

    def columns_of(hbm, vmem, sem, size, i):
        return pltpu.make_async_copy(hbm.at[:, pl.ds(i * size, size)], vmem.at[:, pl.ds(i * size, size)], sem)

    def wait_for(buf, sem):
        pltpu.make_async_copy(buf, buf, sem).wait()

    len_copy = pltpu.make_async_copy(len_hbm, lens, sem_len.at[0])
    pair = 2 * block

    def load_q(j, size, i):
        at = (pl.ds(i * size, size), pl.ds(j * head_dim, head_dim))
        return pltpu.make_async_copy(wq_hbm.at[at], wq.at[at], sem_q.at[j, i])

    queue = [(columns_of(hid_hbm, hid, sem_q.at[0, i], block, i), load_q(0, block, i)) for i in range(K_CHUNKS)]
    queue += [(load_q(j, pair, i),) for j in range(1, dev_heads) for i in range(K_CHUNKS // 2)]
    queue += [
        (rows_of(wk_hbm, wk, sem_kv.at[i], pair, i), rows_of(wv_hbm, wv, sem_kv.at[i], pair, i))
        for i in range(K_CHUNKS // 2)
    ]
    queue += [
        (rows_of(kc_hbm, kc, sem_cache.at[h], half_rows, h), rows_of(vc_hbm, vc, sem_cache.at[h], half_rows, h))
        for h in range(HALVES)
    ]
    queue += [(columns_of(wo_hbm, wo, sem_wo.at[0], out_block, i),) for i in range(4)]
    first_rows = block // dev_heads + block * batch // cols

    def issue(count):
        for _ in range(count):
            if queue:
                for copy in queue.pop(0):
                    copy.start()

    len_copy.start()
    issue(AHEAD)

    barrier = pltpu.get_barrier_semaphore()
    order = sorted(range(1, n), key=lambda i: (min(i, n - i), i), reverse=True)
    for i in order:
        pl.semaphore_signal(barrier, inc=1, device_id={"tp": lax.rem(me + i, n)}, device_id_type=MESH)

    def exchange(src, dst, send_sem, recv_sem, *at):
        for i in order:
            peer = lax.rem(me + i, n)
            pltpu.make_async_remote_copy(
                src_ref=src.at[(*at, peer)],
                dst_ref=dst.at[(*at, me)],
                send_sem=send_sem.at[0],
                recv_sem=recv_sem.at[at[0]],
                device_id={"tp": peer},
                device_id_type=MESH,
            ).start()
        dst[(*at, me)] = src[(*at, me)]

    for j in range(dev_heads):
        size, count = (block, K_CHUNKS) if j == 0 else (pair, K_CHUNKS // 2)
        with jax.named_scope(f"q_mm{j}"):
            for i in range(count):
                wait_for(wq.at[pl.ds(0, first_rows if j == 0 else pair // dev_heads)], sem_q.at[j, i])
                issue(1)
                terms = []
                for way in range(2):
                    span = pl.ds(i * size + way * (size // 2), size // 2)
                    terms.append(jnp.dot(hid[:, span], wq[span, pl.ds(j * head_dim, head_dim)], preferred_element_type=F32))
                if i < count - 1:
                    for way in range(2):
                        acc[way] = terms[way] if i == 0 else acc[way] + terms[way]
                else:
                    q_all = ((acc[0] + terms[0]) + (acc[1] + terms[1])).reshape(n, HALVES, half_rows, head_dim)
                    for h in range(HALVES):
                        qs[h, j] = q_all[:, h].astype(BF16)
        with jax.named_scope(f"q_send{j}"):
            if j == 0:
                pl.semaphore_wait(barrier, n - 1)
            exchange(qs, qr, q_ssem, q_rsem, 0, j)

    with jax.named_scope("angles"):
        len_copy.wait()
        for r in range(rows):
            cos_ref[pl.ds(r, 1), :] = lens[me * rows + r].astype(F32) * freq_ref[...]
        angles = cos_ref[...]
        sin_ref[...] = jnp.sin(angles)
        cos_ref[...] = jnp.cos(angles)

    def exchange_wait(buf, sem, h):
        wait_for(buf.at[h, pl.ds(0, n - 1)], sem.at[h])

    own = pl.ds(pl.multiple_of(me * rows, rows), rows)
    k_sum = jnp.zeros((rows, head_dim), F32)
    v_sum = jnp.zeros((rows, head_dim), F32)
    for i in range(K_CHUNKS // 2):
        with jax.named_scope(f"kv_wait{i}"):
            wait_for(wk.at[pl.ds(0, 2 * pair)], sem_kv.at[i])
        issue(1)
        span = pl.ds(i * 2 * block, 2 * block)
        h_own = hid[own, span]
        k_sum += jnp.dot(h_own, wk[span, :], preferred_element_type=F32)
        v_sum += jnp.dot(h_own, wv[span, :], preferred_element_type=F32)
    k_full = k_sum.astype(BF16).astype(F32)
    cosines, sines = cos_ref[...], sin_ref[...]
    k_lo, k_hi = k_full[:, :half_dim], k_full[:, half_dim:]
    k_rot = jnp.concatenate([k_lo * cosines - k_hi * sines, k_hi * cosines + k_lo * sines], axis=-1)
    kf[...] = k_rot.astype(BF16).astype(F32)
    vf[...] = v_sum.astype(BF16).astype(F32)
    issue(len(queue))
    with jax.named_scope("q_sendB"):
        for h in range(1, HALVES):
            for j in range(dev_heads):
                exchange(qs, qr, q_ssem, q_rsem, h, j)

    slots = lax.broadcasted_iota(jnp.int32, (heads, seq_len), 1)

    def attend(h):
        with jax.named_scope(f"q_wait{h}"):
            wait_for(qr.at[h, :, pl.ds(0, n - 1)], q_rsem.at[h])
        with jax.named_scope(f"rope{h}"):
            span = pl.ds(h * half_rows, half_rows)
            cosines, sines = cos_ref[span, :], sin_ref[span, :]
            for src in range(n):
                for j in range(dev_heads):
                    x = qr[h, j, src].astype(F32)
                    lo, hi = x[:, :half_dim], x[:, half_dim:]
                    place = pl.ds(src * dev_heads + j, half_rows, stride=heads)
                    q_lo[place, :] = lo * cosines - hi * sines
                    q_hi[place, :] = hi * cosines + lo * sines
        with jax.named_scope(f"cache_wait{h}"):
            wait_for(kc.at[pl.ds(0, 2 * half_rows)], sem_cache.at[h])
        with jax.named_scope(f"rows{h}"):
            ats = [pl.ds(r * heads, heads) for r in range(half_rows)]
            news = []
            for r, at in enumerate(ats):
                b = h * half_rows + r
                q = jnp.concatenate([q_lo[at, :], q_hi[at, :]], axis=-1).astype(BF16)
                s_buf[at, :] = lax.dot_general(q, kc[b], (((1,), (1,)), ((), ())), preferred_element_type=F32)
                news.append(jnp.sum(q.astype(F32) * kf[pl.ds(b, 1), :], axis=-1, keepdims=True) * scale)
            sums = []
            for r, at in enumerate(ats):
                length = lens[me * rows + h * half_rows + r]
                s = jnp.where(slots < length, s_buf[at, :] * scale, -1e30)
                top = jnp.maximum(jnp.max(s, axis=-1, keepdims=True), news[r])
                e = jnp.where(slots < length, jnp.exp(s - top), 0.0)
                e_new = jnp.exp(news[r] - top)
                e_buf[at, :] = e.astype(BF16)
                sums.append((e_new, jnp.sum(e, axis=-1, keepdims=True) + e_new))
            for r, at in enumerate(ats):
                b = h * half_rows + r
                e_new, total = sums[r]
                o = jnp.dot(e_buf[at, :], vc[b], preferred_element_type=F32)
                o = (o + e_new.astype(BF16).astype(F32) * vf[pl.ds(b, 1), :]) / total
                o_lo[at, :] = o[:, :half_dim]
                o_hi[at, :] = o[:, half_dim:]
        with jax.named_scope(f"opack{h}"):
            for dst in range(n):
                for j in range(dev_heads):
                    place = pl.ds(dst * dev_heads + j, half_rows, stride=heads)
                    osend[h, dst, :, pl.ds(j * head_dim, half_dim)] = o_lo[place, :].astype(BF16)
                    osend[h, dst, :, pl.ds(j * head_dim + half_dim, half_dim)] = o_hi[place, :].astype(BF16)
        with jax.named_scope(f"o_send{h}"):
            exchange(osend, orecv, o_ssem, o_rsem, h)

    for h in range(HALVES):
        attend(h)

    arm = chips // 2

    first_group = ((0, 0), (0, 1), (1, 1), (2, 0))
    last_group = ((1, 0), (2, 1)) + tuple((j, half) for j in range(3, chips) for half in range(2))

    def partner_copy(h, group, j, half=None):
        at = (h, j) if half is None else (h, j, half)
        return pltpu.make_async_remote_copy(
            src_ref=ps.at[at], dst_ref=pr.at[at], send_sem=p_ssem.at[0], recv_sem=p_rsem.at[h, group],
            device_id={"tp": partner}, device_id_type=MESH,
        )

    def multiplies(h, group, own):
        with jax.named_scope(f"mult{h}_{group[0][0]}_{int(own)}"):
            o_cols = oc[h]

            def products(side, store):
                left = list(group)
                while left:
                    j, half = left.pop(0)
                    whole = j > 0 and bool(left) and left[0][0] == j
                    shift = (1 - 2 * ((j + 1) % 2)) * (arm - (j + 1) // 2)
                    first = (lax.rem(chip + (shift + chips), chips) * 2 + side) * cols + half * part
                    width = cols if whole else part
                    value = jnp.dot(o_cols, wo[:, pl.ds(pl.multiple_of(first, part), width)], preferred_element_type=F32)
                    store(j, half, value[:, :part])
                    if whole:
                        left.pop(0)
                        store(j, 1, value[:, part:])
                    elif j == 0 and not own:
                        partner_copy(h, 4 * half, 0, half).start()

            def store_other(j, half, value):
                ps[h, j, half] = value.astype(BF16)

            def store_mine(j, half, value):
                pm[h, j, half] = value

            if own:
                products(core, store_mine)
                return
            products(1 - core, store_other)
            if group is first_group:
                partner_copy(h, 1, 1, 1).start()
                partner_copy(h, 2, 2, 0).start()
            else:
                partner_copy(h, 3, 1, 0).start()
                partner_copy(h, 3, 2, 1).start()
                for j in range(3, chips):
                    partner_copy(h, 3, j).start()

    def ring_copy(h, way, slot):
        return pltpu.make_async_remote_copy(
            src_ref=rs.at[h, way, slot], dst_ref=rr.at[h, way, slot],
            send_sem=r_ssem.at[0], recv_sem=r_rsem.at[h, way, slot],
            device_id={"tp": neighbours[way]}, device_id_type=MESH,
        )

    met = set()

    def chip_sum(h, j, half):
        group = {(0, 0): 0, (0, 1): 4, (1, 1): 1, (2, 0): 2}.get((j, half), 3)
        if (h, group) not in met:
            met.add((h, group))
            with jax.named_scope(f"pw{h}_{group}"):
                if group != 3:
                    partner_copy(h, group, j, half).wait_recv()
                else:
                    wait_for(pr.at[h, pl.ds(0, len(last_group) // 2)], p_rsem.at[h, 3])
        return pm[h, j, half] + pr[h, j, half].astype(F32)

    def arrived(h, way, slot):
        with jax.named_scope(f"rw{h}_{way}_{slot}"):
            ring_copy(h, way, slot).wait_recv()
        return rr[h, way, slot].astype(F32)

    def pass_on(h, way, long, step):
        hops = (arm if long else arm - 1) - step
        slot = step if long else arm + step
        half = way if long else 1 - way
        value = chip_sum(h, 0 if hops == arm else 1 + 2 * (arm - 1 - hops) + way, half)
        if step > 0:
            value = value + arrived(h, way, slot - 1)
        rs[h, way, slot] = value.astype(BF16)
        ring_copy(h, way, slot).start()

    def reduce_step(h, step):
        for long in (True, False):
            for way in range(2):
                if step < (arm if long else arm - 1):
                    pass_on(h, way, long, step)

    def finish(h):
        for half in range(2):
            value = chip_sum(h, chips - 1, half) + arrived(h, 1 - half, 2 * arm - 2) + arrived(h, half, arm - 1)
            y_ref[:, h, :, pl.ds(half * part, part)] = value.reshape(n, half_rows, part).astype(BF16)

    row_slots = lax.broadcasted_iota(jnp.int32, (seq_len, head_dim), 0)

    def update(b):
        with jax.named_scope(f"update{b}"):
            length = lens[me * rows + b]
            for cache, new in ((kc, kf), (vc, vf)):
                row = jnp.broadcast_to(new[pl.ds(b, 1), :].astype(BF16), (seq_len, head_dim))
                cache[b] = jnp.where(row_slots == length, row, cache[b])

    with jax.named_scope("wo_wait"):
        wait_for(wo, sem_wo.at[0])
    pending = list(range(rows))

    def updates(count):
        for _ in range(count):
            if pending:
                update(pending.pop(0))

    for h in range(HALVES):
        with jax.named_scope(f"o_wait{h}"):
            exchange_wait(orecv, o_rsem, h)
        oc[h] = orecv[h].reshape(n * half_rows, cols)
        multiplies(h, first_group, False)
        multiplies(h, first_group, True)
        if h == 0:
            reduce_step(h, 0)
            multiplies(h, last_group, False)
            multiplies(h, last_group, True)
        else:
            multiplies(h, last_group, False)
            reduce_step(h, 0)
    reduce_step(0, 1)
    for h in range(1, HALVES):
        multiplies(h, last_group, True)
        reduce_step(h, 1)
        updates(3)
    for step in range(2, arm):
        for h in range(HALVES):
            reduce_step(h, step)
            updates(4)
    updates(rows)
    for h in range(HALVES):
        finish(h)

    with jax.named_scope("tail"):
        wait_for(qs.at[:, :, pl.ds(0, n - 1)], q_ssem.at[0])
        wait_for(osend.at[:, pl.ds(0, n - 1)], o_ssem.at[0])
        wait_for(ps, p_ssem.at[0])
        wait_for(rs, r_ssem.at[0])


def write_kernel(y, kc, vc, y_out, k_out, v_out, sem):
    rows = kc.shape[0] // WRITES
    copies = [pltpu.make_async_copy(y, y_out, sem.at[0])]
    for i in range(WRITES):
        span = pl.ds(i * rows, rows)
        copies.append(pltpu.make_async_copy(kc.at[span], k_out.at[span], sem.at[1 + 2 * i]))
        copies.append(pltpu.make_async_copy(vc.at[span], v_out.at[span], sem.at[2 + 2 * i]))
    for copy in copies:
        copy.start()
    for copy in copies:
        copy.wait()


def solution(mesh):
    n = mesh.shape["tp"]
    cache_spec = P(("dp", "tp"), None, None)

    def local_step(hidden, w_query, w_key, w_value, w_out, k_cache, v_cache, lengths):
        rows, seq_len, head_dim = k_cache.shape
        batch, depth = hidden.shape
        cols = w_query.shape[1]
        half_rows = rows // HALVES
        chips = n // 2
        heads = cols * n // head_dim
        half_dim = head_dim // 2
        inv_freq = 10000.0 ** (-(jnp.arange(half_dim, dtype=F32) * 2.0) / head_dim)
        hbm_spec = pl.BlockSpec(memory_space=pltpu.HBM)
        vmem_spec = pl.BlockSpec(memory_space=pltpu.VMEM)
        dma = pltpu.SemaphoreType.DMA
        piece = (n * half_rows, cols // 2)
        y, k_vmem, v_vmem = pl.pallas_call(
            functools.partial(decode_kernel, n),
            out_shape=(
                jax.ShapeDtypeStruct((n, HALVES, half_rows, cols), BF16),
                jax.ShapeDtypeStruct(k_cache.shape, BF16),
                jax.ShapeDtypeStruct(v_cache.shape, BF16),
            ),
            in_specs=[hbm_spec] * 8 + [vmem_spec],
            out_specs=(vmem_spec, vmem_spec, vmem_spec),
            scratch_shapes=[
                pltpu.VMEM((batch, depth), BF16),
                pltpu.VMEM((depth, cols), BF16),
                pltpu.VMEM((depth, head_dim), BF16),
                pltpu.VMEM((depth, head_dim), BF16),
                pltpu.VMEM(w_out.shape, BF16),
                pltpu.SMEM((batch,), jnp.int32),
                pltpu.VMEM((2, batch, head_dim), F32),
                pltpu.VMEM((HALVES, cols // head_dim, n, half_rows, head_dim), BF16),
                pltpu.VMEM((HALVES, cols // head_dim, n, half_rows, head_dim), BF16),
                pltpu.VMEM((half_rows * heads, half_dim), F32),
                pltpu.VMEM((half_rows * heads, half_dim), F32),
                pltpu.VMEM((half_rows * heads, half_dim), F32),
                pltpu.VMEM((half_rows * heads, half_dim), F32),
                pltpu.VMEM((half_rows * heads, seq_len), F32),
                pltpu.VMEM((half_rows * heads, seq_len), BF16),
                pltpu.VMEM((HALVES, n, half_rows, cols), BF16),
                pltpu.VMEM((HALVES, n, half_rows, cols), BF16),
                pltpu.VMEM((HALVES, n * half_rows, cols), BF16),
                pltpu.VMEM((rows, half_dim), F32),
                pltpu.VMEM((rows, half_dim), F32),
                pltpu.VMEM((rows, head_dim), F32),
                pltpu.VMEM((rows, head_dim), F32),
                pltpu.VMEM((HALVES, chips, 2) + piece, F32),
                pltpu.VMEM((HALVES, chips, 2) + piece, BF16),
                pltpu.VMEM((HALVES, chips, 2) + piece, BF16),
                pltpu.VMEM((HALVES, 2, chips - 1) + piece, BF16),
                pltpu.VMEM((HALVES, 2, chips - 1) + piece, BF16),
                dma((1,)),
                dma((cols // head_dim, K_CHUNKS)),
                dma((K_CHUNKS // 2,)),
                dma((HALVES,)),
                dma((1,)),
                dma((1,)),
                dma((HALVES,)),
                dma((1,)),
                dma((HALVES,)),
                dma((1,)),
                dma((HALVES, 5)),
                dma((1,)),
                dma((HALVES, 2, chips - 1)),
            ],
            compiler_params=pltpu.CompilerParams(
                collective_id=0, has_side_effects=True, vmem_limit_bytes=45 * 1024 * 1024
            ),
        )(hidden, w_query, w_key, w_value, w_out, k_cache, v_cache, pltpu.with_memory_space_constraint(lengths, pltpu.HBM), inv_freq[None, :])
        y, k_out, v_out = pl.pallas_call(
            write_kernel,
            out_shape=tuple(jax.ShapeDtypeStruct(a.shape, BF16) for a in (y, k_vmem, v_vmem)),
            in_specs=[vmem_spec] * 3,
            out_specs=(hbm_spec,) * 3,
            scratch_shapes=[dma((1 + 2 * WRITES,))],
            compiler_params=pltpu.CompilerParams(vmem_limit_bytes=1024 * 1024),
        )(y, k_vmem, v_vmem)
        return y.reshape(batch, cols), k_out, v_out

    return jax.shard_map(
        local_step,
        mesh=mesh,
        in_specs=(P("dp", None), P(None, "tp"), P(), P(), P("tp", None), cache_spec, cache_spec, P("dp")),
        out_specs=(P("dp", "tp"), cache_spec, cache_spec),
        check_vma=False,
    )
```

```python
import functools

import jax
import jax.numpy as jnp
from jax import lax
from jax.experimental import pallas as pl
from jax.experimental.pallas import tpu as pltpu
from jax.sharding import PartitionSpec as P

MESH = pl.DeviceIdType.MESH
HALVES = 2
K_CHUNKS = 8
AHEAD = 8
WRITES = 2
F32 = jnp.float32
BF16 = jnp.bfloat16


def decode_kernel(
    n, hid_hbm, wq_hbm, wk_hbm, wv_hbm, wo_hbm, kc_hbm, vc_hbm, len_hbm, freq_ref,
    y_ref, kc, vc,
    hid, wq, wk, wv, wo, lens, acc, qs, qr, q_lo, q_hi, o_lo, o_hi, s_buf, e_buf, osend, orecv, oc, cos_ref, sin_ref, kf, vf,
    pm, ps, pr, rs, rr,
    sem_len, landing, sem_cache, sem_wo,
    q_ssem, q_rsem, o_ssem, o_rsem, p_ssem, r_ssem,
):
    me = lax.axis_index("tp")
    chips = n // 2
    core = lax.rem(me, 2)
    chip = me // 2
    partner = me + 1 - 2 * core
    neighbours = (lax.rem(me + 2, n), lax.rem(me + n - 2, n))

    batch, depth = hid.shape
    cols = wq.shape[1]
    rows = batch // n
    half_rows = rows // HALVES
    seq_len, head_dim = kc.shape[1:]
    half_dim = head_dim // 2
    dev_heads = cols // head_dim
    heads = dev_heads * n
    block = depth // K_CHUNKS
    part = cols // 2
    out_block = wo.shape[1] // 4
    scale = head_dim ** -0.5

    def q_sem(j, i):
        return landing.at[i if j == 0 else K_CHUNKS + (j - 1) * (K_CHUNKS // 2) + i]

    def kv_sem(i):
        return landing.at[K_CHUNKS + (dev_heads - 1) * (K_CHUNKS // 2) + i]

    def ring_sem(h, way, slot):
        return landing.at[(h * 2 + way) * (chips - 1) + slot]

    def partner_sem(h, group):
        return landing.at[HALVES * 2 * (chips - 1) + h * 4 + group]

    def rows_of(hbm, vmem, sem, size, i):
        return pltpu.make_async_copy(hbm.at[pl.ds(i * size, size)], vmem.at[pl.ds(i * size, size)], sem)

    def columns_of(hbm, vmem, sem, size, i):
        return pltpu.make_async_copy(hbm.at[:, pl.ds(i * size, size)], vmem.at[:, pl.ds(i * size, size)], sem)

    def wait_for(buf, sem):
        pltpu.make_async_copy(buf, buf, sem).wait()

    len_copy = pltpu.make_async_copy(len_hbm, lens, sem_len.at[0])
    pair = 2 * block

    def load_q(j, size, i):
        at = (pl.ds(i * size, size), pl.ds(j * head_dim, head_dim))
        return pltpu.make_async_copy(wq_hbm.at[at], wq.at[at], q_sem(j, i))

    queue = [(columns_of(hid_hbm, hid, q_sem(0, i), block, i), load_q(0, block, i)) for i in range(K_CHUNKS)]
    queue += [(load_q(j, pair, i),) for j in range(1, dev_heads) for i in range(K_CHUNKS // 2)]
    queue += [
        (rows_of(wk_hbm, wk, kv_sem(i), pair, i), rows_of(wv_hbm, wv, kv_sem(i), pair, i))
        for i in range(K_CHUNKS // 2)
    ]
    queue += [
        (rows_of(kc_hbm, kc, sem_cache.at[h], half_rows, h), rows_of(vc_hbm, vc, sem_cache.at[h], half_rows, h))
        for h in range(HALVES)
    ]
    queue += [(columns_of(wo_hbm, wo, sem_wo.at[0], out_block, i),) for i in range(4)]
    first_rows = block // dev_heads + block * batch // cols

    def issue(count):
        for _ in range(count):
            if queue:
                for copy in queue.pop(0):
                    copy.start()

    len_copy.start()
    issue(AHEAD)

    barrier = pltpu.get_barrier_semaphore()
    order = sorted(range(1, n), key=lambda i: (min(i, n - i), i), reverse=True)
    for i in order:
        pl.semaphore_signal(barrier, inc=1, device_id={"tp": lax.rem(me + i, n)}, device_id_type=MESH)

    def exchange(src, dst, send_sem, recv_sem, *at):
        for i in order:
            peer = lax.rem(me + i, n)
            pltpu.make_async_remote_copy(
                src_ref=src.at[(*at, peer)],
                dst_ref=dst.at[(*at, me)],
                send_sem=send_sem.at[0],
                recv_sem=recv_sem.at[at[0]],
                device_id={"tp": peer},
                device_id_type=MESH,
            ).start()
        dst[(*at, me)] = src[(*at, me)]

    for j in range(dev_heads):
        size, count = (block, K_CHUNKS) if j == 0 else (pair, K_CHUNKS // 2)
        with jax.named_scope(f"q_mm{j}"):
            for i in range(count):
                wait_for(wq.at[pl.ds(0, first_rows if j == 0 else pair // dev_heads)], q_sem(j, i))
                issue(1)
                terms = []
                for way in range(2):
                    span = pl.ds(i * size + way * (size // 2), size // 2)
                    terms.append(jnp.dot(hid[:, span], wq[span, pl.ds(j * head_dim, head_dim)], preferred_element_type=F32))
                if i < count - 1:
                    for way in range(2):
                        acc[way] = terms[way] if i == 0 else acc[way] + terms[way]
                else:
                    q_all = ((acc[0] + terms[0]) + (acc[1] + terms[1])).reshape(n, HALVES, half_rows, head_dim)
                    for h in range(HALVES):
                        qs[h, j] = q_all[:, h].astype(BF16)
        with jax.named_scope(f"q_send{j}"):
            if j == 0:
                pl.semaphore_wait(barrier, n - 1)
            exchange(qs, qr, q_ssem, q_rsem, 0, j)

    with jax.named_scope("angles"):
        len_copy.wait()
        for r in range(rows):
            cos_ref[pl.ds(r, 1), :] = lens[me * rows + r].astype(F32) * freq_ref[...]
        angles = cos_ref[...]
        sin_ref[...] = jnp.sin(angles)
        cos_ref[...] = jnp.cos(angles)

    def exchange_wait(buf, sem, h):
        wait_for(buf.at[h, pl.ds(0, n - 1)], sem.at[h])

    own = pl.ds(pl.multiple_of(me * rows, rows), rows)
    k_sum = jnp.zeros((rows, head_dim), F32)
    v_sum = jnp.zeros((rows, head_dim), F32)
    for i in range(K_CHUNKS // 2):
        with jax.named_scope(f"kv_wait{i}"):
            wait_for(wk.at[pl.ds(0, 2 * pair)], kv_sem(i))
        issue(1)
        span = pl.ds(i * 2 * block, 2 * block)
        h_own = hid[own, span]
        k_sum += jnp.dot(h_own, wk[span, :], preferred_element_type=F32)
        v_sum += jnp.dot(h_own, wv[span, :], preferred_element_type=F32)
    k_full = k_sum.astype(BF16).astype(F32)
    cosines, sines = cos_ref[...], sin_ref[...]
    k_lo, k_hi = k_full[:, :half_dim], k_full[:, half_dim:]
    k_rot = jnp.concatenate([k_lo * cosines - k_hi * sines, k_hi * cosines + k_lo * sines], axis=-1)
    kf[...] = k_rot.astype(BF16).astype(F32)
    vf[...] = v_sum.astype(BF16).astype(F32)
    issue(len(queue))
    with jax.named_scope("q_sendB"):
        for h in range(1, HALVES):
            for j in range(dev_heads):
                exchange(qs, qr, q_ssem, q_rsem, h, j)

    slots = lax.broadcasted_iota(jnp.int32, (heads, seq_len), 1)

    def attend(h):
        with jax.named_scope(f"q_wait{h}"):
            wait_for(qr.at[h, :, pl.ds(0, n - 1)], q_rsem.at[h])
        with jax.named_scope(f"rope{h}"):
            span = pl.ds(h * half_rows, half_rows)
            cosines, sines = cos_ref[span, :], sin_ref[span, :]
            for src in range(n):
                for j in range(dev_heads):
                    x = qr[h, j, src].astype(F32)
                    lo, hi = x[:, :half_dim], x[:, half_dim:]
                    place = pl.ds(src * dev_heads + j, half_rows, stride=heads)
                    q_lo[place, :] = lo * cosines - hi * sines
                    q_hi[place, :] = hi * cosines + lo * sines
        with jax.named_scope(f"cache_wait{h}"):
            wait_for(kc.at[pl.ds(0, 2 * half_rows)], sem_cache.at[h])
        with jax.named_scope(f"rows{h}"):
            ats = [pl.ds(r * heads, heads) for r in range(half_rows)]
            news = []
            for r, at in enumerate(ats):
                b = h * half_rows + r
                q = jnp.concatenate([q_lo[at, :], q_hi[at, :]], axis=-1).astype(BF16)
                s_buf[at, :] = lax.dot_general(q, kc[b], (((1,), (1,)), ((), ())), preferred_element_type=F32)
                news.append(jnp.sum(q.astype(F32) * kf[pl.ds(b, 1), :], axis=-1, keepdims=True) * scale)
            sums = []
            for r, at in enumerate(ats):
                length = lens[me * rows + h * half_rows + r]
                s = jnp.where(slots < length, s_buf[at, :] * scale, -1e30)
                top = jnp.maximum(jnp.max(s, axis=-1, keepdims=True), news[r])
                e = jnp.where(slots < length, jnp.exp(s - top), 0.0)
                e_new = jnp.exp(news[r] - top)
                e_buf[at, :] = e.astype(BF16)
                sums.append((e_new, jnp.sum(e, axis=-1, keepdims=True) + e_new))
            for r, at in enumerate(ats):
                b = h * half_rows + r
                e_new, total = sums[r]
                o = jnp.dot(e_buf[at, :], vc[b], preferred_element_type=F32)
                o = (o + e_new.astype(BF16).astype(F32) * vf[pl.ds(b, 1), :]) / total
                o_lo[at, :] = o[:, :half_dim]
                o_hi[at, :] = o[:, half_dim:]
        with jax.named_scope(f"opack{h}"):
            for dst in range(n):
                for j in range(dev_heads):
                    place = pl.ds(dst * dev_heads + j, half_rows, stride=heads)
                    osend[h, dst, :, pl.ds(j * head_dim, half_dim)] = o_lo[place, :].astype(BF16)
                    osend[h, dst, :, pl.ds(j * head_dim + half_dim, half_dim)] = o_hi[place, :].astype(BF16)
        with jax.named_scope(f"o_send{h}"):
            exchange(osend, orecv, o_ssem, o_rsem, h)

    for h in range(HALVES):
        attend(h)

    arm = chips // 2

    first_group = ((0, 0), (0, 1), (1, 1), (2, 0))
    last_group = ((1, 0), (2, 1)) + tuple((j, half) for j in range(3, chips) for half in range(2))

    def partner_copy(h, group, j, half=None):
        at = (h, j) if half is None else (h, j, half)
        return pltpu.make_async_remote_copy(
            src_ref=ps.at[at], dst_ref=pr.at[at], send_sem=p_ssem.at[0], recv_sem=partner_sem(h, group),
            device_id={"tp": partner}, device_id_type=MESH,
        )

    def multiplies(h, group):
        with jax.named_scope(f"mult{h}_{group[0][0]}"):
            o_cols = oc[h]

            def products(side, store):
                left = list(group)
                while left:
                    j, half = left.pop(0)
                    whole = bool(left) and left[0][0] == j
                    shift = (1 - 2 * ((j + 1) % 2)) * (arm - (j + 1) // 2)
                    first = (lax.rem(chip + (shift + chips), chips) * 2 + side) * cols + half * part
                    width = cols if whole else part
                    value = jnp.dot(o_cols, wo[:, pl.ds(pl.multiple_of(first, part), width)], preferred_element_type=F32)
                    store(j, half, value[:, :part])
                    if whole:
                        left.pop(0)
                        store(j, 1, value[:, part:])
                        if j == 0 and side is other:
                            partner_copy(h, 0, 0).start()

            def store_other(j, half, value):
                ps[h, j, half] = value.astype(BF16)

            def store_mine(j, half, value):
                pm[h, j, half] = value

            other = 1 - core
            products(other, store_other)
            if group is first_group:
                partner_copy(h, 1, 1, 1).start()
                partner_copy(h, 2, 2, 0).start()
            else:
                partner_copy(h, 3, 1, 0).start()
                partner_copy(h, 3, 2, 1).start()
                for j in range(3, chips):
                    partner_copy(h, 3, j).start()
            products(core, store_mine)

    def ring_copy(h, way, slot):
        return pltpu.make_async_remote_copy(
            src_ref=rs.at[h, way, slot], dst_ref=rr.at[h, way, slot],
            send_sem=r_ssem.at[0], recv_sem=ring_sem(h, way, slot),
            device_id={"tp": neighbours[way]}, device_id_type=MESH,
        )

    met = set()

    def chip_sum(h, j, half):
        group = {(0, 0): 0, (0, 1): 0, (1, 1): 1, (2, 0): 2}.get((j, half), 3)
        if (h, group) not in met:
            met.add((h, group))
            with jax.named_scope(f"pw{h}_{group}"):
                if group == 0:
                    partner_copy(h, 0, 0).wait_recv()
                elif group < 3:
                    partner_copy(h, group, j, half).wait_recv()
                else:
                    wait_for(pr.at[h, pl.ds(0, len(last_group) // 2)], partner_sem(h, 3))
        return pm[h, j, half] + pr[h, j, half].astype(F32)

    def arrived(h, way, slot):
        with jax.named_scope(f"rw{h}_{way}_{slot}"):
            ring_copy(h, way, slot).wait_recv()
        return rr[h, way, slot].astype(F32)

    def pass_on(h, way, long, step):
        hops = (arm if long else arm - 1) - step
        slot = step if long else arm + step
        half = way if long else 1 - way
        value = chip_sum(h, 0 if hops == arm else 1 + 2 * (arm - 1 - hops) + way, half)
        if step > 0:
            value = value + arrived(h, way, slot - 1)
        rs[h, way, slot] = value.astype(BF16)
        ring_copy(h, way, slot).start()

    def reduce_step(h, step):
        for long in (True, False):
            for way in range(2):
                if step < (arm if long else arm - 1):
                    pass_on(h, way, long, step)

    def finish(h):
        for half in range(2):
            value = chip_sum(h, chips - 1, half) + arrived(h, 1 - half, 2 * arm - 2) + arrived(h, half, arm - 1)
            y_ref[:, h, :, pl.ds(half * part, part)] = value.reshape(n, half_rows, part).astype(BF16)

    row_slots = lax.broadcasted_iota(jnp.int32, (seq_len, head_dim), 0)

    def update(b):
        with jax.named_scope(f"update{b}"):
            length = lens[me * rows + b]
            for cache, new in ((kc, kf), (vc, vf)):
                row = jnp.broadcast_to(new[pl.ds(b, 1), :].astype(BF16), (seq_len, head_dim))
                cache[b] = jnp.where(row_slots == length, row, cache[b])

    with jax.named_scope("wo_wait"):
        wait_for(wo, sem_wo.at[0])
    pending = list(range(rows))

    def updates(count):
        for _ in range(count):
            if pending:
                update(pending.pop(0))

    for h in range(HALVES):
        with jax.named_scope(f"o_wait{h}"):
            exchange_wait(orecv, o_rsem, h)
        oc[h] = orecv[h].reshape(n * half_rows, cols)
        multiplies(h, first_group)
        reduce_step(h, 0)
        if h == 0:
            multiplies(h, last_group)
    reduce_step(0, 1)
    for h in range(1, HALVES):
        multiplies(h, last_group)
        reduce_step(h, 1)
        updates(3)
    for step in range(2, arm):
        for h in range(HALVES):
            reduce_step(h, step)
            updates(4)
    updates(rows)
    for h in range(HALVES):
        finish(h)

    with jax.named_scope("tail"):
        wait_for(qs.at[:, :, pl.ds(0, n - 1)], q_ssem.at[0])
        wait_for(osend.at[:, pl.ds(0, n - 1)], o_ssem.at[0])
        wait_for(ps, p_ssem.at[0])
        wait_for(rs, r_ssem.at[0])


def write_kernel(y, kc, vc, y_out, k_out, v_out, sem):
    rows = kc.shape[0] // WRITES
    copies = [pltpu.make_async_copy(y, y_out, sem.at[0])]
    for i in range(WRITES):
        span = pl.ds(i * rows, rows)
        copies.append(pltpu.make_async_copy(kc.at[span], k_out.at[span], sem.at[1 + 2 * i]))
        copies.append(pltpu.make_async_copy(vc.at[span], v_out.at[span], sem.at[2 + 2 * i]))
    for copy in copies:
        copy.start()
    for copy in copies:
        copy.wait()


def solution(mesh):
    n = mesh.shape["tp"]
    cache_spec = P(("dp", "tp"), None, None)

    def local_step(hidden, w_query, w_key, w_value, w_out, k_cache, v_cache, lengths):
        rows, seq_len, head_dim = k_cache.shape
        batch, depth = hidden.shape
        cols = w_query.shape[1]
        half_rows = rows // HALVES
        chips = n // 2
        heads = cols * n // head_dim
        half_dim = head_dim // 2
        inv_freq = 10000.0 ** (-(jnp.arange(half_dim, dtype=F32) * 2.0) / head_dim)
        hbm_spec = pl.BlockSpec(memory_space=pltpu.HBM)
        vmem_spec = pl.BlockSpec(memory_space=pltpu.VMEM)
        dma = pltpu.SemaphoreType.DMA
        piece = (n * half_rows, cols // 2)
        y, k_vmem, v_vmem = pl.pallas_call(
            functools.partial(decode_kernel, n),
            out_shape=(
                jax.ShapeDtypeStruct((n, HALVES, half_rows, cols), BF16),
                jax.ShapeDtypeStruct(k_cache.shape, BF16),
                jax.ShapeDtypeStruct(v_cache.shape, BF16),
            ),
            in_specs=[hbm_spec] * 8 + [vmem_spec],
            out_specs=(vmem_spec, vmem_spec, vmem_spec),
            scratch_shapes=[
                pltpu.VMEM((batch, depth), BF16),
                pltpu.VMEM((depth, cols), BF16),
                pltpu.VMEM((depth, head_dim), BF16),
                pltpu.VMEM((depth, head_dim), BF16),
                pltpu.VMEM(w_out.shape, BF16),
                pltpu.SMEM((batch,), jnp.int32),
                pltpu.VMEM((2, batch, head_dim), F32),
                pltpu.VMEM((HALVES, cols // head_dim, n, half_rows, head_dim), BF16),
                pltpu.VMEM((HALVES, cols // head_dim, n, half_rows, head_dim), BF16),
                pltpu.VMEM((half_rows * heads, half_dim), F32),
                pltpu.VMEM((half_rows * heads, half_dim), F32),
                pltpu.VMEM((half_rows * heads, half_dim), F32),
                pltpu.VMEM((half_rows * heads, half_dim), F32),
                pltpu.VMEM((half_rows * heads, seq_len), F32),
                pltpu.VMEM((half_rows * heads, seq_len), BF16),
                pltpu.VMEM((HALVES, n, half_rows, cols), BF16),
                pltpu.VMEM((HALVES, n, half_rows, cols), BF16),
                pltpu.VMEM((HALVES, n * half_rows, cols), BF16),
                pltpu.VMEM((rows, half_dim), F32),
                pltpu.VMEM((rows, half_dim), F32),
                pltpu.VMEM((rows, head_dim), F32),
                pltpu.VMEM((rows, head_dim), F32),
                pltpu.VMEM((HALVES, chips, 2) + piece, F32),
                pltpu.VMEM((HALVES, chips, 2) + piece, BF16),
                pltpu.VMEM((HALVES, chips, 2) + piece, BF16),
                pltpu.VMEM((HALVES, 2, chips - 1) + piece, BF16),
                pltpu.VMEM((HALVES, 2, chips - 1) + piece, BF16),
                dma((1,)),
                dma((HALVES * 2 * (chips - 1) + HALVES * 4,)),
                dma((HALVES,)),
                dma((1,)),
                dma((1,)),
                dma((HALVES,)),
                dma((1,)),
                dma((HALVES,)),
                dma((1,)),
                dma((1,)),
            ],
            compiler_params=pltpu.CompilerParams(
                collective_id=0, has_side_effects=True, vmem_limit_bytes=45 * 1024 * 1024
            ),
        )(hidden, w_query, w_key, w_value, w_out, k_cache, v_cache, pltpu.with_memory_space_constraint(lengths, pltpu.HBM), inv_freq[None, :])
        y, k_out, v_out = pl.pallas_call(
            write_kernel,
            out_shape=tuple(jax.ShapeDtypeStruct(a.shape, BF16) for a in (y, k_vmem, v_vmem)),
            in_specs=[vmem_spec] * 3,
            out_specs=(hbm_spec,) * 3,
            scratch_shapes=[dma((1 + 2 * WRITES,))],
            compiler_params=pltpu.CompilerParams(vmem_limit_bytes=1024 * 1024),
        )(y, k_vmem, v_vmem)
        return y.reshape(batch, cols), k_out, v_out

    return jax.shard_map(
        local_step,
        mesh=mesh,
        in_specs=(P("dp", None), P(None, "tp"), P(), P(), P("tp", None), cache_spec, cache_spec, P("dp")),
        out_specs=(P("dp", "tp"), cache_spec, cache_spec),
        check_vma=False,
    )
```

```python
import functools

import jax
import jax.numpy as jnp
from jax import lax
from jax.experimental import pallas as pl
from jax.experimental.pallas import tpu as pltpu
from jax.sharding import PartitionSpec as P

MESH = pl.DeviceIdType.MESH
HALVES = 2
K_CHUNKS = 8
AHEAD = 8
WRITES = 2
F32 = jnp.float32
BF16 = jnp.bfloat16


def decode_kernel(
    n, hid_hbm, wq_hbm, wk_hbm, wv_hbm, wo_hbm, kc_hbm, vc_hbm, len_hbm, freq_ref,
    y_ref, kc, vc,
    hid, wq, wk, wv, wo, lens, acc, qs, qr, q_lo, q_hi, o_lo, o_hi, s_buf, e_buf, osend, orecv, oc, cos_ref, sin_ref, kf, vf,
    pm, ps, pr, rs, rr,
    sem_len, landing, sem_cache, sem_wo,
    q_ssem, q_rsem, o_ssem, o_rsem, p_ssem, r_ssem,
):
    me = lax.axis_index("tp")
    chips = n // 2
    core = lax.rem(me, 2)
    chip = me // 2
    partner = me + 1 - 2 * core
    neighbours = (lax.rem(me + 2, n), lax.rem(me + n - 2, n))

    batch, depth = hid.shape
    cols = wq.shape[1]
    rows = batch // n
    half_rows = rows // HALVES
    seq_len, head_dim = kc.shape[1:]
    half_dim = head_dim // 2
    dev_heads = cols // head_dim
    heads = dev_heads * n
    block = depth // K_CHUNKS
    part = cols // 2
    out_block = wo.shape[1] // 4
    scale = head_dim ** -0.5

    def q_sem(j, i):
        return landing.at[i if j == 0 else K_CHUNKS + (j - 1) * (K_CHUNKS // 2) + i]

    def kv_sem(i):
        return landing.at[K_CHUNKS + (dev_heads - 1) * (K_CHUNKS // 2) + i]

    def ring_sem(h, way, slot):
        return landing.at[(h * 2 + way) * (chips - 1) + slot]

    def partner_sem(h, group):
        return landing.at[HALVES * 2 * (chips - 1) + h * 4 + group]

    def rows_of(hbm, vmem, sem, size, i):
        return pltpu.make_async_copy(hbm.at[pl.ds(i * size, size)], vmem.at[pl.ds(i * size, size)], sem)

    def columns_of(hbm, vmem, sem, size, i):
        return pltpu.make_async_copy(hbm.at[:, pl.ds(i * size, size)], vmem.at[:, pl.ds(i * size, size)], sem)

    def wait_for(buf, sem):
        pltpu.make_async_copy(buf, buf, sem).wait()

    len_copy = pltpu.make_async_copy(len_hbm, lens, sem_len.at[0])
    pair = 2 * block

    def load_q(j, size, i):
        at = (pl.ds(i * size, size), pl.ds(j * head_dim, head_dim))
        return pltpu.make_async_copy(wq_hbm.at[at], wq.at[at], q_sem(j, i))

    queue = [(columns_of(hid_hbm, hid, q_sem(0, i), block, i), load_q(0, block, i)) for i in range(K_CHUNKS)]
    queue += [(load_q(j, pair, i),) for j in range(1, dev_heads) for i in range(K_CHUNKS // 2)]
    queue += [
        (rows_of(wk_hbm, wk, kv_sem(i), pair, i), rows_of(wv_hbm, wv, kv_sem(i), pair, i))
        for i in range(K_CHUNKS // 2)
    ]
    queue += [
        (rows_of(kc_hbm, kc, sem_cache.at[h], half_rows, h), rows_of(vc_hbm, vc, sem_cache.at[h], half_rows, h))
        for h in range(HALVES)
    ]
    queue += [(columns_of(wo_hbm, wo, sem_wo.at[0], out_block, i),) for i in range(4)]
    first_rows = block // dev_heads + block * batch // cols

    def issue(count):
        for _ in range(count):
            if queue:
                for copy in queue.pop(0):
                    copy.start()

    len_copy.start()
    issue(AHEAD)

    barrier = pltpu.get_barrier_semaphore()
    order = sorted(range(1, n), key=lambda i: (min(i, n - i), i), reverse=True)
    for i in order:
        pl.semaphore_signal(barrier, inc=1, device_id={"tp": lax.rem(me + i, n)}, device_id_type=MESH)

    def exchange(src, dst, send_sem, recv_sem, *at):
        for i in order:
            peer = lax.rem(me + i, n)
            pltpu.make_async_remote_copy(
                src_ref=src.at[(*at, peer)],
                dst_ref=dst.at[(*at, me)],
                send_sem=send_sem.at[0],
                recv_sem=recv_sem.at[at[0]],
                device_id={"tp": peer},
                device_id_type=MESH,
            ).start()
        dst[(*at, me)] = src[(*at, me)]

    for j in range(dev_heads):
        size, count = (block, K_CHUNKS) if j == 0 else (pair, K_CHUNKS // 2)
        with jax.named_scope(f"q_mm{j}"):
            for i in range(count):
                wait_for(wq.at[pl.ds(0, first_rows if j == 0 else pair // dev_heads)], q_sem(j, i))
                issue(1)
                terms = []
                for way in range(2):
                    span = pl.ds(i * size + way * (size // 2), size // 2)
                    terms.append(jnp.dot(hid[:, span], wq[span, pl.ds(j * head_dim, head_dim)], preferred_element_type=F32))
                if i < count - 1:
                    for way in range(2):
                        acc[way] = terms[way] if i == 0 else acc[way] + terms[way]
                else:
                    q_all = ((acc[0] + terms[0]) + (acc[1] + terms[1])).reshape(n, HALVES, half_rows, head_dim)
                    for h in range(HALVES):
                        qs[h, j] = q_all[:, h].astype(BF16)
        with jax.named_scope(f"q_send{j}"):
            if j == 0:
                pl.semaphore_wait(barrier, n - 1)
            exchange(qs, qr, q_ssem, q_rsem, 0, j)

    with jax.named_scope("angles"):
        len_copy.wait()
        for r in range(rows):
            cos_ref[pl.ds(r, 1), :] = lens[me * rows + r].astype(F32) * freq_ref[...]
        angles = cos_ref[...]
        sin_ref[...] = jnp.sin(angles)
        cos_ref[...] = jnp.cos(angles)

    def exchange_wait(buf, sem, h):
        wait_for(buf.at[h, pl.ds(0, n - 1)], sem.at[h])

    own = pl.ds(pl.multiple_of(me * rows, rows), rows)
    k_sum = jnp.zeros((rows, head_dim), F32)
    v_sum = jnp.zeros((rows, head_dim), F32)
    for i in range(K_CHUNKS // 2):
        with jax.named_scope(f"kv_wait{i}"):
            wait_for(wk.at[pl.ds(0, 2 * pair)], kv_sem(i))
        issue(1)
        span = pl.ds(i * 2 * block, 2 * block)
        h_own = hid[own, span]
        k_sum += jnp.dot(h_own, wk[span, :], preferred_element_type=F32)
        v_sum += jnp.dot(h_own, wv[span, :], preferred_element_type=F32)
    k_full = k_sum.astype(BF16).astype(F32)
    cosines, sines = cos_ref[...], sin_ref[...]
    k_lo, k_hi = k_full[:, :half_dim], k_full[:, half_dim:]
    k_rot = jnp.concatenate([k_lo * cosines - k_hi * sines, k_hi * cosines + k_lo * sines], axis=-1)
    kf[...] = k_rot.astype(BF16).astype(F32)
    vf[...] = v_sum.astype(BF16).astype(F32)
    issue(len(queue))
    with jax.named_scope("q_sendB"):
        for h in range(1, HALVES):
            for j in range(dev_heads):
                exchange(qs, qr, q_ssem, q_rsem, h, j)

    slots = lax.broadcasted_iota(jnp.int32, (heads, seq_len), 1)

    def attend(h):
        with jax.named_scope(f"q_wait{h}"):
            wait_for(qr.at[h, :, pl.ds(0, n - 1)], q_rsem.at[h])
        with jax.named_scope(f"rope{h}"):
            span = pl.ds(h * half_rows, half_rows)
            cosines, sines = cos_ref[span, :], sin_ref[span, :]
            for src in range(n):
                for j in range(dev_heads):
                    x = qr[h, j, src].astype(F32)
                    lo, hi = x[:, :half_dim], x[:, half_dim:]
                    place = pl.ds(src * dev_heads + j, half_rows, stride=heads)
                    q_lo[place, :] = lo * cosines - hi * sines
                    q_hi[place, :] = hi * cosines + lo * sines
        with jax.named_scope(f"cache_wait{h}"):
            wait_for(kc.at[pl.ds(0, 2 * half_rows)], sem_cache.at[h])
        with jax.named_scope(f"rows{h}"):
            ats = [pl.ds(r * heads, heads) for r in range(half_rows)]
            news = []
            for r, at in enumerate(ats):
                b = h * half_rows + r
                q = jnp.concatenate([q_lo[at, :], q_hi[at, :]], axis=-1).astype(BF16)
                s_buf[at, :] = lax.dot_general(q, kc[b], (((1,), (1,)), ((), ())), preferred_element_type=F32)
                news.append(jnp.sum(q.astype(F32) * kf[pl.ds(b, 1), :], axis=-1, keepdims=True) * scale)
            sums = []
            for r, at in enumerate(ats):
                length = lens[me * rows + h * half_rows + r]
                s = jnp.where(slots < length, s_buf[at, :] * scale, -1e30)
                top = jnp.maximum(jnp.max(s, axis=-1, keepdims=True), news[r])
                e = jnp.where(slots < length, jnp.exp(s - top), 0.0)
                e_new = jnp.exp(news[r] - top)
                e_buf[at, :] = e.astype(BF16)
                sums.append((e_new, jnp.sum(e, axis=-1, keepdims=True) + e_new))
            for r, at in enumerate(ats):
                b = h * half_rows + r
                e_new, total = sums[r]
                o = jnp.dot(e_buf[at, :], vc[b], preferred_element_type=F32)
                o = (o + e_new.astype(BF16).astype(F32) * vf[pl.ds(b, 1), :]) / total
                o_lo[at, :] = o[:, :half_dim]
                o_hi[at, :] = o[:, half_dim:]
        with jax.named_scope(f"opack{h}"):
            for dst in range(n):
                for j in range(dev_heads):
                    place = pl.ds(dst * dev_heads + j, half_rows, stride=heads)
                    osend[h, dst, :, pl.ds(j * head_dim, half_dim)] = o_lo[place, :].astype(BF16)
                    osend[h, dst, :, pl.ds(j * head_dim + half_dim, half_dim)] = o_hi[place, :].astype(BF16)
        with jax.named_scope(f"o_send{h}"):
            exchange(osend, orecv, o_ssem, o_rsem, h)

    for h in range(HALVES):
        attend(h)

    arm = chips // 2

    first_group = ((0, 0), (0, 1), (1, 1), (2, 0))
    last_group = ((1, 0), (2, 1)) + tuple((j, half) for j in range(3, chips) for half in range(2))

    def partner_copy(h, group, j, half=None):
        at = (h, j) if half is None else (h, j, half)
        return pltpu.make_async_remote_copy(
            src_ref=ps.at[at], dst_ref=pr.at[at], send_sem=p_ssem.at[0], recv_sem=partner_sem(h, group),
            device_id={"tp": partner}, device_id_type=MESH,
        )

    def multiplies(h, group):
        with jax.named_scope(f"mult{h}_{group[0][0]}"):
            o_cols = oc[h]

            def products(side, store):
                left = list(group)
                while left:
                    j, half = left.pop(0)
                    whole = bool(left) and left[0][0] == j
                    shift = (1 - 2 * ((j + 1) % 2)) * (arm - (j + 1) // 2)
                    first = (lax.rem(chip + (shift + chips), chips) * 2 + side) * cols + half * part
                    width = cols if whole else part
                    value = jnp.dot(o_cols, wo[:, pl.ds(pl.multiple_of(first, part), width)], preferred_element_type=F32)
                    store(j, half, value[:, :part])
                    if whole:
                        left.pop(0)
                        store(j, 1, value[:, part:])
                        if j == 0 and side is other:
                            partner_copy(h, 0, 0).start()

            def store_other(j, half, value):
                ps[h, j, half] = value.astype(BF16)

            def store_mine(j, half, value):
                pm[h, j, half] = value

            other = 1 - core
            products(other, store_other)
            if group is first_group:
                partner_copy(h, 1, 1, 1).start()
                partner_copy(h, 2, 2, 0).start()
            else:
                partner_copy(h, 3, 1, 0).start()
                partner_copy(h, 3, 2, 1).start()
                for j in range(3, chips):
                    partner_copy(h, 3, j).start()
            products(core, store_mine)

    def ring_copy(h, way, slot):
        return pltpu.make_async_remote_copy(
            src_ref=rs.at[h, way, slot], dst_ref=rr.at[h, way, slot],
            send_sem=r_ssem.at[0], recv_sem=ring_sem(h, way, slot),
            device_id={"tp": neighbours[way]}, device_id_type=MESH,
        )

    met = set()

    def chip_sum(h, j, half):
        group = {(0, 0): 0, (0, 1): 0, (1, 1): 1, (2, 0): 2}.get((j, half), 3)
        if (h, group) not in met:
            met.add((h, group))
            with jax.named_scope(f"pw{h}_{group}"):
                if group == 0:
                    partner_copy(h, 0, 0).wait_recv()
                elif group < 3:
                    partner_copy(h, group, j, half).wait_recv()
                else:
                    wait_for(pr.at[h, pl.ds(0, len(last_group) // 2)], partner_sem(h, 3))
        return pm[h, j, half] + pr[h, j, half].astype(F32)

    def arrived(h, way, slot):
        with jax.named_scope(f"rw{h}_{way}_{slot}"):
            ring_copy(h, way, slot).wait_recv()
        return rr[h, way, slot].astype(F32)

    def pass_on(h, way, long, step):
        hops = (arm if long else arm - 1) - step
        slot = step if long else arm + step
        half = way if long else 1 - way
        value = chip_sum(h, 0 if hops == arm else 1 + 2 * (arm - 1 - hops) + way, half)
        if step > 0:
            value = value + arrived(h, way, slot - 1)
        rs[h, way, slot] = value.astype(BF16)
        ring_copy(h, way, slot).start()

    def reduce_step(h, step):
        for long in (True, False):
            for way in (h % 2, 1 - h % 2):
                if step < (arm if long else arm - 1):
                    pass_on(h, way, long, step)

    def finish(h):
        for half in range(2):
            value = chip_sum(h, chips - 1, half) + arrived(h, 1 - half, 2 * arm - 2) + arrived(h, half, arm - 1)
            y_ref[:, h, :, pl.ds(half * part, part)] = value.reshape(n, half_rows, part).astype(BF16)

    row_slots = lax.broadcasted_iota(jnp.int32, (seq_len, head_dim), 0)

    def update(b):
        with jax.named_scope(f"update{b}"):
            length = lens[me * rows + b]
            for cache, new in ((kc, kf), (vc, vf)):
                row = jnp.broadcast_to(new[pl.ds(b, 1), :].astype(BF16), (seq_len, head_dim))
                cache[b] = jnp.where(row_slots == length, row, cache[b])

    with jax.named_scope("wo_wait"):
        wait_for(wo, sem_wo.at[0])
    pending = list(range(rows))

    def updates(count):
        for _ in range(count):
            if pending:
                update(pending.pop(0))

    for h in range(HALVES):
        with jax.named_scope(f"o_wait{h}"):
            exchange_wait(orecv, o_rsem, h)
        oc[h] = orecv[h].reshape(n * half_rows, cols)
        multiplies(h, first_group)
        reduce_step(h, 0)
        if h == 0:
            multiplies(h, last_group)
    reduce_step(0, 1)
    for h in range(1, HALVES):
        multiplies(h, last_group)
        reduce_step(h, 1)
        updates(3)
    for step in range(2, arm):
        for h in range(HALVES):
            reduce_step(h, step)
            updates(4)
    updates(rows)
    for h in range(HALVES):
        finish(h)

    with jax.named_scope("tail"):
        wait_for(qs.at[:, :, pl.ds(0, n - 1)], q_ssem.at[0])
        wait_for(osend.at[:, pl.ds(0, n - 1)], o_ssem.at[0])
        wait_for(ps, p_ssem.at[0])
        wait_for(rs, r_ssem.at[0])


def write_kernel(y, kc, vc, y_out, k_out, v_out, sem):
    rows = kc.shape[0] // WRITES
    copies = [pltpu.make_async_copy(y, y_out, sem.at[0])]
    for i in range(WRITES):
        span = pl.ds(i * rows, rows)
        copies.append(pltpu.make_async_copy(kc.at[span], k_out.at[span], sem.at[1 + 2 * i]))
        copies.append(pltpu.make_async_copy(vc.at[span], v_out.at[span], sem.at[2 + 2 * i]))
    for copy in copies:
        copy.start()
    for copy in copies:
        copy.wait()


def solution(mesh):
    n = mesh.shape["tp"]
    cache_spec = P(("dp", "tp"), None, None)

    def local_step(hidden, w_query, w_key, w_value, w_out, k_cache, v_cache, lengths):
        rows, seq_len, head_dim = k_cache.shape
        batch, depth = hidden.shape
        cols = w_query.shape[1]
        half_rows = rows // HALVES
        chips = n // 2
        heads = cols * n // head_dim
        half_dim = head_dim // 2
        inv_freq = 10000.0 ** (-(jnp.arange(half_dim, dtype=F32) * 2.0) / head_dim)
        hbm_spec = pl.BlockSpec(memory_space=pltpu.HBM)
        vmem_spec = pl.BlockSpec(memory_space=pltpu.VMEM)
        dma = pltpu.SemaphoreType.DMA
        piece = (n * half_rows, cols // 2)
        y, k_vmem, v_vmem = pl.pallas_call(
            functools.partial(decode_kernel, n),
            out_shape=(
                jax.ShapeDtypeStruct((n, HALVES, half_rows, cols), BF16),
                jax.ShapeDtypeStruct(k_cache.shape, BF16),
                jax.ShapeDtypeStruct(v_cache.shape, BF16),
            ),
            in_specs=[hbm_spec] * 8 + [vmem_spec],
            out_specs=(vmem_spec, vmem_spec, vmem_spec),
            scratch_shapes=[
                pltpu.VMEM((batch, depth), BF16),
                pltpu.VMEM((depth, cols), BF16),
                pltpu.VMEM((depth, head_dim), BF16),
                pltpu.VMEM((depth, head_dim), BF16),
                pltpu.VMEM(w_out.shape, BF16),
                pltpu.SMEM((batch,), jnp.int32),
                pltpu.VMEM((2, batch, head_dim), F32),
                pltpu.VMEM((HALVES, cols // head_dim, n, half_rows, head_dim), BF16),
                pltpu.VMEM((HALVES, cols // head_dim, n, half_rows, head_dim), BF16),
                pltpu.VMEM((half_rows * heads, half_dim), F32),
                pltpu.VMEM((half_rows * heads, half_dim), F32),
                pltpu.VMEM((half_rows * heads, half_dim), F32),
                pltpu.VMEM((half_rows * heads, half_dim), F32),
                pltpu.VMEM((half_rows * heads, seq_len), F32),
                pltpu.VMEM((half_rows * heads, seq_len), BF16),
                pltpu.VMEM((HALVES, n, half_rows, cols), BF16),
                pltpu.VMEM((HALVES, n, half_rows, cols), BF16),
                pltpu.VMEM((HALVES, n * half_rows, cols), BF16),
                pltpu.VMEM((rows, half_dim), F32),
                pltpu.VMEM((rows, half_dim), F32),
                pltpu.VMEM((rows, head_dim), F32),
                pltpu.VMEM((rows, head_dim), F32),
                pltpu.VMEM((HALVES, chips, 2) + piece, F32),
                pltpu.VMEM((HALVES, chips, 2) + piece, BF16),
                pltpu.VMEM((HALVES, chips, 2) + piece, BF16),
                pltpu.VMEM((HALVES, 2, chips - 1) + piece, BF16),
                pltpu.VMEM((HALVES, 2, chips - 1) + piece, BF16),
                dma((1,)),
                dma((HALVES * 2 * (chips - 1) + HALVES * 4,)),
                dma((HALVES,)),
                dma((1,)),
                dma((1,)),
                dma((HALVES,)),
                dma((1,)),
                dma((HALVES,)),
                dma((1,)),
                dma((1,)),
            ],
            compiler_params=pltpu.CompilerParams(
                collective_id=0, has_side_effects=True, vmem_limit_bytes=45 * 1024 * 1024
            ),
        )(hidden, w_query, w_key, w_value, w_out, k_cache, v_cache, pltpu.with_memory_space_constraint(lengths, pltpu.HBM), inv_freq[None, :])
        y, k_out, v_out = pl.pallas_call(
            write_kernel,
            out_shape=tuple(jax.ShapeDtypeStruct(a.shape, BF16) for a in (y, k_vmem, v_vmem)),
            in_specs=[vmem_spec] * 3,
            out_specs=(hbm_spec,) * 3,
            scratch_shapes=[dma((1 + 2 * WRITES,))],
            compiler_params=pltpu.CompilerParams(vmem_limit_bytes=1024 * 1024),
        )(y, k_vmem, v_vmem)
        return y.reshape(batch, cols), k_out, v_out

    return jax.shard_map(
        local_step,
        mesh=mesh,
        in_specs=(P("dp", None), P(None, "tp"), P(), P(), P("tp", None), cache_spec, cache_spec, P("dp")),
        out_specs=(P("dp", "tp"), cache_spec, cache_spec),
        check_vma=False,
    )
```
